32 devices in a mesh: lat: 4 (over z), lon: 8 (over y, x, core).
Axes of the slice: x: 2, y: 2, z: 4, core: 2. Of those that a mesh axis runs over, the one named last changes fastest.
Arguments:
- zonal_wind: float32 [32, 32, 2048], P(None, 'lat', 'lon'), may hold values from -6 to 6
- merid_wind: float32 [32, 32, 2048], P(None, 'lat', 'lon'), may hold values from -6 to 6
- vertical_wind: float32 [32, 32, 2048], P(None, 'lat', 'lon'), may hold values from -6 to 6
- pressure: float32 [32, 32, 2048], P(None, 'lat', 'lon'), may hold values from -6 to 6
- zonal_coef: float32 [32], P('lat'), may hold values from 0.05 to 0.4
- merid_coef: float32 [32], P('lat'), may hold values from 0.05 to 0.4
- level_coef: float32 [32], replicated, may hold values from 0.3 to 1.5
- sound_coef: float32 [32, 32, 2048], P(None, 'lat', 'lon'), may hold values from 0.2 to 2
- cutoff: int32 [32], replicated, may hold values from 1 to 511
- filter_mask: int32 [32], replicated, may hold values from 0 to 1, as said below
Outputs:
- zonal_next: float32 [32, 32, 2048], P(None, 'lat', 'lon')
- merid_next: float32 [32, 32, 2048], P(None, 'lat', 'lon')
- vertical_next: float32 [32, 32, 2048], P(None, 'lat', 'lon')
- pressure_next: float32 [32, 32, 2048], P(None, 'lat', 'lon')
The draws below stay inside these ranges and needn't reach their ends.
Inputs may be any that keep to these rules, and one draw needn't show every extreme that they name: `filter_mask`: for every latitude j below 16 exactly one of j and j + 16 is filtered; the filtered ones are the first n and the last 16 - n latitudes, for some n from 4 to 12.
All inputs are finite; a program needn't handle non-finite values.
Results may differ from the reference program's by a relative error of at most 0.0001.
Values sent between devices are 32-bit elements; how exact they have to be, the bound alone decides.
A program may use at most 64 MiB of HBM per device.

```python
import math
import jax
import jax.numpy as jnp
from jax import lax

NLON = 2048
NLEV = 32
SUBSTEPS = 2
NLAT = 32


def draw_filter_mask(key, part):
    latitudes = jnp.arange(NLAT)
    northern = jax.random.randint(jax.random.fold_in(key, 17), (), NLAT // 8, 3 * NLAT // 8 + 1)
    southern_start = NLAT // 2 + northern
    return jnp.logical_or(latitudes < northern, latitudes >= southern_start).astype(jnp.int32)


def set_ends(drawn, own_key, smallest, top_value):
    place = [jax.random.randint(jax.random.fold_in(own_key, axis), (), 0, length) for axis, length in enumerate(drawn.shape)]
    widest = drawn.shape.index(max(drawn.shape))
    beside = place[:widest] + [(place[widest] + 1) % drawn.shape[widest]] + place[widest + 1:]
    return drawn.at[tuple(place)].set(smallest).at[tuple(beside)].set(top_value)


def block_scale(stream_key, extent, cuts, low, top_value):
    level = 1.0
    for position, parts in cuts:
        draws = jax.random.uniform(jax.random.fold_in(jax.random.fold_in(stream_key, 6), position), (parts,), jnp.float32, low / len(cuts), top_value / len(cuts))
        level = level * jnp.repeat(jnp.exp(draws), extent[position] // parts).reshape((-1,) + (1,) * (len(extent) - 1 - position))
    return level


def noise(own_key, dims, deviation, reach, shards=(), dtype=jnp.bfloat16):
    entries = deviation * jax.random.normal(own_key, dims, jnp.float32)
    if shards:
        entries = entries * block_scale(own_key, dims, shards, -0.22, 0.18)
    return jnp.clip(entries, -reach, reach).astype(dtype)


def setup_inputs(seed: int = 0) -> dict:
    streams_of = jax.random.split(jax.random.key(seed), 11)
    return {
        "zonal_wind": noise(streams_of[0], (NLEV, NLAT, NLON), 1.0, 6.0, ((1, 4), (2, 8)), jnp.float32),
        "merid_wind": noise(streams_of[1], (NLEV, NLAT, NLON), 1.0, 6.0, ((1, 4), (2, 8)), jnp.float32),
        "vertical_wind": noise(streams_of[2], (NLEV, NLAT, NLON), 1.0, 6.0, ((1, 4), (2, 8)), jnp.float32),
        "pressure": noise(streams_of[3], (NLEV, NLAT, NLON), 1.0, 6.0, ((1, 4), (2, 8)), jnp.float32),
        "zonal_coef": jnp.clip(jnp.exp(math.log(0.4) - 2.0794415 * jax.random.uniform(streams_of[4], (NLAT,), jnp.float32) ** block_scale(streams_of[4], (NLAT,), ((0, 4),), -0.2, 0.2)), 0.05, 0.4),
        "merid_coef": jnp.clip(jnp.exp(math.log(0.4) - 2.0794415 * jax.random.uniform(streams_of[5], (NLAT,), jnp.float32) ** block_scale(streams_of[5], (NLAT,), ((0, 4),), -0.2, 0.2)), 0.05, 0.4),
        "level_coef": jnp.clip(jnp.exp(jax.random.uniform(streams_of[6], (NLEV,), jnp.float32, math.log(0.3), math.log(1.5))), 0.3, 1.5),
        "sound_coef": jnp.clip(jnp.exp(math.log(2.0) - 2.3025851 * jax.random.uniform(streams_of[7], (NLEV, NLAT, NLON), jnp.float32) ** block_scale(streams_of[7], (NLEV, NLAT, NLON), ((1, 4), (2, 8)), -0.2, 0.2)), 0.2, 2.0),
        "cutoff": set_ends(jax.random.randint(streams_of[8], (NLAT,), 1, NLON // 4), jax.random.fold_in(streams_of[8], 1), 1, (NLON // 4) - 1).astype(jnp.int32),
        "filter_mask": draw_filter_mask(jax.random.fold_in(streams_of[10], 71), 0),
    }


def zonal_diff(field):
    return jnp.roll(field, -1, axis=2) - jnp.roll(field, 1, axis=2)


def merid_diff(field):
    padded = jnp.pad(field, ((0, 0), (1, 1), (0, 0)))
    return padded[:, 2:, :] - padded[:, :-2, :]


def damping(wavenum, limits):
    bound_col = limits[:, None]
    ratio = bound_col / jnp.maximum(wavenum[None, :], 1.0)
    return jnp.where(wavenum[None, :] > bound_col, ratio * ratio, 1.0)


def polar_damp(field, cutoff, filter_mask):
    wavenum = jnp.arange(NLON // 2 + 1).astype(jnp.float32)
    factor = damping(wavenum, cutoff.astype(jnp.float32))

    def one_level(slab):
        spectra = jnp.fft.rfft(slab, axis=1)
        return jnp.fft.irfft(spectra * factor, n=NLON, axis=1).astype(jnp.float32)

    damped = lax.map(one_level, field)
    return jnp.where(filter_mask[None, :, None] > 0, damped, field)


def column_solve(vertical_wind, pstar, level_coef, sound_coef):
    levels = vertical_wind.shape[0]
    zero_slab = jnp.zeros_like(vertical_wind[0])
    ratios = []
    values = []
    prev_ratio = zero_slab
    prev_value = zero_slab
    for level in range(levels):
        alpha = level_coef[level]
        below = alpha * sound_coef[level]
        if level + 1 < levels:
            above = alpha * sound_coef[level + 1]
            rhs = vertical_wind[level] - alpha * (pstar[level + 1] - pstar[level])
        else:
            above = zero_slab
            rhs = vertical_wind[level] + alpha * pstar[level]
        pivot = 1.0 + below + above + below * prev_ratio
        prev_ratio = -above / pivot
        prev_value = (rhs + below * prev_value) / pivot
        ratios.append(prev_ratio)
        values.append(prev_value)
    solved = [zero_slab] * levels
    upper_value = values[levels - 1]
    solved[levels - 1] = upper_value
    for level in range(levels - 2, -1, -1):
        upper_value = values[level] - ratios[level] * upper_value
        solved[level] = upper_value
    new_wind = jnp.stack(solved)
    wind_below = jnp.concatenate([zero_slab[None], new_wind[:-1]], axis=0)
    new_pressure = pstar - sound_coef * (new_wind - wind_below)
    return new_wind, new_pressure


def reference(zonal_wind, merid_wind, vertical_wind, pressure, zonal_coef, merid_coef, level_coef, sound_coef, cutoff, filter_mask):
    zonal_rows = zonal_coef[None, :, None]
    merid_rows = merid_coef[None, :, None]
    for step in range(SUBSTEPS):
        zonal_step = -zonal_rows * zonal_diff(pressure)
        merid_step = -merid_rows * merid_diff(pressure)
        zonal_wind = zonal_wind + polar_damp(zonal_step, cutoff, filter_mask)
        merid_wind = merid_wind + polar_damp(merid_step, cutoff, filter_mask)
        diverge = zonal_rows * zonal_diff(zonal_wind) + merid_rows * merid_diff(merid_wind)
        pstar = pressure - sound_coef * diverge
        vertical_wind, pressure = column_solve(vertical_wind, pstar, level_coef, sound_coef)
    return (zonal_wind, merid_wind, vertical_wind, pressure)
```

```python
import functools
import math

import ml_dtypes
import numpy as np
import jax
import jax.numpy as jnp
from jax import lax
from jax.experimental import pallas as pl
from jax.experimental.pallas import tpu as pltpu
from jax.sharding import PartitionSpec as P

SUBSTEPS = 2
FUSED_VMEM = 40 * 2 ** 20
FINISH_VMEM = 4 * 2 ** 20


def extended(block, sides, width):
    for axis, dim in sides:
        count = lax.axis_size(axis)
        forward = [(i, i + 1) for i in range(count - 1)]
        forward.append((count - 1, 0))
        backward = [(target, source) for source, target in forward]
        low = lax.ppermute(
            lax.slice_in_dim(block, block.shape[dim] - width, None, axis=dim), axis, forward
        )
        high = lax.ppermute(lax.slice_in_dim(block, 0, width, axis=dim), axis, backward)
        block = jnp.concatenate([low, block, high], axis=dim)
    return block


def rim_fix(padded, lat_dim):
    band_index = lax.axis_index("lat")
    bands = lax.axis_size("lat")
    extent = padded.shape[lat_dim]
    position = lax.broadcasted_iota(jnp.int32, padded.shape, lat_dim)
    first_edge = jnp.logical_and(position == 0, band_index == 0)
    final_edge = jnp.logical_and(position == extent - 1, band_index == bands - 1)
    return jnp.where(jnp.logical_or(first_edge, final_edge), 0.0, padded)


def dft_tables(length):
    half_len = length // 2
    sample = lax.broadcasted_iota(jnp.int32, (length, length), 0)
    column = lax.broadcasted_iota(jnp.int32, (length, length), 1)
    is_cosine = column <= half_len
    wavenum = jnp.where(is_cosine, column, column - half_len)
    phase = sample * wavenum % length
    angle = 2.0 * math.pi / length * phase.astype(jnp.float32)
    forward = jnp.where(is_cosine, jnp.cos(angle), jnp.sin(angle))
    single = jnp.logical_and(is_cosine, jnp.logical_or(wavenum == 0, wavenum == half_len))
    weight = jnp.where(single, 1.0, 2.0) / length
    inverse = jnp.transpose(forward * weight)
    wave_row = wavenum[0].astype(jnp.float32)
    return (forward, inverse, wave_row)


def damping(wave_row, limits):
    bound_col = limits[:, None]
    ratio = bound_col / jnp.maximum(wave_row[None, :], 1.0)
    return jnp.where(wave_row[None, :] > bound_col, ratio * ratio, 1.0)


def transform_band(block, limits, forward, inverse, wave_row):
    circles = lax.all_to_all(block, "lon", split_axis=1, concat_axis=3, tiled=True)
    spectra = jnp.einsum("vetj,jc->vetc", circles, forward, precision=lax.Precision.HIGHEST)
    scaled = spectra * damping(wave_row, limits)
    damped = jnp.einsum("vetc,cj->vetj", scaled, inverse, precision=lax.Precision.HIGHEST)
    return lax.all_to_all(damped, "lon", split_axis=3, concat_axis=1, tiled=True)


def filtered_increments(increments, own_flags, own_limits, forward, inverse, wave_row):
    flag_cols = own_flags[:, None]
    damped = transform_band(increments, own_limits, forward, inverse, wave_row)
    return jnp.where(flag_cols, damped, increments)


def column_solve(vertical_wind, pstar, level_coef, sound_coef):
    levels = vertical_wind.shape[0]
    zero_slab = jnp.zeros_like(vertical_wind[0])
    ratios = []
    values = []
    prev_ratio = zero_slab
    prev_value = zero_slab
    for level in range(levels):
        alpha = level_coef[level]
        below = alpha * sound_coef[level]
        if level + 1 < levels:
            above = alpha * sound_coef[level + 1]
            rhs = vertical_wind[level] - alpha * (pstar[level + 1] - pstar[level])
        else:
            above = zero_slab
            rhs = vertical_wind[level] + alpha * pstar[level]
        pivot = 1.0 + below + above + below * prev_ratio
        prev_ratio = -above / pivot
        prev_value = (rhs + below * prev_value) / pivot
        ratios.append(prev_ratio)
        values.append(prev_value)
    solved = [zero_slab] * levels
    upper_value = values[levels - 1]
    solved[levels - 1] = upper_value
    for level in range(levels - 2, -1, -1):
        upper_value = values[level] - ratios[level] * upper_value
        solved[level] = upper_value
    new_wind = jnp.stack(solved)
    wind_below = jnp.concatenate([zero_slab[None], new_wind[:-1]], axis=0)
    new_pressure = pstar - sound_coef * (new_wind - wind_below)
    return (new_wind, new_pressure)


def wide_body(
    zonal_wind,
    merid_wind,
    vertical_wind,
    pressure,
    zonal_coef,
    merid_coef,
    level_coef,
    sound_coef,
    cutoff,
    filter_mask,
):
    lat_rows = pressure.shape[1]
    start = lax.axis_index("lat") * lat_rows
    own_flags = lax.dynamic_slice_in_dim(filter_mask, start, lat_rows) > 0
    own_limits = lax.dynamic_slice_in_dim(cutoff, start, lat_rows).astype(jnp.float32)
    forward, inverse, wave_row = dft_tables(pressure.shape[2] * lax.axis_size("lon"))
    zonal_rows = zonal_coef[None, :, None]
    merid_rows = merid_coef[None, :, None]
    for step in range(SUBSTEPS):
        padded = extended(pressure, (("lat", 1), ("lon", 2)), 1)
        padded = rim_fix(padded, 1)
        zonal_step = -zonal_rows * (padded[:, 1:-1, 2:] - padded[:, 1:-1, :-2])
        merid_step = -merid_rows * (padded[:, 2:, 1:-1] - padded[:, :-2, 1:-1])
        increments = jnp.stack([zonal_step, merid_step])
        damped = filtered_increments(increments, own_flags, own_limits, forward, inverse, wave_row)
        winds = jnp.stack([zonal_wind, merid_wind]) + damped
        wind_pad = extended(winds, (("lat", 2), ("lon", 3)), 1)
        wind_pad = rim_fix(wind_pad, 2)
        diverge = zonal_rows * (wind_pad[0, :, 1:-1, 2:] - wind_pad[0, :, 1:-1, :-2])
        diverge = diverge + merid_rows * (wind_pad[1, :, 2:, 1:-1] - wind_pad[1, :, :-2, 1:-1])
        pstar = pressure - sound_coef * diverge
        vertical_wind, pressure = column_solve(vertical_wind, pstar, level_coef, sound_coef)
        zonal_wind = winds[0]
        merid_wind = winds[1]
    return (zonal_wind, merid_wind, vertical_wind, pressure)


LANE = 128
TILE = 2 * LANE


def circle_tables(length):
    blocks = length // LANE
    half = blocks // 2
    m = np.arange(LANE, dtype=np.float64)[:, None]
    tables = np.zeros((half, TILE, TILE))
    waves = np.zeros((half, TILE))
    c = np.arange(LANE)[None, :]
    low = np.where(c <= LANE // 2, np.cos(2 * np.pi * m * c / LANE), np.sin(2 * np.pi * m * (c - LANE // 2) / LANE))
    low = low * np.where((c == 0) | (c == LANE // 2), np.sqrt(1.0 / LANE), np.sqrt(2.0 / LANE))
    k2 = np.arange(LANE // 2)[None, :]
    angle = 2 * np.pi * m * (half + blocks * k2) / length
    mid = np.concatenate([np.cos(angle), np.sin(angle)], axis=1) * np.sqrt(2.0 / LANE)
    tables[0, :LANE, :LANE] = low
    tables[0, LANE:, LANE:] = mid
    waves[0, :LANE] = blocks * np.where(c[0] <= LANE // 2, c[0], c[0] - LANE // 2)
    waves[0, LANE:] = np.tile(half + blocks * k2[0], 2)
    for k1 in range(1, half):
        k = k1 + blocks * c
        angle = 2 * np.pi * ((m * k) % length) / length
        cos, sin = np.cos(angle) / np.sqrt(LANE), np.sin(angle) / np.sqrt(LANE)
        tables[k1] = np.block([[cos, -sin], [sin, cos]])
        waves[k1] = np.tile(np.minimum(k[0], length - k[0]), 2)
    high = tables.astype(ml_dtypes.bfloat16)
    rest = (tables - high.astype(np.float64)).astype(ml_dtypes.bfloat16)
    scale = np.full((half, TILE), 2.0 / blocks)
    scale[0] = 1.0 / blocks
    rows = np.zeros((half, 8, TILE), np.float32)
    rows[:, 0] = waves
    rows[:, 1] = 4.0 * np.sin(2 * np.pi * waves / length) ** 2
    rows[:, 2] = scale
    return high, rest, rows


def split_parts(value):
    high = value.astype(jnp.bfloat16)
    rest = (value - high.astype(jnp.float32)).astype(jnp.bfloat16)
    return high, rest


def three_products(value, high_table, rest_table, transposed):
    high, rest = split_parts(value)
    dims = (((1,), (1 if transposed else 0,)), ((), ()))
    rows = value.shape[0]
    both = lax.dot_general(jnp.concatenate([high, rest], axis=0), high_table, dims, preferred_element_type=jnp.float32)
    corr = lax.dot_general(high, rest_table, dims, preferred_element_type=jnp.float32)
    return both[:rows] + (both[rows:] + corr)


def weighted(terms):
    total = None
    for coef, value in terms:
        if abs(coef) < 1e-12:
            continue
        if abs(abs(coef) - 1.0) < 1e-12:
            term = value
        else:
            term = abs(coef) * value
        if total is None:
            total = term if coef > 0 else -term
        else:
            total = total + term if coef > 0 else total - term
    return total


def coarse_forward(xs):
    count = len(xs)
    half = count // 2
    even = {b: xs[b] + xs[count - b] for b in range(1, half)}
    odd = {b: xs[b] - xs[count - b] for b in range(1, half)}
    real, imag = [], {}
    for k in range(half + 1):
        ends = xs[0] + xs[half] if k % 2 == 0 else xs[0] - xs[half]
        real.append(weighted([(1.0, ends)] + [(math.cos(2 * math.pi * b * k / count), even[b]) for b in range(1, half)]))
    for k in range(1, half):
        imag[k] = weighted([(-math.sin(2 * math.pi * b * k / count), odd[b]) for b in range(1, half)])
    pairs = [(real[0], real[half])] + [(real[k], imag[k]) for k in range(1, half)]
    return pairs


def coarse_inverse(pairs):
    half = len(pairs)
    count = 2 * half
    first, last = pairs[0]
    xs = [None] * count
    for b in range(half + 1):
        ends = first + last if b % 2 == 0 else first - last
        cos_part = weighted([(1.0, ends)] + [(math.cos(2 * math.pi * b * k / count), pairs[k][0]) for k in range(1, half)])
        if b in (0, half):
            xs[b] = cos_part
        else:
            sin_part = weighted([(-math.sin(2 * math.pi * b * k / count), pairs[k][1]) for k in range(1, half)])
            xs[b] = cos_part + sin_part
            xs[count - b] = cos_part - sin_part
    return xs


def to_spectrum(x_ref, high_ref, rest_ref, work_ref, spec_ref, units, per_band, accumulate):
    split = x_ref.shape[2] // LANE

    def one_unit(unit, carry):
        xs = [
            x_ref[d * units + unit, :, h * LANE:(h + 1) * LANE]
            for d in range(per_band)
            for h in range(split)
        ]
        for t, (left, right) in enumerate(coarse_forward(xs)):
            work_ref[t, unit, :, :LANE] = left
            work_ref[t, unit, :, LANE:] = right
        return carry

    lax.fori_loop(0, units, one_unit, 0)
    for t in range(high_ref.shape[0]):
        value = three_products(joined(work_ref[t]), high_ref[t], rest_ref[t], False)
        if accumulate:
            value = value + spec_ref[t]
        spec_ref[t] = value


def joined(value):
    return value.reshape((value.shape[0] * value.shape[1], value.shape[2]))


def circle_blocks(work_ref, band):
    pairs = [(work_ref[t, band, :, :LANE], work_ref[t, band, :, LANE:]) for t in range(work_ref.shape[0])]
    return coarse_inverse(pairs)


def put_blocks(out_ref, xs, unit, units):
    split = out_ref.shape[2] // LANE
    for b, value in enumerate(xs):
        out_ref[(b // split) * units + unit, :, (b % split) * LANE:(b % split + 1) * LANE] = value


def circle_diff(xs):
    count = len(xs)
    lane = lax.broadcasted_iota(jnp.int32, xs[0].shape, 1)
    ahead = [pltpu.roll(x, LANE - 1, 1) for x in xs]
    behind = [pltpu.roll(x, 1, 1) for x in xs]
    out = []
    for b in range(count):
        nxt = jnp.where(lane == LANE - 1, ahead[(b + 1) % count], ahead[b])
        prv = jnp.where(lane == 0, behind[(b - 1) % count], behind[b])
        out.append(nxt - prv)
    return out


def filter_values(limit, wave, scale):
    quotient = limit / jnp.maximum(wave, 1.0)
    return jnp.where(wave > limit, quotient * quotient, 1.0) * scale


def spectral_terms(spec_ref, t, units, rows_ref, own_ref, near_ref):
    rows = own_ref.shape[1]
    wave, sines, scale = rows_ref[t, 0:1, :], rows_ref[t, 1:2, :], rows_ref[t, 2:3, :]
    zonal = own_ref[0, :, 0:1]
    merid = own_ref[1, :, 0:1]
    factor = filter_values(own_ref[2, :, 0:1], wave, scale)
    south = near_ref[0, 1, rows - 1:rows, 0:1] * filter_values(near_ref[0, 2, rows - 1:rows, 0:1], wave, scale)
    north = near_ref[1, 1, 0:1, 0:1] * filter_values(near_ref[1, 2, 0:1, 0:1], wave, scale)
    row = lax.broadcasted_iota(jnp.int32, (rows, TILE), 0)
    around = merid * factor
    along = (zonal * zonal) * sines * factor
    smooth, v_parts, d_parts = [], [], []
    for l in range(units):
        own = spec_ref[t, l * rows:(l + 1) * rows, :]
        below = spec_ref[t, units * rows + 2 * l:units * rows + 2 * l + 2, :]
        above = spec_ref[t, (units + 1) * rows + 2 * l:(units + 1) * rows + 2 * l + 2, :]
        upper = jnp.where(row == rows - 1, above[0:1], pltpu.roll(own, rows - 1, 0))
        lower = jnp.where(row == 0, below[1:2], pltpu.roll(own, 1, 0))
        mid = -around * (upper - lower)
        v_south = -south * (own[0:1] - below[0:1])
        v_north = -north * (above[1:2] - own[rows - 1:rows])
        upper = jnp.where(row == rows - 1, v_north, pltpu.roll(mid, rows - 1, 0))
        lower = jnp.where(row == 0, v_south, pltpu.roll(mid, 1, 0))
        smooth.append(factor * own)
        v_parts.append(mid)
        d_parts.append(along * own + merid * (upper - lower))
    return smooth, v_parts, d_parts


def factor_columns(a_ref, s_ref, ratio_ref, inv_ref):
    levels = s_ref.shape[0]
    prev = jnp.zeros(s_ref.shape[1:], jnp.float32)
    for level in range(levels):
        alpha = a_ref[level]
        below = alpha * s_ref[level]
        above = alpha * s_ref[level + 1] if level + 1 < levels else jnp.zeros_like(below)
        inv = 1.0 / (1.0 + below + above + below * prev)
        prev = -above * inv
        ratio_ref[level] = prev
        inv_ref[level] = inv


def solve_columns(a_ref, s_ref, w_ref, p_ref, base_ref, d_ref, ratio_ref, inv_ref, w_out, p_out):
    levels = s_ref.shape[0]

    def star(level):
        return p_ref[level] - s_ref[level] * (base_ref[level] + d_ref[level])

    here = star(0)
    prev = jnp.zeros_like(here)
    for level in range(levels):
        alpha = a_ref[level]
        p_out[level] = here
        if level + 1 < levels:
            nxt = star(level + 1)
            rhs = w_ref[level] - alpha * (nxt - here)
        else:
            nxt = here
            rhs = w_ref[level] + alpha * here
        prev = (rhs + alpha * s_ref[level] * prev) * inv_ref[level]
        w_out[level] = prev
        here = nxt
    upper = w_out[levels - 1]
    for level in range(levels - 1, 0, -1):
        lower = w_out[level - 1] - ratio_ref[level - 1] * upper
        w_out[level - 1] = lower
        p_out[level] = p_out[level] - s_ref[level] * (upper - lower)
        upper = lower
    p_out[0] = p_out[0] - s_ref[0] * upper


def base_divergence(u_ref, v_ref, own_ref, west_ref, east_ref, south_ref, north_ref, base_ref, is_first, is_last):
    zonal = own_ref[0][:, 0:1]
    merid = own_ref[1][:, 0:1]
    rows, width = u_ref.shape[1:]
    lane = lax.broadcasted_iota(jnp.int32, (rows, width), 1)
    row = lax.broadcasted_iota(jnp.int32, (rows, width), 0)
    keep_south = jnp.where(is_first, 0.0, 1.0)
    keep_north = jnp.where(is_last, 0.0, 1.0)
    west = west_ref[...]
    east = east_ref[...]
    for level in range(u_ref.shape[0]):
        u = u_ref[level]
        v = v_ref[level]
        ahead = jnp.where(lane == width - 1, east[:, level:level + 1], pltpu.roll(u, width - 1, 1))
        behind = jnp.where(lane == 0, west[:, level:level + 1], pltpu.roll(u, 1, 1))
        upper = jnp.where(row == rows - 1, keep_north * north_ref[level:level + 1, :], pltpu.roll(v, rows - 1, 0))
        lower = jnp.where(row == 0, keep_south * south_ref[level:level + 1, :], pltpu.roll(v, 1, 0))
        base_ref[level] = zonal * (ahead - behind) + merid * (upper - lower)


def pack_edges(u_ref, v_ref, first_col, last_col, first_row, last_row):
    rows, width = u_ref.shape[1:]
    lane = lax.broadcasted_iota(jnp.int32, (rows, LANE), 1)
    first = jnp.zeros((rows, LANE), jnp.float32)
    last = jnp.zeros((rows, LANE), jnp.float32)
    for level in range(u_ref.shape[0]):
        first = jnp.where(lane == level, u_ref[level, :, 0:1], first)
        last = jnp.where(lane == level, u_ref[level, :, width - 1:width], last)
        first_row[level:level + 1, :] = v_ref[level, 0:1, :]
        last_row[level:level + 1, :] = v_ref[level, rows - 1:rows, :]
    first_col[...] = first
    last_col[...] = last


def pack_halo(source, low, high, units):
    rows = source.shape[1]
    for g in range(low.shape[0]):
        for l in range(units):
            low[g, 2 * l:2 * l + 2, :] = source[g * units + l, 0:2, :]
            high[g, 2 * l:2 * l + 2, :] = source[g * units + l, rows - 2:rows, :]


def own_coefs(zc_ref, mc_ref, cutoff_ref, mask_ref, own_ref, first_lat, unfiltered):
    rows = own_ref.shape[1]
    row = lax.broadcasted_iota(jnp.int32, own_ref.shape[1:], 0)
    zonal = jnp.zeros(own_ref.shape[1:], jnp.float32)
    merid = jnp.zeros(own_ref.shape[1:], jnp.float32)
    limit = jnp.zeros(own_ref.shape[1:], jnp.int32)
    for r in range(rows):
        zonal = jnp.where(row == r, zc_ref[r], zonal)
        merid = jnp.where(row == r, mc_ref[r], merid)
        filtered = mask_ref[first_lat + r]
        bound = filtered * cutoff_ref[first_lat + r] + (1 - filtered) * unfiltered
        limit = jnp.where(row == r, bound, limit)
    own_ref[0] = zonal
    own_ref[1] = merid
    own_ref[2] = limit.astype(jnp.float32)


def fused_kernel(
    bands, per_band, a_ref, zc_ref, mc_ref, cutoff_ref, mask_ref, u_ref, v_ref, w_far, p_ref, s_far, high_far, rest_far, rows_ref,
    u_out, v_out, w_out, p_out,
    d1, d2, ur, vr, ds1, ds2, us, vs, w_mid, p_mid, base, ratio, inv,
    x1, x2, wide, work, qwork, vwork, spec, own_ref, near, cols_send, cols_recv, rows_send, rows_recv, low, high,
    send_sems, recv_sems, edge_send, edge_recv, halo_send, halo_recv,
    w_ref, s_ref, high_ref, rest_ref, load_sems,
):
    count = bands * per_band
    band_me = lax.axis_index("lat")
    lon_me = lax.axis_index("lon")
    me = band_me * per_band + lon_me
    half = high_ref.shape[0]
    lat_rows = u_ref.shape[1]
    units = u_ref.shape[0] // per_band
    spread = units + 2
    mesh_id = pl.DeviceIdType.MESH
    is_first = band_me == 0
    is_last = band_me == bands - 1

    loads = [
        pltpu.make_async_copy(far, here, load_sems.at[n])
        for n, (far, here) in enumerate(((high_far, high_ref), (rest_far, rest_ref), (s_far, s_ref), (w_far, w_ref)))
    ]
    for load in loads:
        load.start()
    barrier = pltpu.get_barrier_semaphore()

    def greet(i, carry):
        other = (me + i) % count
        pl.semaphore_signal(barrier, inc=1, device_id=(other // per_band, other % per_band), device_id_type=mesh_id)
        return carry

    lax.fori_loop(1, count, greet, 0)
    own_coefs(zc_ref, mc_ref, cutoff_ref, mask_ref, own_ref, band_me * lat_rows, half * TILE)
    pack_halo(p_ref, low.at[0], high.at[0], units)
    pack_edges(u_ref, v_ref, cols_send.at[0], cols_send.at[1], rows_send.at[0], rows_send.at[1])

    @pl.when(is_first)
    def _():
        near[0] = jnp.zeros(near.shape[1:], jnp.float32)
        for d in range(per_band):
            x1[d * spread + units] = jnp.zeros(x1.shape[1:], jnp.float32)
            x2[d * spread + units] = jnp.zeros(x2.shape[1:], jnp.float32)

    @pl.when(is_last)
    def _():
        near[1] = jnp.zeros(near.shape[1:], jnp.float32)
        for d in range(per_band):
            x1[d * spread + units + 1] = jnp.zeros(x1.shape[1:], jnp.float32)
            x2[d * spread + units + 1] = jnp.zeros(x2.shape[1:], jnp.float32)

    pl.semaphore_wait(barrier, count - 1)

    def scatter(source, target, sem, stride):
        def one(i, carry):
            g = (lon_me + i) % per_band
            pltpu.make_async_remote_copy(
                src_ref=source.at[pl.ds(g * units, units)], dst_ref=target.at[pl.ds(lon_me * stride, units)],
                send_sem=send_sems.at[sem], recv_sem=recv_sems.at[sem],
                device_id=(band_me, g), device_id_type=mesh_id,
            ).start()
            return carry

        lax.fori_loop(1, per_band, one, 0)
        for l in range(units):
            target[lon_me * stride + l] = source[lon_me * units + l]

    def gathered(target, sem):
        block = target.at[pl.ds(0, (per_band - 1) * units)]
        pltpu.make_async_copy(block, block, recv_sems.at[sem]).wait()

    def sent(source, sem):
        block = source.at[pl.ds(0, (per_band - 1) * units)]
        pltpu.make_async_copy(block, block, send_sems.at[sem]).wait()

    def spread_halo(target, phase):
        def one(source, slot, sem, other):
            def step(i, carry):
                g = (lon_me + i) % per_band
                pltpu.make_async_remote_copy(
                    src_ref=source.at[g], dst_ref=target.at[lon_me * spread + slot],
                    send_sem=halo_send.at[sem], recv_sem=halo_recv.at[sem],
                    device_id=(other, g), device_id_type=mesh_id,
                ).start()
                return carry

            lax.fori_loop(0, per_band, step, 0)

        @pl.when(jnp.logical_not(is_first))
        def _():
            one(low.at[phase], units + 1, 2 * phase, band_me - 1)

        @pl.when(jnp.logical_not(is_last))
        def _():
            one(high.at[phase], units, 2 * phase + 1, band_me + 1)

    def halo_wait(phase, sems, upward):
        block = low.at[phase]

        @pl.when(jnp.logical_not(is_first))
        def _():
            pltpu.make_async_copy(block, block, sems.at[2 * phase + (0 if upward else 1)]).wait()

        @pl.when(jnp.logical_not(is_last))
        def _():
            pltpu.make_async_copy(block, block, sems.at[2 * phase + (1 if upward else 0)]).wait()

    def coef_copy(step, side):
        return pltpu.make_async_remote_copy(
            src_ref=own_ref, dst_ref=near.at[side], send_sem=edge_send.at[4 + side], recv_sem=edge_recv.at[4 + side],
            device_id=((band_me + bands + step) % bands, lon_me), device_id_type=mesh_id,
        )

    @pl.when(jnp.logical_not(is_first))
    def _():
        coef_copy(-1, 1).start()

    @pl.when(jnp.logical_not(is_last))
    def _():
        coef_copy(1, 0).start()

    scatter(p_ref, x1, 0, spread)
    spread_halo(x1, 0)

    edge_copies = []
    for side, step in ((0, -1), (1, 1)):
        edge_copies.append(pltpu.make_async_remote_copy(
            src_ref=cols_send.at[side], dst_ref=cols_recv.at[side], send_sem=edge_send.at[side], recv_sem=edge_recv.at[side],
            device_id=(band_me, (lon_me + per_band + step) % per_band), device_id_type=mesh_id,
        ))
        edge_copies.append(pltpu.make_async_remote_copy(
            src_ref=rows_send.at[side], dst_ref=rows_recv.at[side], send_sem=edge_send.at[2 + side], recv_sem=edge_recv.at[2 + side],
            device_id=((band_me + bands + step) % bands, lon_me), device_id_type=mesh_id,
        ))
    for copy in edge_copies:
        copy.start()

    @pl.when(jnp.logical_not(is_first))
    def _():
        coef_copy(1, 0).wait_recv()

    @pl.when(jnp.logical_not(is_last))
    def _():
        coef_copy(-1, 1).wait_recv()

    for load in loads:
        load.wait()
    gathered(x1, 0)
    halo_wait(0, halo_recv, False)
    to_spectrum(x1, high_ref, rest_ref, wide, spec, spread, per_band, False)
    for t in range(half):
        _, _, d_parts = spectral_terms(spec, t, units, rows_ref, own_ref, near)
        d_part = jnp.concatenate(d_parts, axis=0)
        work[t] = three_products(d_part, high_ref[t], rest_ref[t], True).reshape(work.shape[1:])

    def first_back(unit, carry):
        put_blocks(ds1, circle_blocks(work, unit), unit, units)
        return carry

    lax.fori_loop(0, units, first_back, 0)
    scatter(ds1, d1, 1, units)

    factor_columns(a_ref, s_ref, ratio, inv)
    for copy in edge_copies:
        copy.wait_recv()
    base_divergence(
        u_ref, v_ref, own_ref, cols_recv.at[1], cols_recv.at[0], rows_recv.at[1], rows_recv.at[0], base,
        is_first, is_last,
    )
    gathered(d1, 1)
    solve_columns(a_ref, s_ref, w_ref, p_ref, base, d1, ratio, inv, w_mid, p_mid)
    scatter(p_mid, x2, 2, spread)
    pack_halo(p_mid, low.at[1], high.at[1], units)
    spread_halo(x2, 1)
    gathered(x2, 2)
    halo_wait(1, halo_recv, False)
    to_spectrum(x2, high_ref, rest_ref, wide, spec, spread, per_band, True)
    lats = units * lat_rows
    for t in range(half):
        smooth, v_parts, d_parts = spectral_terms(spec, t, units, rows_ref, own_ref, near)
        value = three_products(jnp.concatenate(d_parts + smooth + v_parts, axis=0), high_ref[t], rest_ref[t], True)
        work[t] = value[:lats].reshape(work.shape[1:])
        qwork[t] = value[lats:2 * lats].reshape(work.shape[1:])
        vwork[t] = value[2 * lats:].reshape(work.shape[1:])

    def second_back(band, carry):
        put_blocks(ds2, circle_blocks(work, band), band, units)
        return carry

    lax.fori_loop(0, units, second_back, 0)
    scatter(ds2, d2, 3, units)

    def winds_back(band, carry):
        put_blocks(vs, circle_blocks(vwork, band), band, units)
        zonal = own_ref[0, :, 0:1]
        moved = circle_diff(circle_blocks(qwork, band))
        put_blocks(us, [-zonal * x for x in moved], band, units)
        return carry

    lax.fori_loop(0, units, winds_back, 0)
    scatter(us, ur, 4, units)
    scatter(vs, vr, 5, units)
    gathered(d2, 3)
    solve_columns(a_ref, s_ref, w_mid, p_mid, base, d2, ratio, inv, w_out, p_out)
    gathered(ur, 4)
    u_out[...] = u_ref[...] + ur[...]
    gathered(vr, 5)
    v_out[...] = v_ref[...] + vr[...]
    for source, sem in ((p_ref, 0), (ds1, 1), (p_mid, 2), (ds2, 3), (us, 4), (vs, 5)):
        sent(source, sem)
    for phase in range(2):
        halo_wait(phase, halo_send, True)
    for copy in edge_copies:
        copy.wait_send()

    @pl.when(jnp.logical_not(is_first))
    def _():
        coef_copy(-1, 1).wait_send()

    @pl.when(jnp.logical_not(is_last))
    def _():
        coef_copy(1, 0).wait_send()


def deliver_kernel(*refs):
    count = (len(refs) - 1) // 2
    sems = refs[-1]
    copies = [pltpu.make_async_copy(refs[n], refs[count + n], sems.at[n]) for n in range(count)]
    for copy in copies:
        copy.start()
    for copy in copies:
        copy.wait()


def deliver(arrays):
    count = len(arrays)
    return pl.pallas_call(
        deliver_kernel,
        out_shape=tuple(jax.ShapeDtypeStruct(a.shape, a.dtype) for a in arrays),
        in_specs=[pl.BlockSpec(memory_space=pltpu.VMEM)] * count,
        out_specs=(pl.BlockSpec(memory_space=pl.ANY),) * count,
        scratch_shapes=[pltpu.SemaphoreType.DMA((count,))],
        compiler_params=pltpu.CompilerParams(vmem_limit_bytes=FINISH_VMEM),
    )(*arrays)


def level_body(
    tables,
    zonal_wind,
    merid_wind,
    vertical_wind,
    pressure,
    zonal_coef,
    merid_coef,
    level_coef,
    sound_coef,
    cutoff,
    filter_mask,
):
    high, rest, rows = (jnp.asarray(t) for t in tables)
    half = high.shape[0]
    bands = lax.axis_size("lat")
    per_band = lax.axis_size("lon")
    levels, lat_rows, width = pressure.shape
    units = levels // per_band
    spread = units + 2
    vmem = pl.BlockSpec(memory_space=pltpu.VMEM)
    smem = pl.BlockSpec(memory_space=pltpu.SMEM)
    far = pl.BlockSpec(memory_space=pl.ANY)
    block = jax.ShapeDtypeStruct(pressure.shape, jnp.float32)

    def scratch(*shape):
        return pltpu.VMEM(shape, jnp.float32)

    field = scratch(*pressure.shape)
    arrivals = scratch(per_band * spread, lat_rows, width)
    waves = scratch(half, units, lat_rows, TILE)
    dma = pltpu.SemaphoreType.DMA
    results = pl.pallas_call(
        functools.partial(fused_kernel, bands, per_band),
        out_shape=(pltpu.VMEM(pressure.shape, jnp.float32),) * 4,
        in_specs=[smem] * 5 + [vmem] * 2 + [far, vmem, far, far, far, vmem],
        out_specs=(vmem,) * 4,
        scratch_shapes=[field] * 13 + [arrivals] * 2 + [scratch(half, spread, lat_rows, TILE)] + [waves] * 3 + [
            scratch(half, spread * lat_rows, TILE),
            scratch(3, lat_rows, LANE), scratch(2, 3, lat_rows, LANE),
            scratch(2, lat_rows, LANE), scratch(2, lat_rows, LANE),
            scratch(2, levels, width), scratch(2, levels, width),
            scratch(2, per_band, lat_rows, width), scratch(2, per_band, lat_rows, width),
            dma((6,)), dma((6,)), dma((6,)), dma((6,)), dma((4,)), dma((4,)),
            field, field, pltpu.VMEM(high.shape, high.dtype), pltpu.VMEM(rest.shape, rest.dtype), dma((4,)),
        ],
        compiler_params=pltpu.CompilerParams(collective_id=0, has_side_effects=True, vmem_limit_bytes=FUSED_VMEM),
    )(*[pltpu.with_memory_space_constraint(x, pltpu.HBM) for x in (
        level_coef, zonal_coef, merid_coef, cutoff, filter_mask,
        zonal_wind, merid_wind, vertical_wind, pressure, sound_coef, high, rest, rows,
    )])
    return deliver(results)


def body(tables, *arrays):
    pressure = arrays[3]
    per_band = lax.axis_size("lon")
    levels, lat_rows, width = pressure.shape
    fits = lat_rows == 8 and levels == 4 * per_band and levels <= LANE and width % LANE == 0
    if fits:
        return level_body(tables, *arrays)
    return wide_body(*arrays)


def solution(mesh):
    in_specs = (
        P(None, "lat", "lon"),
        P(None, "lat", "lon"),
        P(None, "lat", "lon"),
        P(None, "lat", "lon"),
        P("lat"),
        P("lat"),
        P(),
        P(None, "lat", "lon"),
        P(),
        P(),
    )
    out_specs = (
        P(None, "lat", "lon"),
        P(None, "lat", "lon"),
        P(None, "lat", "lon"),
        P(None, "lat", "lon"),
    )

    def whole(*arrays):
        tables = circle_tables(arrays[0].shape[2])
        step = jax.shard_map(functools.partial(body, tables), mesh=mesh, in_specs=in_specs, out_specs=out_specs, check_vma=False)
        return step(*arrays)

    return whole
```

```python
import functools
import math

import ml_dtypes
import numpy as np
import jax
import jax.numpy as jnp
from jax import lax
from jax.experimental import pallas as pl
from jax.experimental.pallas import tpu as pltpu
from jax.sharding import PartitionSpec as P

SUBSTEPS = 2
FUSED_VMEM = 40 * 2 ** 20
FINISH_VMEM = 4 * 2 ** 20


def extended(block, sides, width):
    for axis, dim in sides:
        count = lax.axis_size(axis)
        forward = [(i, i + 1) for i in range(count - 1)]
        forward.append((count - 1, 0))
        backward = [(target, source) for source, target in forward]
        low = lax.ppermute(
            lax.slice_in_dim(block, block.shape[dim] - width, None, axis=dim), axis, forward
        )
        high = lax.ppermute(lax.slice_in_dim(block, 0, width, axis=dim), axis, backward)
        block = jnp.concatenate([low, block, high], axis=dim)
    return block


def rim_fix(padded, lat_dim):
    band_index = lax.axis_index("lat")
    bands = lax.axis_size("lat")
    extent = padded.shape[lat_dim]
    position = lax.broadcasted_iota(jnp.int32, padded.shape, lat_dim)
    first_edge = jnp.logical_and(position == 0, band_index == 0)
    final_edge = jnp.logical_and(position == extent - 1, band_index == bands - 1)
    return jnp.where(jnp.logical_or(first_edge, final_edge), 0.0, padded)


def dft_tables(length):
    half_len = length // 2
    sample = lax.broadcasted_iota(jnp.int32, (length, length), 0)
    column = lax.broadcasted_iota(jnp.int32, (length, length), 1)
    is_cosine = column <= half_len
    wavenum = jnp.where(is_cosine, column, column - half_len)
    phase = sample * wavenum % length
    angle = 2.0 * math.pi / length * phase.astype(jnp.float32)
    forward = jnp.where(is_cosine, jnp.cos(angle), jnp.sin(angle))
    single = jnp.logical_and(is_cosine, jnp.logical_or(wavenum == 0, wavenum == half_len))
    weight = jnp.where(single, 1.0, 2.0) / length
    inverse = jnp.transpose(forward * weight)
    wave_row = wavenum[0].astype(jnp.float32)
    return (forward, inverse, wave_row)


def damping(wave_row, limits):
    bound_col = limits[:, None]
    ratio = bound_col / jnp.maximum(wave_row[None, :], 1.0)
    return jnp.where(wave_row[None, :] > bound_col, ratio * ratio, 1.0)


def transform_band(block, limits, forward, inverse, wave_row):
    circles = lax.all_to_all(block, "lon", split_axis=1, concat_axis=3, tiled=True)
    spectra = jnp.einsum("vetj,jc->vetc", circles, forward, precision=lax.Precision.HIGHEST)
    scaled = spectra * damping(wave_row, limits)
    damped = jnp.einsum("vetc,cj->vetj", scaled, inverse, precision=lax.Precision.HIGHEST)
    return lax.all_to_all(damped, "lon", split_axis=3, concat_axis=1, tiled=True)


def filtered_increments(increments, own_flags, own_limits, forward, inverse, wave_row):
    flag_cols = own_flags[:, None]
    damped = transform_band(increments, own_limits, forward, inverse, wave_row)
    return jnp.where(flag_cols, damped, increments)


def column_solve(vertical_wind, pstar, level_coef, sound_coef):
    levels = vertical_wind.shape[0]
    zero_slab = jnp.zeros_like(vertical_wind[0])
    ratios = []
    values = []
    prev_ratio = zero_slab
    prev_value = zero_slab
    for level in range(levels):
        alpha = level_coef[level]
        below = alpha * sound_coef[level]
        if level + 1 < levels:
            above = alpha * sound_coef[level + 1]
            rhs = vertical_wind[level] - alpha * (pstar[level + 1] - pstar[level])
        else:
            above = zero_slab
            rhs = vertical_wind[level] + alpha * pstar[level]
        pivot = 1.0 + below + above + below * prev_ratio
        prev_ratio = -above / pivot
        prev_value = (rhs + below * prev_value) / pivot
        ratios.append(prev_ratio)
        values.append(prev_value)
    solved = [zero_slab] * levels
    upper_value = values[levels - 1]
    solved[levels - 1] = upper_value
    for level in range(levels - 2, -1, -1):
        upper_value = values[level] - ratios[level] * upper_value
        solved[level] = upper_value
    new_wind = jnp.stack(solved)
    wind_below = jnp.concatenate([zero_slab[None], new_wind[:-1]], axis=0)
    new_pressure = pstar - sound_coef * (new_wind - wind_below)
    return (new_wind, new_pressure)


def wide_body(
    zonal_wind,
    merid_wind,
    vertical_wind,
    pressure,
    zonal_coef,
    merid_coef,
    level_coef,
    sound_coef,
    cutoff,
    filter_mask,
):
    lat_rows = pressure.shape[1]
    start = lax.axis_index("lat") * lat_rows
    own_flags = lax.dynamic_slice_in_dim(filter_mask, start, lat_rows) > 0
    own_limits = lax.dynamic_slice_in_dim(cutoff, start, lat_rows).astype(jnp.float32)
    forward, inverse, wave_row = dft_tables(pressure.shape[2] * lax.axis_size("lon"))
    zonal_rows = zonal_coef[None, :, None]
    merid_rows = merid_coef[None, :, None]
    for step in range(SUBSTEPS):
        padded = extended(pressure, (("lat", 1), ("lon", 2)), 1)
        padded = rim_fix(padded, 1)
        zonal_step = -zonal_rows * (padded[:, 1:-1, 2:] - padded[:, 1:-1, :-2])
        merid_step = -merid_rows * (padded[:, 2:, 1:-1] - padded[:, :-2, 1:-1])
        increments = jnp.stack([zonal_step, merid_step])
        damped = filtered_increments(increments, own_flags, own_limits, forward, inverse, wave_row)
        winds = jnp.stack([zonal_wind, merid_wind]) + damped
        wind_pad = extended(winds, (("lat", 2), ("lon", 3)), 1)
        wind_pad = rim_fix(wind_pad, 2)
        diverge = zonal_rows * (wind_pad[0, :, 1:-1, 2:] - wind_pad[0, :, 1:-1, :-2])
        diverge = diverge + merid_rows * (wind_pad[1, :, 2:, 1:-1] - wind_pad[1, :, :-2, 1:-1])
        pstar = pressure - sound_coef * diverge
        vertical_wind, pressure = column_solve(vertical_wind, pstar, level_coef, sound_coef)
        zonal_wind = winds[0]
        merid_wind = winds[1]
    return (zonal_wind, merid_wind, vertical_wind, pressure)


LANE = 128
TILE = 2 * LANE


def circle_tables(length):
    blocks = length // LANE
    half = blocks // 2
    m = np.arange(LANE, dtype=np.float64)[:, None]
    c = np.arange(LANE)[None, :]
    angle = 2 * np.pi * ((m * c) % LANE) / LANE
    cos, sin = np.cos(angle) / np.sqrt(LANE), np.sin(angle) / np.sqrt(LANE)
    table = np.block([[cos, -sin], [sin, cos]])
    high = table.astype(ml_dtypes.bfloat16)
    rest = (table - high.astype(np.float64)).astype(ml_dtypes.bfloat16)
    rows = np.zeros((half + 1, 8, TILE), np.float32)
    for k1 in range(half + 1):
        k = k1 + blocks * c[0]
        waves = np.tile(np.minimum(k, length - k), 2)
        scale = (1.0 if k1 in (0, half) else 2.0) / blocks
        turn = 2 * np.pi * m[:, 0] * k1 / length
        rows[k1, 0] = waves
        rows[k1, 1] = 4.0 * np.sin(2 * np.pi * waves / length) ** 2
        rows[k1, 2] = np.where(np.arange(TILE) < LANE, scale, -scale)
        rows[k1, 3] = np.concatenate([np.cos(turn), np.sin(turn)])
    return np.stack([high, rest]), rows


def split_parts(value):
    high = value.astype(jnp.bfloat16)
    rest = (value - high.astype(jnp.float32)).astype(jnp.bfloat16)
    return high, rest


def three_products(value, table_ref):
    high, rest = split_parts(value)
    dims = (((1,), (0,)), ((), ()))
    rows = value.shape[0]
    table = table_ref[0]
    both = lax.dot_general(jnp.concatenate([high, rest], axis=0), table, dims, preferred_element_type=jnp.float32)
    corr = lax.dot_general(high, table_ref[1], dims, preferred_element_type=jnp.float32)
    return both[:rows] + (both[rows:] + corr)


def weighted(terms):
    total = None
    for coef, value in terms:
        if abs(coef) < 1e-12:
            continue
        if abs(abs(coef) - 1.0) < 1e-12:
            term = value
        else:
            term = abs(coef) * value
        if total is None:
            total = term if coef > 0 else -term
        else:
            total = total + term if coef > 0 else total - term
    return total


def coarse_forward(xs):
    count = len(xs)
    half = count // 2
    even = {b: xs[b] + xs[count - b] for b in range(1, half)}
    odd = {b: xs[b] - xs[count - b] for b in range(1, half)}
    real, imag = [], {}
    for k in range(half + 1):
        ends = xs[0] + xs[half] if k % 2 == 0 else xs[0] - xs[half]
        real.append(weighted([(1.0, ends)] + [(math.cos(2 * math.pi * b * k / count), even[b]) for b in range(1, half)]))
    for k in range(1, half):
        imag[k] = weighted([(-math.sin(2 * math.pi * b * k / count), odd[b]) for b in range(1, half)])
    pairs = [(real[0], real[half])] + [(real[k], imag[k]) for k in range(1, half)]
    return pairs


def coarse_inverse(pairs):
    half = len(pairs)
    count = 2 * half
    first, last = pairs[0]
    xs = [None] * count
    for b in range(half + 1):
        ends = first + last if b % 2 == 0 else first - last
        cos_part = weighted([(1.0, ends)] + [(math.cos(2 * math.pi * b * k / count), pairs[k][0]) for k in range(1, half)])
        if b in (0, half):
            xs[b] = cos_part
        else:
            sin_part = weighted([(-math.sin(2 * math.pi * b * k / count), pairs[k][1]) for k in range(1, half)])
            xs[b] = cos_part + sin_part
            xs[count - b] = cos_part - sin_part
    return xs


def whole_tiles(count):
    return -(-count // 16) * 16


def forward_fill(xs, rows_ref, work_ref, start):
    pairs = coarse_forward(xs)
    half = len(pairs)
    first, last = pairs[0]
    for t in range(half + 1):
        cos, sin = rows_ref[t, 3:4, :LANE], rows_ref[t, 3:4, LANE:]
        if t == 0:
            left, right = first, jnp.zeros_like(first)
        elif t == half:
            left, right = last * cos, -(last * sin)
        else:
            real, imag = pairs[t]
            left, right = real * cos + imag * sin, imag * cos - real * sin
        work_ref[start + 8 * t:start + 8 * t + 8, :LANE] = left
        work_ref[start + 8 * t:start + 8 * t + 8, LANE:] = right


def inverse_blocks(back_ref, rows_ref, start):
    half = rows_ref.shape[0] - 1
    pairs = []
    ends = []
    for t in range(half + 1):
        left = back_ref[start + 8 * t:start + 8 * t + 8, :LANE]
        right = back_ref[start + 8 * t:start + 8 * t + 8, LANE:]
        cos, sin = rows_ref[t, 3:4, :LANE], rows_ref[t, 3:4, LANE:]
        if t == 0:
            ends.append(left)
        elif t == half:
            ends.append(left * cos + right * sin)
        else:
            pairs.append((left * cos + right * sin, left * sin - right * cos))
    return coarse_inverse([tuple(ends)] + pairs)


def put_blocks(out_ref, xs, unit, units):
    split = out_ref.shape[2] // LANE
    for b, value in enumerate(xs):
        out_ref[(b // split) * units + unit, :, (b % split) * LANE:(b % split + 1) * LANE] = value


def circle_diff(xs):
    count = len(xs)
    lane = lax.broadcasted_iota(jnp.int32, xs[0].shape, 1)
    ahead = [pltpu.roll(x, LANE - 1, 1) for x in xs]
    behind = [pltpu.roll(x, 1, 1) for x in xs]
    out = []
    for b in range(count):
        nxt = jnp.where(lane == LANE - 1, ahead[(b + 1) % count], ahead[b])
        prv = jnp.where(lane == 0, behind[(b - 1) % count], behind[b])
        out.append(nxt - prv)
    return out


def border_tiles(edge_ref, xs, unit):
    count = len(xs)
    split = count // edge_ref.shape[0]
    lane = lax.broadcasted_iota(jnp.int32, xs[0].shape, 1)
    turned = [pltpu.roll(x, 2 * unit + 1, 1) for x in xs]
    for d in range(edge_ref.shape[0]):
        west, east = turned[(d * split - 1) % count], turned[(d * split + split) % count]
        kept = edge_ref[d] if unit else jnp.zeros_like(west)
        edge_ref[d] = jnp.where(lane == 2 * unit, west, jnp.where(lane == 2 * unit + 1, east, kept))


def filter_values(limit, wave, scale):
    quotient = limit / jnp.maximum(wave, 1.0)
    return jnp.where(wave > limit, quotient * quotient, 1.0) * scale


def filter_terms(rows_ref, own_ref, near_ref, filt_ref, side_ref):
    rows = own_ref.shape[1]
    zonal, merid, limit = own_ref[0, :, 0:1], own_ref[1, :, 0:1], own_ref[2, :, 0:1]
    for t in range(rows_ref.shape[0]):
        wave, sines, scale = rows_ref[t, 0:1, :], rows_ref[t, 1:2, :], rows_ref[t, 2:3, :]
        factor = filter_values(limit, wave, scale)
        filt_ref[t, 0] = factor
        filt_ref[t, 1] = merid * factor
        filt_ref[t, 2] = (zonal * zonal) * sines * factor
        south = near_ref[0, 1, rows - 1:rows, 0:1] * filter_values(near_ref[0, 2, rows - 1:rows, 0:1], wave, scale)
        north = near_ref[1, 1, 0:1, 0:1] * filter_values(near_ref[1, 2, 0:1, 0:1], wave, scale)
        side_ref[t, 0:1, :] = south
        side_ref[t, 1:2, :] = north


def merid_terms(spec_ref, unit, t, filt_ref, side_ref):
    tile = spec_ref.shape[1] // filt_ref.shape[0]
    units = spec_ref.shape[0] - 2
    own = spec_ref[unit, tile * t:tile * t + tile, :]
    row = lax.broadcasted_iota(jnp.int32, own.shape, 0)
    at = tile * t + 2 * unit
    below_far, below = spec_ref[units, at:at + 1, :], spec_ref[units, at + 1:at + 2, :]
    above, above_far = spec_ref[units + 1, at:at + 1, :], spec_ref[units + 1, at + 1:at + 2, :]
    upper = jnp.where(row == tile - 1, above, pltpu.roll(own, tile - 1, 0))
    lower = jnp.where(row == 0, below, pltpu.roll(own, 1, 0))
    mid = -filt_ref[t, 1] * (upper - lower)
    v_south = -side_ref[t, 0:1, :] * (own[0:1] - below_far)
    v_north = -side_ref[t, 1:2, :] * (above_far - own[tile - 1:tile])
    return own, row, mid, v_south, v_north


def factor_columns(a_ref, s_ref, ratio_ref, inv_ref):
    levels = s_ref.shape[0]
    prev = jnp.zeros(s_ref.shape[1:], jnp.float32)
    for level in range(levels):
        alpha = a_ref[level]
        below = alpha * s_ref[level]
        above = alpha * s_ref[level + 1] if level + 1 < levels else jnp.zeros_like(below)
        inv = 1.0 / (1.0 + below + above + below * prev)
        prev = -above * inv
        ratio_ref[level] = prev
        inv_ref[level] = inv


def solve_columns(a_ref, s_ref, w_ref, p_ref, parts, ratio_ref, inv_ref, w_out, p_out):
    levels = s_ref.shape[0]

    def star(level):
        total = parts[0][level]
        for part in parts[1:]:
            total = total + part[level]
        return p_ref[level] - s_ref[level] * total

    here = star(0)
    prev = jnp.zeros_like(here)
    for level in range(levels):
        alpha = a_ref[level]
        p_out[level] = here
        if level + 1 < levels:
            nxt = star(level + 1)
            rhs = w_ref[level] - alpha * (nxt - here)
        else:
            nxt = here
            rhs = w_ref[level] + alpha * here
        prev = (rhs + alpha * s_ref[level] * prev) * inv_ref[level]
        w_out[level] = prev
        here = nxt
    upper = w_out[levels - 1]
    for level in range(levels - 1, 0, -1):
        lower = w_out[level - 1] - ratio_ref[level - 1] * upper
        w_out[level - 1] = lower
        p_out[level] = p_out[level] - s_ref[level] * (upper - lower)
        upper = lower
    p_out[0] = p_out[0] - s_ref[0] * upper


def divergence(u, v, zonal, merid, west, east, south, north):
    rows, width = u.shape
    lane = lax.broadcasted_iota(jnp.int32, (rows, width), 1)
    row = lax.broadcasted_iota(jnp.int32, (rows, width), 0)
    ahead = jnp.where(lane == width - 1, east, pltpu.roll(u, width - 1, 1))
    behind = jnp.where(lane == 0, west, pltpu.roll(u, 1, 1))
    upper = jnp.where(row == rows - 1, north, pltpu.roll(v, rows - 1, 0))
    lower = jnp.where(row == 0, south, pltpu.roll(v, 1, 0))
    return zonal * (ahead - behind) + merid * (upper - lower)


def base_divergence(u_ref, v_ref, own_ref, west_ref, east_ref, south_ref, north_ref, base_ref, is_first, is_last):
    zonal, merid = own_ref[0, :, 0:1], own_ref[1, :, 0:1]
    keep_south = jnp.where(is_first, 0.0, 1.0)
    keep_north = jnp.where(is_last, 0.0, 1.0)
    west = west_ref[...]
    east = east_ref[...]
    for level in range(u_ref.shape[0]):
        base_ref[level] = divergence(
            u_ref[level], v_ref[level], zonal, merid, west[:, level:level + 1], east[:, level:level + 1],
            keep_south * south_ref[level:level + 1, :], keep_north * north_ref[level:level + 1, :],
        )


def added_divergence(ur, vr, own_ref, border_ref, rim_ref, base_ref, units):
    zonal, merid = own_ref[0, :, 0:1], own_ref[1, :, 0:1]
    for d in range(border_ref.shape[0]):
        border = border_ref[d]
        for l in range(units):
            level = d * units + l
            base_ref[level] = base_ref[level] + divergence(
                ur[level], vr[level], zonal, merid, border[:, 2 * l:2 * l + 1], border[:, 2 * l + 1:2 * l + 2],
                rim_ref[d, 2 * l:2 * l + 1, :], rim_ref[d, 2 * l + 1:2 * l + 2, :],
            )


def pack_edges(u_ref, v_ref, first_col, last_col, first_row, last_row):
    rows, width = u_ref.shape[1:]
    lane = lax.broadcasted_iota(jnp.int32, (rows, LANE), 1)
    first = jnp.zeros((rows, LANE), jnp.float32)
    last = jnp.zeros((rows, LANE), jnp.float32)
    for level in range(u_ref.shape[0]):
        first = jnp.where(lane == level, u_ref[level, :, 0:1], first)
        last = jnp.where(lane == level, u_ref[level, :, width - 1:width], last)
        first_row[level:level + 1, :] = v_ref[level, 0:1, :]
        last_row[level:level + 1, :] = v_ref[level, rows - 1:rows, :]
    first_col[...] = first
    last_col[...] = last


def pack_halo(source, low, high, units):
    rows = source.shape[1]
    for g in range(low.shape[0]):
        for l in range(units):
            low[g, 2 * l:2 * l + 2, :] = source[g * units + l, 0:2, :]
            high[g, 2 * l:2 * l + 2, :] = source[g * units + l, rows - 2:rows, :]


def own_coefs(zc_ref, mc_ref, cutoff_ref, mask_ref, own_ref, first_lat, unfiltered):
    rows = own_ref.shape[1]
    row = lax.broadcasted_iota(jnp.int32, own_ref.shape[1:], 0)
    zonal = jnp.zeros(own_ref.shape[1:], jnp.float32)
    merid = jnp.zeros(own_ref.shape[1:], jnp.float32)
    limit = jnp.zeros(own_ref.shape[1:], jnp.int32)
    for r in range(rows):
        zonal = jnp.where(row == r, zc_ref[r], zonal)
        merid = jnp.where(row == r, mc_ref[r], merid)
        filtered = mask_ref[first_lat + r]
        bound = filtered * cutoff_ref[first_lat + r] + (1 - filtered) * unfiltered
        limit = jnp.where(row == r, bound, limit)
    own_ref[0] = zonal
    own_ref[1] = merid
    own_ref[2] = limit.astype(jnp.float32)


def flipped(index, mask):
    bit = 1
    while bit <= mask:
        if mask & bit:
            index = index + bit * (1 - 2 * (index // bit % 2))
        bit *= 2
    return index


def partner_masks(count):
    return sorted(range(1, count), key=lambda mask: (-bin(mask // 2).count("1"), mask % 2, mask))


def fused_kernel(
    bands, per_band, a_far, zc_far, mc_far, cutoff_far, mask_far, u_far, v_far, w_far, p_far, s_far, table_far, rows_far,
    u_out, v_out, w_out, p_out,
    x1, x2, d1, ur, vr, ds1, us, vs, w_mid, p_mid, base, ratio, inv, u_ref, v_ref, w_ref, p_ref, s_ref,
    halo1, halo2, low, high, table_ref, rows_ref, spec, work, back, filt, sides,
    own_ref, near, cols_send, cols_recv, rows_send, rows_recv, border_send, border_recv, rim_send, rim_recv,
    a_ref, zc_ref, mc_ref, cutoff_ref, mask_ref,
    load_sems, send_sems, recv_sems, edge_send, edge_recv, halo_send, halo_recv, last_send, last_recv,
):
    band_me = lax.axis_index("lat")
    lon_me = lax.axis_index("lon")
    lat_rows = u_ref.shape[1]
    units = u_ref.shape[0] // per_band
    channels = rows_ref.shape[0]
    half = channels - 1
    per_unit = channels * lat_rows
    split = u_ref.shape[2] // LANE
    mesh_id = pl.DeviceIdType.MESH
    is_first = band_me == 0
    is_last = band_me == bands - 1
    not_first = jnp.logical_not(is_first)
    not_last = jnp.logical_not(is_last)
    masks = partner_masks(per_band)
    partners = [flipped(lon_me, mask) for mask in masks]

    pairs = (
        (p_far, p_ref), (zc_far, zc_ref), (mc_far, mc_ref), (cutoff_far, cutoff_ref), (mask_far, mask_ref), (a_far, a_ref),
        (rows_far, rows_ref), (u_far, u_ref), (v_far, v_ref), (table_far, table_ref), (s_far, s_ref), (w_far, w_ref),
    )
    loads = [pltpu.make_async_copy(far, here, load_sems.at[n]) for n, (far, here) in enumerate(pairs)]
    for load in loads:
        load.start()
    barrier = pltpu.get_barrier_semaphore()

    def greet(band, lon):
        pl.semaphore_signal(barrier, inc=1, device_id=(band, lon), device_id_type=mesh_id)

    for partner in partners:
        greet(band_me, partner)
    for there, step in ((not_first, -1), (not_last, 1)):
        @pl.when(there)
        def _():
            for other in partners + [lon_me]:
                greet(band_me + step, other)

    loads[0].wait()
    pack_halo(p_ref, low.at[0], high.at[0], units)
    expected = per_band - 1 + jnp.where(is_first, 0, per_band) + jnp.where(is_last, 0, per_band)
    pl.semaphore_wait(barrier, expected)

    def scatter(source, target, sem, unit):
        for g in partners:
            pltpu.make_async_remote_copy(
                src_ref=source.at[pl.ds(g * units + unit, 1)], dst_ref=target.at[pl.ds(lon_me * units + unit, 1)],
                send_sem=send_sems.at[sem], recv_sem=recv_sems.at[sem, unit],
                device_id=(band_me, g), device_id_type=mesh_id,
            ).start()
        target[lon_me * units + unit] = source[lon_me * units + unit]

    def gathered(target, sem, unit):
        block = target.at[pl.ds(0, per_band - 1)]
        pltpu.make_async_copy(block, block, recv_sems.at[sem, unit]).wait()

    def sent(source, sem):
        block = source.at[pl.ds(0, (per_band - 1) * units)]
        pltpu.make_async_copy(block, block, send_sems.at[sem]).wait()

    def spread_halo(target, phase):
        def one(source, slot, sem, other):
            for g in partners + [lon_me]:
                pltpu.make_async_remote_copy(
                    src_ref=source.at[g], dst_ref=target.at[slot, lon_me],
                    send_sem=halo_send.at[sem], recv_sem=halo_recv.at[sem],
                    device_id=(other, g), device_id_type=mesh_id,
                ).start()

        @pl.when(not_first)
        def _():
            one(low.at[phase], 1, 2 * phase, band_me - 1)

        @pl.when(not_last)
        def _():
            one(high.at[phase], 0, 2 * phase + 1, band_me + 1)

    def halo_wait(phase, sems, upward):
        block = low.at[phase]

        @pl.when(not_first)
        def _():
            pltpu.make_async_copy(block, block, sems.at[2 * phase + (0 if upward else 1)]).wait()

        @pl.when(not_last)
        def _():
            pltpu.make_async_copy(block, block, sems.at[2 * phase + (1 if upward else 0)]).wait()

    def coef_copy(step, side):
        return pltpu.make_async_remote_copy(
            src_ref=own_ref, dst_ref=near.at[side], send_sem=edge_send.at[4 + side], recv_sem=edge_recv.at[4 + side],
            device_id=((band_me + bands + step) % bands, lon_me), device_id_type=mesh_id,
        )

    spread_halo(halo1, 0)
    for unit in range(units):
        scatter(p_ref, x1, 0, unit)

    for load in loads[1:7]:
        load.wait()
    own_coefs(zc_ref, mc_ref, cutoff_ref, mask_ref, own_ref, band_me * lat_rows, half * TILE)

    @pl.when(not_first)
    def _():
        coef_copy(-1, 1).start()

    @pl.when(not_last)
    def _():
        coef_copy(1, 0).start()

    @pl.when(is_first)
    def _():
        near[0] = jnp.zeros(near.shape[1:], jnp.float32)
        for g in range(per_band):
            halo1[0, g] = jnp.zeros(halo1.shape[2:], jnp.float32)
            halo2[0, g] = jnp.zeros(halo2.shape[2:], jnp.float32)

    @pl.when(is_last)
    def _():
        near[1] = jnp.zeros(near.shape[1:], jnp.float32)
        for g in range(per_band):
            halo1[1, g] = jnp.zeros(halo1.shape[2:], jnp.float32)
            halo2[1, g] = jnp.zeros(halo2.shape[2:], jnp.float32)

    work[...] = jnp.zeros(work.shape, jnp.float32)
    for load in loads[7:9]:
        load.wait()
    pack_edges(u_ref, v_ref, cols_send.at[0], cols_send.at[1], rows_send.at[0], rows_send.at[1])
    edge_copies = []
    for side, step in ((0, -1), (1, 1)):
        edge_copies.append(pltpu.make_async_remote_copy(
            src_ref=cols_send.at[side], dst_ref=cols_recv.at[side], send_sem=edge_send.at[side], recv_sem=edge_recv.at[side],
            device_id=(band_me, (lon_me + per_band + step) % per_band), device_id_type=mesh_id,
        ))
    for copy in edge_copies:
        copy.start()

    def row_copy(step, side):
        return pltpu.make_async_remote_copy(
            src_ref=rows_send.at[side], dst_ref=rows_recv.at[side], send_sem=edge_send.at[2 + side], recv_sem=edge_recv.at[2 + side],
            device_id=((band_me + bands + step) % bands, lon_me), device_id_type=mesh_id,
        )

    @pl.when(not_first)
    def _():
        row_copy(-1, 0).start()

    @pl.when(not_last)
    def _():
        row_copy(1, 1).start()

    @pl.when(is_first)
    def _():
        rows_recv[1] = jnp.zeros(rows_recv.shape[1:], jnp.float32)

    @pl.when(is_last)
    def _():
        rows_recv[0] = jnp.zeros(rows_recv.shape[1:], jnp.float32)

    for load in loads[9:]:
        load.wait()
    factor_columns(a_ref, s_ref, ratio, inv)

    @pl.when(not_first)
    def _():
        coef_copy(1, 0).wait_recv()

    @pl.when(not_last)
    def _():
        coef_copy(-1, 1).wait_recv()

    filter_terms(rows_ref, own_ref, near, filt, sides)

    def circles(source, first, count, stride):
        return [
            [source[d * stride + first + n, :, h * LANE:(h + 1) * LANE] for d in range(per_band) for h in range(split)]
            for n in range(count)
        ]

    def forward(tiles, places, accumulate):
        for n, xs in enumerate(tiles):
            forward_fill(xs, rows_ref, work, n * per_unit)
        used = len(tiles) * per_unit
        value = three_products(work[0:whole_tiles(used), :], table_ref)
        for n, place in enumerate(places):
            part = value[n * per_unit:(n + 1) * per_unit]
            spec[place] = spec[place] + part if accumulate else part

    def halo_spectra(halo, phase, accumulate):
        halo_wait(phase, halo_recv, False)
        tiles = [
            [halo[slot, d, :, h * LANE:(h + 1) * LANE] for d in range(per_band) for h in range(split)] for slot in range(2)
        ]
        forward(tiles, [units, units + 1], accumulate)

    def inverse(count):
        back[0:whole_tiles(count * per_unit), :] = three_products(work[0:whole_tiles(count * per_unit), :], table_ref)

    halo_spectra(halo1, 0, False)
    for unit in range(units):
        gathered(x1, 0, unit)
        forward(circles(x1, unit, 1, units), [unit], False)
        for t in range(channels):
            own, row, mid, v_south, v_north = merid_terms(spec, unit, t, filt, sides)
            upper = jnp.where(row == lat_rows - 1, v_north, pltpu.roll(mid, lat_rows - 1, 0))
            lower = jnp.where(row == 0, v_south, pltpu.roll(mid, 1, 0))
            merid = own_ref[1, :, 0:1]
            work[lat_rows * t:lat_rows * (t + 1), :] = filt[t, 2] * own + merid * (upper - lower)
        inverse(1)
        put_blocks(ds1, inverse_blocks(back, rows_ref, 0), unit, units)
        scatter(ds1, d1, 1, unit)

    for copy in edge_copies:
        copy.wait_recv()

    @pl.when(not_first)
    def _():
        row_copy(1, 1).wait_recv()

    @pl.when(not_last)
    def _():
        row_copy(-1, 0).wait_recv()

    base_divergence(
        u_ref, v_ref, own_ref, cols_recv.at[1], cols_recv.at[0], rows_recv.at[1], rows_recv.at[0], base,
        is_first, is_last,
    )
    for unit in range(units):
        gathered(d1, 1, unit)
    solve_columns(a_ref, s_ref, w_ref, p_ref, (base, d1), ratio, inv, w_mid, p_mid)
    pack_halo(p_mid, low.at[1], high.at[1], units)
    spread_halo(halo2, 1)
    for unit in range(units):
        scatter(p_mid, x2, 2, unit)

    halo_spectra(halo2, 1, True)
    rim_at = 2 * per_unit
    for unit in range(units):
        gathered(x2, 2, unit)
        forward(circles(x2, unit, 1, units), [unit], True)
        for t in range(channels):
            own, row, mid, v_south, v_north = merid_terms(spec, unit, t, filt, sides)
            work[lat_rows * t:lat_rows * (t + 1), :] = filt[t, 0] * own
            work[per_unit + lat_rows * t:per_unit + lat_rows * (t + 1), :] = mid
            rim = rim_at + lat_rows * t + 2 * unit
            work[rim:rim + 1, :] = v_south
            work[rim + 1:rim + 2, :] = v_north
        inverse(3 if unit == units - 1 else 2)
        zonal = own_ref[0, :, 0:1]
        moved = [-zonal * x for x in circle_diff(inverse_blocks(back, rows_ref, 0))]
        put_blocks(us, moved, unit, units)
        border_tiles(border_send, moved, unit)
        scatter(us, ur, 3, unit)
        put_blocks(vs, inverse_blocks(back, rows_ref, per_unit), unit, units)
        scatter(vs, vr, 4, unit)
    rims = inverse_blocks(back, rows_ref, rim_at)
    for b, value in enumerate(rims):
        rim_send[b // split, :, (b % split) * LANE:(b % split + 1) * LANE] = value

    def last_copy(source, target, n, g):
        return pltpu.make_async_remote_copy(
            src_ref=source.at[pl.ds(g, 1)], dst_ref=target.at[pl.ds(lon_me, 1)], send_sem=last_send.at[n], recv_sem=last_recv.at[n],
            device_id=(band_me, g), device_id_type=mesh_id,
        )

    for n, (source, target) in enumerate(((border_send, border_recv), (rim_send, rim_recv))):
        for g in partners:
            last_copy(source, target, n, g).start()
        target[lon_me] = source[lon_me]

    for unit in range(units):
        gathered(ur, 3, unit)
        gathered(vr, 4, unit)
        for d in range(per_band):
            level = d * units + unit
            u_out[level] = u_ref[level] + ur[level]
            v_out[level] = v_ref[level] + vr[level]
    for n, target in enumerate((border_recv, rim_recv)):
        block = target.at[pl.ds(0, per_band - 1)]
        pltpu.make_async_copy(block, block, last_recv.at[n]).wait()
    added_divergence(ur, vr, own_ref, border_recv, rim_recv, base, units)
    solve_columns(a_ref, s_ref, w_mid, p_mid, (base,), ratio, inv, w_out, p_out)
    for source, sem in ((p_ref, 0), (ds1, 1), (p_mid, 2), (us, 3), (vs, 4)):
        sent(source, sem)
    for n, source in enumerate((border_send, rim_send)):
        block = source.at[pl.ds(0, per_band - 1)]
        pltpu.make_async_copy(block, block, last_send.at[n]).wait()
    for phase in range(2):
        halo_wait(phase, halo_send, True)
    for copy in edge_copies:
        copy.wait_send()

    @pl.when(not_first)
    def _():
        coef_copy(-1, 1).wait_send()
        row_copy(-1, 0).wait_send()

    @pl.when(not_last)
    def _():
        coef_copy(1, 0).wait_send()
        row_copy(1, 1).wait_send()


def deliver_kernel(*refs):
    count = (len(refs) - 1) // 2
    sems = refs[-1]
    copies = [pltpu.make_async_copy(refs[n], refs[count + n], sems.at[n]) for n in range(count)]
    for copy in copies:
        copy.start()
    for copy in copies:
        copy.wait()


def deliver(arrays):
    count = len(arrays)
    return pl.pallas_call(
        deliver_kernel,
        out_shape=tuple(jax.ShapeDtypeStruct(a.shape, a.dtype) for a in arrays),
        in_specs=[pl.BlockSpec(memory_space=pltpu.VMEM)] * count,
        out_specs=(pl.BlockSpec(memory_space=pl.ANY),) * count,
        scratch_shapes=[pltpu.SemaphoreType.DMA((count,))],
        compiler_params=pltpu.CompilerParams(vmem_limit_bytes=FINISH_VMEM),
    )(*arrays)


def level_body(
    tables,
    zonal_wind,
    merid_wind,
    vertical_wind,
    pressure,
    zonal_coef,
    merid_coef,
    level_coef,
    sound_coef,
    cutoff,
    filter_mask,
):
    table, rows = (jnp.asarray(t) for t in tables)
    channels = rows.shape[0]
    bands = lax.axis_size("lat")
    per_band = lax.axis_size("lon")
    levels, lat_rows, width = pressure.shape
    units = levels // per_band
    per_unit = channels * lat_rows
    vmem = pl.BlockSpec(memory_space=pltpu.VMEM)
    far = pl.BlockSpec(memory_space=pl.ANY)

    def scratch(*shape):
        return pltpu.VMEM(shape, jnp.float32)

    field = scratch(*pressure.shape)
    halo = scratch(2, per_band, lat_rows, width)
    spare = scratch(whole_tiles(3 * per_unit), TILE)
    dma = pltpu.SemaphoreType.DMA
    operands = (
        level_coef, zonal_coef, merid_coef, cutoff, filter_mask,
        zonal_wind, merid_wind, vertical_wind, pressure, sound_coef, table, rows,
    )
    results = pl.pallas_call(
        functools.partial(fused_kernel, bands, per_band),
        out_shape=(pltpu.VMEM(pressure.shape, jnp.float32),) * 4,
        in_specs=[far] * len(operands),
        out_specs=(vmem,) * 4,
        scratch_shapes=[field] * 18 + [halo] * 4 + [
            pltpu.VMEM(table.shape, table.dtype), scratch(*rows.shape),
            scratch(units + 2, per_unit, TILE), spare, spare,
            scratch(channels, 3, lat_rows, TILE), scratch(channels, 8, TILE),
            scratch(3, lat_rows, LANE), scratch(2, 3, lat_rows, LANE),
            scratch(2, lat_rows, LANE), scratch(2, lat_rows, LANE),
            scratch(2, levels, width), scratch(2, levels, width),
            scratch(per_band, lat_rows, LANE), scratch(per_band, lat_rows, LANE),
            scratch(per_band, lat_rows, width), scratch(per_band, lat_rows, width),
            pltpu.SMEM(level_coef.shape, jnp.float32), pltpu.SMEM(zonal_coef.shape, jnp.float32),
            pltpu.SMEM(merid_coef.shape, jnp.float32), pltpu.SMEM(cutoff.shape, jnp.int32),
            pltpu.SMEM(filter_mask.shape, jnp.int32),
            dma((len(operands),)), dma((5,)), dma((5, units)), dma((6,)), dma((6,)), dma((4,)), dma((4,)), dma((2,)), dma((2,)),
        ],
        compiler_params=pltpu.CompilerParams(collective_id=0, has_side_effects=True, vmem_limit_bytes=FUSED_VMEM),
    )(*[pltpu.with_memory_space_constraint(x, pltpu.HBM) for x in operands])
    return deliver(results)


def body(tables, *arrays):
    pressure = arrays[3]
    per_band = lax.axis_size("lon")
    levels, lat_rows, width = pressure.shape
    fits = lat_rows == 8 and levels == 4 * per_band and levels <= LANE and width % LANE == 0 and per_band & (per_band - 1) == 0
    if fits:
        return level_body(tables, *arrays)
    return wide_body(*arrays)


def solution(mesh):
    in_specs = (
        P(None, "lat", "lon"),
        P(None, "lat", "lon"),
        P(None, "lat", "lon"),
        P(None, "lat", "lon"),
        P("lat"),
        P("lat"),
        P(),
        P(None, "lat", "lon"),
        P(),
        P(),
    )
    out_specs = (
        P(None, "lat", "lon"),
        P(None, "lat", "lon"),
        P(None, "lat", "lon"),
        P(None, "lat", "lon"),
    )

    def whole(*arrays):
        tables = circle_tables(arrays[0].shape[2])
        step = jax.shard_map(functools.partial(body, tables), mesh=mesh, in_specs=in_specs, out_specs=out_specs, check_vma=False)
        return step(*arrays)

    return whole
```

```python
import functools
import math

import ml_dtypes
import numpy as np
import jax
import jax.numpy as jnp
from jax import lax
from jax.experimental import pallas as pl
from jax.experimental.pallas import tpu as pltpu
from jax.sharding import PartitionSpec as P

SUBSTEPS = 2
FUSED_VMEM = 40 * 2 ** 20
FINISH_VMEM = 4 * 2 ** 20


def extended(block, sides, width):
    for axis, dim in sides:
        count = lax.axis_size(axis)
        forward = [(i, i + 1) for i in range(count - 1)]
        forward.append((count - 1, 0))
        backward = [(target, source) for source, target in forward]
        low = lax.ppermute(
            lax.slice_in_dim(block, block.shape[dim] - width, None, axis=dim), axis, forward
        )
        high = lax.ppermute(lax.slice_in_dim(block, 0, width, axis=dim), axis, backward)
        block = jnp.concatenate([low, block, high], axis=dim)
    return block


def rim_fix(padded, lat_dim):
    band_index = lax.axis_index("lat")
    bands = lax.axis_size("lat")
    extent = padded.shape[lat_dim]
    position = lax.broadcasted_iota(jnp.int32, padded.shape, lat_dim)
    first_edge = jnp.logical_and(position == 0, band_index == 0)
    final_edge = jnp.logical_and(position == extent - 1, band_index == bands - 1)
    return jnp.where(jnp.logical_or(first_edge, final_edge), 0.0, padded)


def dft_tables(length):
    half_len = length // 2
    sample = lax.broadcasted_iota(jnp.int32, (length, length), 0)
    column = lax.broadcasted_iota(jnp.int32, (length, length), 1)
    is_cosine = column <= half_len
    wavenum = jnp.where(is_cosine, column, column - half_len)
    phase = sample * wavenum % length
    angle = 2.0 * math.pi / length * phase.astype(jnp.float32)
    forward = jnp.where(is_cosine, jnp.cos(angle), jnp.sin(angle))
    single = jnp.logical_and(is_cosine, jnp.logical_or(wavenum == 0, wavenum == half_len))
    weight = jnp.where(single, 1.0, 2.0) / length
    inverse = jnp.transpose(forward * weight)
    wave_row = wavenum[0].astype(jnp.float32)
    return (forward, inverse, wave_row)


def damping(wave_row, limits):
    bound_col = limits[:, None]
    ratio = bound_col / jnp.maximum(wave_row[None, :], 1.0)
    return jnp.where(wave_row[None, :] > bound_col, ratio * ratio, 1.0)


def transform_band(block, limits, forward, inverse, wave_row):
    circles = lax.all_to_all(block, "lon", split_axis=1, concat_axis=3, tiled=True)
    spectra = jnp.einsum("vetj,jc->vetc", circles, forward, precision=lax.Precision.HIGHEST)
    scaled = spectra * damping(wave_row, limits)
    damped = jnp.einsum("vetc,cj->vetj", scaled, inverse, precision=lax.Precision.HIGHEST)
    return lax.all_to_all(damped, "lon", split_axis=3, concat_axis=1, tiled=True)


def filtered_increments(increments, own_flags, own_limits, forward, inverse, wave_row):
    flag_cols = own_flags[:, None]
    damped = transform_band(increments, own_limits, forward, inverse, wave_row)
    return jnp.where(flag_cols, damped, increments)


def column_solve(vertical_wind, pstar, level_coef, sound_coef):
    levels = vertical_wind.shape[0]
    zero_slab = jnp.zeros_like(vertical_wind[0])
    ratios = []
    values = []
    prev_ratio = zero_slab
    prev_value = zero_slab
    for level in range(levels):
        alpha = level_coef[level]
        below = alpha * sound_coef[level]
        if level + 1 < levels:
            above = alpha * sound_coef[level + 1]
            rhs = vertical_wind[level] - alpha * (pstar[level + 1] - pstar[level])
        else:
            above = zero_slab
            rhs = vertical_wind[level] + alpha * pstar[level]
        pivot = 1.0 + below + above + below * prev_ratio
        prev_ratio = -above / pivot
        prev_value = (rhs + below * prev_value) / pivot
        ratios.append(prev_ratio)
        values.append(prev_value)
    solved = [zero_slab] * levels
    upper_value = values[levels - 1]
    solved[levels - 1] = upper_value
    for level in range(levels - 2, -1, -1):
        upper_value = values[level] - ratios[level] * upper_value
        solved[level] = upper_value
    new_wind = jnp.stack(solved)
    wind_below = jnp.concatenate([zero_slab[None], new_wind[:-1]], axis=0)
    new_pressure = pstar - sound_coef * (new_wind - wind_below)
    return (new_wind, new_pressure)


def wide_body(
    zonal_wind,
    merid_wind,
    vertical_wind,
    pressure,
    zonal_coef,
    merid_coef,
    level_coef,
    sound_coef,
    cutoff,
    filter_mask,
):
    lat_rows = pressure.shape[1]
    start = lax.axis_index("lat") * lat_rows
    own_flags = lax.dynamic_slice_in_dim(filter_mask, start, lat_rows) > 0
    own_limits = lax.dynamic_slice_in_dim(cutoff, start, lat_rows).astype(jnp.float32)
    forward, inverse, wave_row = dft_tables(pressure.shape[2] * lax.axis_size("lon"))
    zonal_rows = zonal_coef[None, :, None]
    merid_rows = merid_coef[None, :, None]
    for step in range(SUBSTEPS):
        padded = extended(pressure, (("lat", 1), ("lon", 2)), 1)
        padded = rim_fix(padded, 1)
        zonal_step = -zonal_rows * (padded[:, 1:-1, 2:] - padded[:, 1:-1, :-2])
        merid_step = -merid_rows * (padded[:, 2:, 1:-1] - padded[:, :-2, 1:-1])
        increments = jnp.stack([zonal_step, merid_step])
        damped = filtered_increments(increments, own_flags, own_limits, forward, inverse, wave_row)
        winds = jnp.stack([zonal_wind, merid_wind]) + damped
        wind_pad = extended(winds, (("lat", 2), ("lon", 3)), 1)
        wind_pad = rim_fix(wind_pad, 2)
        diverge = zonal_rows * (wind_pad[0, :, 1:-1, 2:] - wind_pad[0, :, 1:-1, :-2])
        diverge = diverge + merid_rows * (wind_pad[1, :, 2:, 1:-1] - wind_pad[1, :, :-2, 1:-1])
        pstar = pressure - sound_coef * diverge
        vertical_wind, pressure = column_solve(vertical_wind, pstar, level_coef, sound_coef)
        zonal_wind = winds[0]
        merid_wind = winds[1]
    return (zonal_wind, merid_wind, vertical_wind, pressure)


LANE = 128
TILE = 2 * LANE


def circle_tables(length):
    blocks = length // LANE
    half = blocks // 2
    m = np.arange(LANE, dtype=np.float64)[:, None]
    c = np.arange(LANE)[None, :]
    angle = 2 * np.pi * ((m * c) % LANE) / LANE
    cos, sin = np.cos(angle) / np.sqrt(LANE), np.sin(angle) / np.sqrt(LANE)
    table = np.block([[cos, -sin], [sin, cos]])
    high = table.astype(ml_dtypes.bfloat16)
    rest = (table - high.astype(np.float64)).astype(ml_dtypes.bfloat16)
    rows = np.zeros((half + 1, 8, TILE), np.float32)
    for k1 in range(half + 1):
        k = k1 + blocks * c[0]
        waves = np.tile(np.minimum(k, length - k), 2)
        scale = (1.0 if k1 in (0, half) else 2.0) / blocks
        turn = 2 * np.pi * m[:, 0] * k1 / length
        rows[k1, 0] = waves
        rows[k1, 1] = 4.0 * np.sin(2 * np.pi * waves / length) ** 2
        rows[k1, 2] = np.where(np.arange(TILE) < LANE, scale, -scale)
        rows[k1, 3] = np.concatenate([np.cos(turn), np.sin(turn)])
    return np.stack([high, rest]), rows


def split_parts(value):
    high = value.astype(jnp.bfloat16)
    rest = (value - high.astype(jnp.float32)).astype(jnp.bfloat16)
    return high, rest


def three_products(value, table_ref):
    high, rest = split_parts(value)
    dims = (((1,), (0,)), ((), ()))
    rows = value.shape[0]
    table = table_ref[0]
    both = lax.dot_general(jnp.concatenate([high, rest], axis=0), table, dims, preferred_element_type=jnp.float32)
    corr = lax.dot_general(high, table_ref[1], dims, preferred_element_type=jnp.float32)
    return both[:rows] + (both[rows:] + corr)


def weighted(terms):
    total = None
    for coef, value in terms:
        if abs(coef) < 1e-12:
            continue
        if abs(abs(coef) - 1.0) < 1e-12:
            term = value
        else:
            term = abs(coef) * value
        if total is None:
            total = term if coef > 0 else -term
        else:
            total = total + term if coef > 0 else total - term
    return total


def coarse_forward(xs):
    count = len(xs)
    half = count // 2
    even = {b: xs[b] + xs[count - b] for b in range(1, half)}
    odd = {b: xs[b] - xs[count - b] for b in range(1, half)}
    real, imag = [], {}
    for k in range(half + 1):
        ends = xs[0] + xs[half] if k % 2 == 0 else xs[0] - xs[half]
        real.append(weighted([(1.0, ends)] + [(math.cos(2 * math.pi * b * k / count), even[b]) for b in range(1, half)]))
    for k in range(1, half):
        imag[k] = weighted([(-math.sin(2 * math.pi * b * k / count), odd[b]) for b in range(1, half)])
    pairs = [(real[0], real[half])] + [(real[k], imag[k]) for k in range(1, half)]
    return pairs


def coarse_inverse(pairs):
    half = len(pairs)
    count = 2 * half
    first, last = pairs[0]
    xs = [None] * count
    for b in range(half + 1):
        ends = first + last if b % 2 == 0 else first - last
        cos_part = weighted([(1.0, ends)] + [(math.cos(2 * math.pi * b * k / count), pairs[k][0]) for k in range(1, half)])
        if b in (0, half):
            xs[b] = cos_part
        else:
            sin_part = weighted([(-math.sin(2 * math.pi * b * k / count), pairs[k][1]) for k in range(1, half)])
            xs[b] = cos_part + sin_part
            xs[count - b] = cos_part - sin_part
    return xs


def whole_tiles(count):
    return -(-count // 16) * 16


def forward_fill(xs, rows_ref, work_ref, start):
    pairs = coarse_forward(xs)
    half = len(pairs)
    first, last = pairs[0]
    for t in range(half + 1):
        cos, sin = rows_ref[t, 3:4, :LANE], rows_ref[t, 3:4, LANE:]
        if t == 0:
            left, right = first, jnp.zeros_like(first)
        elif t == half:
            left, right = last * cos, -(last * sin)
        else:
            real, imag = pairs[t]
            left, right = real * cos + imag * sin, imag * cos - real * sin
        work_ref[start + 8 * t:start + 8 * t + 8, :LANE] = left
        work_ref[start + 8 * t:start + 8 * t + 8, LANE:] = right


def inverse_blocks(back_ref, rows_ref, start):
    half = rows_ref.shape[0] - 1
    pairs = []
    ends = []
    for t in range(half + 1):
        left = back_ref[start + 8 * t:start + 8 * t + 8, :LANE]
        right = back_ref[start + 8 * t:start + 8 * t + 8, LANE:]
        cos, sin = rows_ref[t, 3:4, :LANE], rows_ref[t, 3:4, LANE:]
        if t == 0:
            ends.append(left)
        elif t == half:
            ends.append(left * cos + right * sin)
        else:
            pairs.append((left * cos + right * sin, left * sin - right * cos))
    return coarse_inverse([tuple(ends)] + pairs)


def put_blocks(out_ref, xs, unit, units):
    split = out_ref.shape[2] // LANE
    for b, value in enumerate(xs):
        out_ref[(b // split) * units + unit, :, (b % split) * LANE:(b % split + 1) * LANE] = value


def circle_diff(xs):
    count = len(xs)
    lane = lax.broadcasted_iota(jnp.int32, xs[0].shape, 1)
    ahead = [pltpu.roll(x, LANE - 1, 1) for x in xs]
    behind = [pltpu.roll(x, 1, 1) for x in xs]
    out = []
    for b in range(count):
        nxt = jnp.where(lane == LANE - 1, ahead[(b + 1) % count], ahead[b])
        prv = jnp.where(lane == 0, behind[(b - 1) % count], behind[b])
        out.append(nxt - prv)
    return out


def border_rows(edge_ref, send_ref):
    for d in range(edge_ref.shape[0]):
        send_ref[d] = jnp.sum(pltpu.roll(edge_ref[d], 0, 1, stride=8, stride_axis=0), axis=0, keepdims=True)


def border_columns(row):
    value = jnp.broadcast_to(row, (8, LANE))
    place = lax.broadcasted_iota(jnp.int32, (8, LANE), 0)
    for bit in (1, 2, 4):
        value = jnp.where(place // bit % 2 == 1, pltpu.roll(value, LANE - 8 * bit, 1), value)
    return value


def border_tiles(edge_ref, xs, unit):
    count = len(xs)
    split = count // edge_ref.shape[0]
    lane = lax.broadcasted_iota(jnp.int32, xs[0].shape, 1)
    turned = [pltpu.roll(x, 2 * unit + 1, 1) for x in xs]
    for d in range(edge_ref.shape[0]):
        west, east = turned[(d * split - 1) % count], turned[(d * split + split) % count]
        kept = edge_ref[d] if unit else jnp.zeros_like(west)
        edge_ref[d] = jnp.where(lane == 2 * unit, west, jnp.where(lane == 2 * unit + 1, east, kept))


def filter_values(limit, wave, scale):
    quotient = limit / jnp.maximum(wave, 1.0)
    return jnp.where(wave > limit, quotient * quotient, 1.0) * scale


def filter_terms(rows_ref, own_ref, near_ref, filt_ref, side_ref):
    rows = own_ref.shape[1]
    zonal, merid, limit = own_ref[0, :, 0:1], own_ref[1, :, 0:1], own_ref[2, :, 0:1]
    for t in range(rows_ref.shape[0]):
        wave, sines, scale = rows_ref[t, 0:1, :], rows_ref[t, 1:2, :], rows_ref[t, 2:3, :]
        factor = filter_values(limit, wave, scale)
        filt_ref[t, 0] = factor
        filt_ref[t, 1] = merid * factor
        filt_ref[t, 2] = (zonal * zonal) * sines * factor
        south = near_ref[0, 1, rows - 1:rows, 0:1] * filter_values(near_ref[0, 2, rows - 1:rows, 0:1], wave, scale)
        north = near_ref[1, 1, 0:1, 0:1] * filter_values(near_ref[1, 2, 0:1, 0:1], wave, scale)
        side_ref[t, 0:1, :] = south
        side_ref[t, 1:2, :] = north


def merid_terms(spec_ref, unit, t, filt_ref, side_ref, south_ref, north_ref, at):
    tile = spec_ref.shape[1] // filt_ref.shape[0]
    own = spec_ref[unit, tile * t:tile * t + tile, :]
    row = lax.broadcasted_iota(jnp.int32, own.shape, 0)
    below_far, below = south_ref[at:at + 1, :], south_ref[at + 1:at + 2, :]
    above, above_far = north_ref[at:at + 1, :], north_ref[at + 1:at + 2, :]
    upper = jnp.where(row == tile - 1, above, pltpu.roll(own, tile - 1, 0))
    lower = jnp.where(row == 0, below, pltpu.roll(own, 1, 0))
    mid = -filt_ref[t, 1] * (upper - lower)
    v_south = -side_ref[t, 0:1, :] * (own[0:1] - below_far)
    v_north = -side_ref[t, 1:2, :] * (above_far - own[tile - 1:tile])
    return own, row, mid, v_south, v_north


def factor_columns(a_ref, s_ref, ratio_ref, inv_ref):
    levels = s_ref.shape[0]
    prev = jnp.zeros(s_ref.shape[1:], jnp.float32)
    for level in range(levels):
        alpha = a_ref[level]
        below = alpha * s_ref[level]
        above = alpha * s_ref[level + 1] if level + 1 < levels else jnp.zeros_like(below)
        inv = 1.0 / (1.0 + below + above + below * prev)
        prev = -above * inv
        ratio_ref[level] = prev
        inv_ref[level] = inv


def solve_columns(a_ref, s_ref, w_ref, p_ref, parts, ratio_ref, inv_ref, w_out, p_out):
    levels = s_ref.shape[0]

    def star(level):
        total = parts[0][level]
        for part in parts[1:]:
            total = total + part[level]
        return p_ref[level] - s_ref[level] * total

    here = star(0)
    prev = jnp.zeros_like(here)
    for level in range(levels):
        alpha = a_ref[level]
        p_out[level] = here
        if level + 1 < levels:
            nxt = star(level + 1)
            rhs = w_ref[level] - alpha * (nxt - here)
        else:
            nxt = here
            rhs = w_ref[level] + alpha * here
        prev = (rhs + alpha * s_ref[level] * prev) * inv_ref[level]
        w_out[level] = prev
        here = nxt
    upper = w_out[levels - 1]
    for level in range(levels - 1, 0, -1):
        lower = w_out[level - 1] - ratio_ref[level - 1] * upper
        w_out[level - 1] = lower
        p_out[level] = p_out[level] - s_ref[level] * (upper - lower)
        upper = lower
    p_out[0] = p_out[0] - s_ref[0] * upper


def divergence(u, v, zonal, merid, west, east, south, north):
    rows, width = u.shape
    lane = lax.broadcasted_iota(jnp.int32, (rows, width), 1)
    row = lax.broadcasted_iota(jnp.int32, (rows, width), 0)
    ahead = jnp.where(lane == width - 1, east, pltpu.roll(u, width - 1, 1))
    behind = jnp.where(lane == 0, west, pltpu.roll(u, 1, 1))
    upper = jnp.where(row == rows - 1, north, pltpu.roll(v, rows - 1, 0))
    lower = jnp.where(row == 0, south, pltpu.roll(v, 1, 0))
    return zonal * (ahead - behind) + merid * (upper - lower)


def base_divergence(u_ref, v_ref, own_ref, west_ref, east_ref, south_ref, north_ref, base_ref, is_first, is_last):
    zonal, merid = own_ref[0, :, 0:1], own_ref[1, :, 0:1]
    keep_south = jnp.where(is_first, 0.0, 1.0)
    keep_north = jnp.where(is_last, 0.0, 1.0)
    west = west_ref[...]
    east = east_ref[...]
    for level in range(u_ref.shape[0]):
        base_ref[level] = divergence(
            u_ref[level], v_ref[level], zonal, merid, west[:, level:level + 1], east[:, level:level + 1],
            keep_south * south_ref[level:level + 1, :], keep_north * north_ref[level:level + 1, :],
        )


def added_divergence(ur, vr, own_ref, base_ref, levels):
    zonal, merid = own_ref[0, :, 0:1], own_ref[1, :, 0:1]
    for level in levels:
        base_ref[level] = base_ref[level] + divergence(ur[level], vr[level], zonal, merid, 0.0, 0.0, 0.0, 0.0)


def added_borders(own_ref, border_ref, base_ref, units):
    zonal = own_ref[0, :, 0:1]
    width = base_ref.shape[2]
    lane = lax.broadcasted_iota(jnp.int32, (8, LANE), 1)
    for d in range(border_ref.shape[0]):
        border = border_columns(border_ref[d])
        for l in range(units):
            level = d * units + l
            west = jnp.where(lane == 0, zonal * border[:, 2 * l:2 * l + 1], 0.0)
            east = jnp.where(lane == LANE - 1, zonal * border[:, 2 * l + 1:2 * l + 2], 0.0)
            base_ref[level, :, :LANE] = base_ref[level, :, :LANE] - west
            base_ref[level, :, width - LANE:] = base_ref[level, :, width - LANE:] + east


def added_rims(own_ref, rim_ref, base_ref, units):
    merid = own_ref[1, :, 0:1]
    rows = base_ref.shape[1]
    for d in range(rim_ref.shape[0]):
        for l in range(units):
            level = d * units + l
            base_ref[level, 0:1, :] = base_ref[level, 0:1, :] - merid[0:1] * rim_ref[d, 2 * l:2 * l + 1, :]
            base_ref[level, rows - 1:rows, :] = base_ref[level, rows - 1:rows, :] + merid[rows - 1:rows] * rim_ref[d, 2 * l + 1:2 * l + 2, :]


def pack_edges(u_ref, v_ref, first_col, last_col, first_row, last_row):
    rows, width = u_ref.shape[1:]
    lane = lax.broadcasted_iota(jnp.int32, (rows, LANE), 1)
    first = jnp.zeros((rows, LANE), jnp.float32)
    last = jnp.zeros((rows, LANE), jnp.float32)
    for level in range(u_ref.shape[0]):
        first = jnp.where(lane == level, u_ref[level, :, 0:1], first)
        last = jnp.where(lane == level, u_ref[level, :, width - 1:width], last)
        first_row[level:level + 1, :] = v_ref[level, 0:1, :]
        last_row[level:level + 1, :] = v_ref[level, rows - 1:rows, :]
    first_col[...] = first
    last_col[...] = last


def pack_halo(source, low, high, units):
    rows = source.shape[1]
    for g in range(low.shape[0]):
        for l in range(units):
            low[g, 2 * l:2 * l + 2, :] = source[g * units + l, 0:2, :]
            high[g, 2 * l:2 * l + 2, :] = source[g * units + l, rows - 2:rows, :]


def own_coefs(zc_ref, mc_ref, cutoff_ref, mask_ref, own_ref, first_lat, unfiltered):
    rows = own_ref.shape[1]
    row = lax.broadcasted_iota(jnp.int32, own_ref.shape[1:], 0)
    zonal = jnp.zeros(own_ref.shape[1:], jnp.float32)
    merid = jnp.zeros(own_ref.shape[1:], jnp.float32)
    limit = jnp.zeros(own_ref.shape[1:], jnp.int32)
    for r in range(rows):
        zonal = jnp.where(row == r, zc_ref[r], zonal)
        merid = jnp.where(row == r, mc_ref[r], merid)
        filtered = mask_ref[first_lat + r]
        bound = filtered * cutoff_ref[first_lat + r] + (1 - filtered) * unfiltered
        limit = jnp.where(row == r, bound, limit)
    own_ref[0] = zonal
    own_ref[1] = merid
    own_ref[2] = limit.astype(jnp.float32)


def flipped(index, mask):
    bit = 1
    while bit <= mask:
        if mask & bit:
            index = index + bit * (1 - 2 * (index // bit % 2))
        bit *= 2
    return index


def partner_masks(count):
    return sorted(range(1, count), key=lambda mask: (-bin(mask // 2).count("1"), mask % 2, mask))


def fused_kernel(
    bands, per_band, a_far, zc_far, mc_far, cutoff_far, mask_far, u_far, v_far, w_far, p_far, s_far, table_far, rows_far,
    u_out, v_out, w_out, p_out,
    x1, x2, d1, ur, vr, ds1, us, vs, w_mid, p_mid, base, ratio, inv, u_ref, v_ref, w_ref, p_ref, s_ref,
    halo1, low, high, chain_send, chain_recv, table_ref, rows_ref, spec, work, back, filt, sides,
    own_ref, near, cols_send, cols_recv, rows_send, rows_recv, border_tile, border_send, border_recv, rim_send, rim_recv,
    a_ref, zc_ref, mc_ref, cutoff_ref, mask_ref,
    load_sems, send_sems, recv_sems, edge_send, edge_recv, halo_send, halo_recv, last_send, last_recv, chain_out, chain_in,
):
    band_me = lax.axis_index("lat")
    lon_me = lax.axis_index("lon")
    lat_rows = u_ref.shape[1]
    units = u_ref.shape[0] // per_band
    channels = rows_ref.shape[0]
    half = channels - 1
    per_unit = channels * lat_rows
    split = u_ref.shape[2] // LANE
    mesh_id = pl.DeviceIdType.MESH
    is_first = band_me == 0
    is_last = band_me == bands - 1
    not_first = jnp.logical_not(is_first)
    not_last = jnp.logical_not(is_last)
    masks = partner_masks(per_band)
    partners = [flipped(lon_me, mask) for mask in masks]

    pairs = (
        (p_far, p_ref), (zc_far, zc_ref), (mc_far, mc_ref), (cutoff_far, cutoff_ref), (mask_far, mask_ref), (a_far, a_ref),
        (rows_far, rows_ref), (u_far, u_ref), (v_far, v_ref), (table_far, table_ref), (s_far, s_ref), (w_far, w_ref),
    )
    loads = [pltpu.make_async_copy(far, here, load_sems.at[n]) for n, (far, here) in enumerate(pairs)]
    for load in loads:
        load.start()
    barrier = pltpu.get_barrier_semaphore()

    def greet(band, lon):
        pl.semaphore_signal(barrier, inc=1, device_id=(band, lon), device_id_type=mesh_id)

    for partner in partners:
        greet(band_me, partner)
    for there, step in ((not_first, -1), (not_last, 1)):
        @pl.when(there)
        def _():
            for other in partners + [lon_me]:
                greet(band_me + step, other)

    loads[0].wait()
    pack_halo(p_ref, low, high, units)
    expected = per_band - 1 + jnp.where(is_first, 0, per_band) + jnp.where(is_last, 0, per_band)
    pl.semaphore_wait(barrier, expected)

    def scatter(source, target, sem, unit):
        for g in partners:
            pltpu.make_async_remote_copy(
                src_ref=source.at[pl.ds(g * units + unit, 1)], dst_ref=target.at[pl.ds(lon_me * units + unit, 1)],
                send_sem=send_sems.at[sem], recv_sem=recv_sems.at[sem, unit],
                device_id=(band_me, g), device_id_type=mesh_id,
            ).start()
        target[lon_me * units + unit] = source[lon_me * units + unit]

    def gathered(target, sem, unit):
        block = target.at[pl.ds(0, per_band - 1)]
        pltpu.make_async_copy(block, block, recv_sems.at[sem, unit]).wait()

    def sent(source, sem):
        block = source.at[pl.ds(0, (per_band - 1) * units)]
        pltpu.make_async_copy(block, block, send_sems.at[sem]).wait()

    def spread_halo(target):
        def one(source, slot, sem, other):
            for g in partners + [lon_me]:
                pltpu.make_async_remote_copy(
                    src_ref=source.at[g], dst_ref=target.at[slot, lon_me],
                    send_sem=halo_send.at[sem], recv_sem=halo_recv.at[sem],
                    device_id=(other, g), device_id_type=mesh_id,
                ).start()

        @pl.when(not_first)
        def _():
            one(low, 1, 0, band_me - 1)

        @pl.when(not_last)
        def _():
            one(high, 0, 1, band_me + 1)

    def halo_wait(sems, upward):
        @pl.when(not_first)
        def _():
            pltpu.make_async_copy(low, low, sems.at[0 if upward else 1]).wait()

        @pl.when(not_last)
        def _():
            pltpu.make_async_copy(low, low, sems.at[1 if upward else 0]).wait()

    def chain_copy(unit, side):
        return pltpu.make_async_remote_copy(
            src_ref=chain_send.at[side, unit], dst_ref=chain_recv.at[side, unit],
            send_sem=chain_out.at[side], recv_sem=chain_in.at[side, unit],
            device_id=((band_me + bands + 1 - 2 * side) % bands, lon_me), device_id_type=mesh_id,
        )

    def coef_copy(step, side):
        return pltpu.make_async_remote_copy(
            src_ref=own_ref, dst_ref=near.at[side], send_sem=edge_send.at[4 + side], recv_sem=edge_recv.at[4 + side],
            device_id=((band_me + bands + step) % bands, lon_me), device_id_type=mesh_id,
        )

    spread_halo(halo1)
    for unit in range(units):
        scatter(p_ref, x1, 0, unit)

    for load in loads[1:7]:
        load.wait()
    own_coefs(zc_ref, mc_ref, cutoff_ref, mask_ref, own_ref, band_me * lat_rows, half * TILE)

    @pl.when(not_first)
    def _():
        coef_copy(-1, 1).start()

    @pl.when(not_last)
    def _():
        coef_copy(1, 0).start()

    @pl.when(is_first)
    def _():
        near[0] = jnp.zeros(near.shape[1:], jnp.float32)
        chain_recv[0] = jnp.zeros(chain_recv.shape[1:], jnp.float32)
        for g in range(per_band):
            halo1[0, g] = jnp.zeros(halo1.shape[2:], jnp.float32)

    @pl.when(is_last)
    def _():
        near[1] = jnp.zeros(near.shape[1:], jnp.float32)
        chain_recv[1] = jnp.zeros(chain_recv.shape[1:], jnp.float32)
        for g in range(per_band):
            halo1[1, g] = jnp.zeros(halo1.shape[2:], jnp.float32)

    work[...] = jnp.zeros(work.shape, jnp.float32)
    for load in loads[7:9]:
        load.wait()
    pack_edges(u_ref, v_ref, cols_send.at[0], cols_send.at[1], rows_send.at[0], rows_send.at[1])
    edge_copies = []
    for side, step in ((0, -1), (1, 1)):
        edge_copies.append(pltpu.make_async_remote_copy(
            src_ref=cols_send.at[side], dst_ref=cols_recv.at[side], send_sem=edge_send.at[side], recv_sem=edge_recv.at[side],
            device_id=(band_me, (lon_me + per_band + step) % per_band), device_id_type=mesh_id,
        ))
    for copy in edge_copies:
        copy.start()

    def row_copy(step, side):
        return pltpu.make_async_remote_copy(
            src_ref=rows_send.at[side], dst_ref=rows_recv.at[side], send_sem=edge_send.at[2 + side], recv_sem=edge_recv.at[2 + side],
            device_id=((band_me + bands + step) % bands, lon_me), device_id_type=mesh_id,
        )

    @pl.when(not_first)
    def _():
        row_copy(-1, 0).start()

    @pl.when(not_last)
    def _():
        row_copy(1, 1).start()

    @pl.when(is_first)
    def _():
        rows_recv[1] = jnp.zeros(rows_recv.shape[1:], jnp.float32)

    @pl.when(is_last)
    def _():
        rows_recv[0] = jnp.zeros(rows_recv.shape[1:], jnp.float32)

    for load in loads[9:]:
        load.wait()
    factor_columns(a_ref, s_ref, ratio, inv)

    @pl.when(not_first)
    def _():
        coef_copy(1, 0).wait_recv()

    @pl.when(not_last)
    def _():
        coef_copy(-1, 1).wait_recv()

    filter_terms(rows_ref, own_ref, near, filt, sides)

    def circles(source, first, count, stride):
        return [
            [source[d * stride + first + n, :, h * LANE:(h + 1) * LANE] for d in range(per_band) for h in range(split)]
            for n in range(count)
        ]

    def forward(tiles, places, accumulate):
        for n, xs in enumerate(tiles):
            forward_fill(xs, rows_ref, work, n * per_unit)
        used = len(tiles) * per_unit
        value = three_products(work[0:whole_tiles(used), :], table_ref)
        for n, place in enumerate(places):
            part = value[n * per_unit:(n + 1) * per_unit]
            spec[place] = spec[place] + part if accumulate else part

    def inverse(count):
        back[0:whole_tiles(count * per_unit), :] = three_products(work[0:whole_tiles(count * per_unit), :], table_ref)

    halo_wait(halo_recv, False)
    forward([
        [halo1[slot, d, :, h * LANE:(h + 1) * LANE] for d in range(per_band) for h in range(split)] for slot in range(2)
    ], [units, units + 1], False)
    for unit in range(units):
        gathered(x1, 0, unit)
        forward(circles(x1, unit, 1, units), [unit], False)
        for t in range(channels):
            at = lat_rows * t + 2 * unit
            own, row, mid, v_south, v_north = merid_terms(spec, unit, t, filt, sides, spec.at[units], spec.at[units + 1], at)
            upper = jnp.where(row == lat_rows - 1, v_north, pltpu.roll(mid, lat_rows - 1, 0))
            lower = jnp.where(row == 0, v_south, pltpu.roll(mid, 1, 0))
            merid = own_ref[1, :, 0:1]
            work[lat_rows * t:lat_rows * (t + 1), :] = filt[t, 2] * own + merid * (upper - lower)
        inverse(1)
        put_blocks(ds1, inverse_blocks(back, rows_ref, 0), unit, units)
        scatter(ds1, d1, 1, unit)

    for copy in edge_copies:
        copy.wait_recv()

    @pl.when(not_first)
    def _():
        row_copy(1, 1).wait_recv()

    @pl.when(not_last)
    def _():
        row_copy(-1, 0).wait_recv()

    base_divergence(
        u_ref, v_ref, own_ref, cols_recv.at[1], cols_recv.at[0], rows_recv.at[1], rows_recv.at[0], base,
        is_first, is_last,
    )
    for unit in range(units):
        gathered(d1, 1, unit)
    solve_columns(a_ref, s_ref, w_ref, p_ref, (base, d1), ratio, inv, w_mid, p_mid)
    for unit in range(units):
        scatter(p_mid, x2, 2, unit)

    zonal = own_ref[0, :, 0:1]
    for unit in range(units):
        gathered(x2, 2, unit)
        forward(circles(x2, unit, 1, units), [unit], True)
        for t in range(channels):
            at = lat_rows * t
            chain_send[0, unit, 2 * t:2 * t + 2, :] = spec[unit, at + lat_rows - 2:at + lat_rows, :]
            chain_send[1, unit, 2 * t:2 * t + 2, :] = spec[unit, at:at + 2, :]

        @pl.when(not_last)
        def _():
            chain_copy(unit, 0).start()

        @pl.when(not_first)
        def _():
            chain_copy(unit, 1).start()

        for t in range(channels):
            at = lat_rows * t
            work[at:at + lat_rows, :] = filt[t, 0] * spec[unit, at:at + lat_rows, :]
        inverse(1)
        moved = [-zonal * x for x in circle_diff(inverse_blocks(back, rows_ref, 0))]
        put_blocks(us, moved, unit, units)
        scatter(us, ur, 3, unit)
        border_tiles(border_tile, moved, unit)
    border_rows(border_tile, border_send)

    def last_copy(source, target, n, g):
        return pltpu.make_async_remote_copy(
            src_ref=source.at[pl.ds(g, 1)], dst_ref=target.at[pl.ds(lon_me, 1)], send_sem=last_send.at[n], recv_sem=last_recv.at[n],
            device_id=(band_me, g), device_id_type=mesh_id,
        )

    def last_scatter(source, target, n):
        for g in partners:
            last_copy(source, target, n, g).start()
        target[lon_me] = source[lon_me]

    last_scatter(border_send, border_recv, 0)
    rim_at = per_unit
    for unit in range(units):
        @pl.when(not_first)
        def _():
            chain_copy(unit, 0).wait_recv()

        @pl.when(not_last)
        def _():
            chain_copy(unit, 1).wait_recv()

        for t in range(channels):
            own, row, mid, v_south, v_north = merid_terms(
                spec, unit, t, filt, sides, chain_recv.at[0, unit], chain_recv.at[1, unit], 2 * t,
            )
            work[lat_rows * t:lat_rows * (t + 1), :] = mid
            rim = rim_at + lat_rows * t + 2 * unit
            work[rim:rim + 1, :] = v_south
            work[rim + 1:rim + 2, :] = v_north
        inverse(2 if unit == units - 1 else 1)
        put_blocks(vs, inverse_blocks(back, rows_ref, 0), unit, units)
        scatter(vs, vr, 4, unit)
    rims = inverse_blocks(back, rows_ref, rim_at)
    for b, value in enumerate(rims):
        rim_send[b // split, :, (b % split) * LANE:(b % split + 1) * LANE] = value

    last_scatter(rim_send, rim_recv, 1)

    def last_wait(target, sems, n):
        block = target.at[pl.ds(0, per_band - 1)]
        pltpu.make_async_copy(block, block, sems.at[n]).wait()

    for unit in range(units):
        gathered(ur, 3, unit)
        for d in range(per_band):
            level = d * units + unit
            u_out[level] = u_ref[level] + ur[level]
    last_wait(border_recv, last_recv, 0)
    added_borders(own_ref, border_recv, base, units)
    for unit in range(units):
        gathered(vr, 4, unit)
        own_levels = [d * units + unit for d in range(per_band)]
        for level in own_levels:
            v_out[level] = v_ref[level] + vr[level]
        added_divergence(ur, vr, own_ref, base, own_levels)
    last_wait(rim_recv, last_recv, 1)
    added_rims(own_ref, rim_recv, base, units)
    solve_columns(a_ref, s_ref, w_mid, p_mid, (base,), ratio, inv, w_out, p_out)
    for source, sem in ((p_ref, 0), (ds1, 1), (p_mid, 2), (us, 3), (vs, 4)):
        sent(source, sem)
    last_wait(border_send, last_send, 0)
    last_wait(rim_send, last_send, 1)
    halo_wait(halo_send, True)
    for copy in edge_copies:
        copy.wait_send()

    @pl.when(not_first)
    def _():
        pltpu.make_async_copy(chain_send.at[1], chain_send.at[1], chain_out.at[1]).wait()
        coef_copy(-1, 1).wait_send()
        row_copy(-1, 0).wait_send()

    @pl.when(not_last)
    def _():
        pltpu.make_async_copy(chain_send.at[0], chain_send.at[0], chain_out.at[0]).wait()
        coef_copy(1, 0).wait_send()
        row_copy(1, 1).wait_send()


def deliver_kernel(*refs):
    count = (len(refs) - 1) // 2
    sems = refs[-1]
    copies = [pltpu.make_async_copy(refs[n], refs[count + n], sems.at[n]) for n in range(count)]
    for copy in copies:
        copy.start()
    for copy in copies:
        copy.wait()


def deliver(arrays):
    count = len(arrays)
    return pl.pallas_call(
        deliver_kernel,
        out_shape=tuple(jax.ShapeDtypeStruct(a.shape, a.dtype) for a in arrays),
        in_specs=[pl.BlockSpec(memory_space=pltpu.VMEM)] * count,
        out_specs=(pl.BlockSpec(memory_space=pl.ANY),) * count,
        scratch_shapes=[pltpu.SemaphoreType.DMA((count,))],
        compiler_params=pltpu.CompilerParams(vmem_limit_bytes=FINISH_VMEM),
    )(*arrays)


def level_body(
    tables,
    zonal_wind,
    merid_wind,
    vertical_wind,
    pressure,
    zonal_coef,
    merid_coef,
    level_coef,
    sound_coef,
    cutoff,
    filter_mask,
):
    table, rows = (jnp.asarray(t) for t in tables)
    channels = rows.shape[0]
    bands = lax.axis_size("lat")
    per_band = lax.axis_size("lon")
    levels, lat_rows, width = pressure.shape
    units = levels // per_band
    per_unit = channels * lat_rows
    vmem = pl.BlockSpec(memory_space=pltpu.VMEM)
    far = pl.BlockSpec(memory_space=pl.ANY)

    def scratch(*shape):
        return pltpu.VMEM(shape, jnp.float32)

    field = scratch(*pressure.shape)
    halo = scratch(2, per_band, lat_rows, width)
    chain = scratch(2, units, -(-2 * channels // 8) * 8, TILE)
    spare = scratch(whole_tiles(2 * per_unit), TILE)
    dma = pltpu.SemaphoreType.DMA
    operands = (
        level_coef, zonal_coef, merid_coef, cutoff, filter_mask,
        zonal_wind, merid_wind, vertical_wind, pressure, sound_coef, table, rows,
    )
    results = pl.pallas_call(
        functools.partial(fused_kernel, bands, per_band),
        out_shape=(pltpu.VMEM(pressure.shape, jnp.float32),) * 4,
        in_specs=[far] * len(operands),
        out_specs=(vmem,) * 4,
        scratch_shapes=[field] * 18 + [halo, scratch(per_band, lat_rows, width), scratch(per_band, lat_rows, width), chain, chain] + [
            pltpu.VMEM(table.shape, table.dtype), scratch(*rows.shape),
            scratch(units + 2, per_unit, TILE), spare, spare,
            scratch(channels, 3, lat_rows, TILE), scratch(channels, 8, TILE),
            scratch(3, lat_rows, LANE), scratch(2, 3, lat_rows, LANE),
            scratch(2, lat_rows, LANE), scratch(2, lat_rows, LANE),
            scratch(2, levels, width), scratch(2, levels, width),
            scratch(per_band, lat_rows, LANE), scratch(per_band, 1, LANE), scratch(per_band, 1, LANE),
            scratch(per_band, lat_rows, width), scratch(per_band, lat_rows, width),
            pltpu.SMEM(level_coef.shape, jnp.float32), pltpu.SMEM(zonal_coef.shape, jnp.float32),
            pltpu.SMEM(merid_coef.shape, jnp.float32), pltpu.SMEM(cutoff.shape, jnp.int32),
            pltpu.SMEM(filter_mask.shape, jnp.int32),
            dma((len(operands),)), dma((5,)), dma((5, units)), dma((6,)), dma((6,)), dma((2,)), dma((2,)), dma((2,)), dma((2,)), dma((2,)), dma((2, units)),
        ],
        compiler_params=pltpu.CompilerParams(collective_id=0, has_side_effects=True, vmem_limit_bytes=FUSED_VMEM),
    )(*[pltpu.with_memory_space_constraint(x, pltpu.HBM) for x in operands])
    return deliver(results)


def body(tables, *arrays):
    pressure = arrays[3]
    per_band = lax.axis_size("lon")
    levels, lat_rows, width = pressure.shape
    fits = lat_rows == 8 and levels == 4 * per_band and levels <= LANE and width % LANE == 0 and per_band & (per_band - 1) == 0
    if fits:
        return level_body(tables, *arrays)
    return wide_body(*arrays)


def solution(mesh):
    in_specs = (
        P(None, "lat", "lon"),
        P(None, "lat", "lon"),
        P(None, "lat", "lon"),
        P(None, "lat", "lon"),
        P("lat"),
        P("lat"),
        P(),
        P(None, "lat", "lon"),
        P(),
        P(),
    )
    out_specs = (
        P(None, "lat", "lon"),
        P(None, "lat", "lon"),
        P(None, "lat", "lon"),
        P(None, "lat", "lon"),
    )

    def whole(*arrays):
        tables = circle_tables(arrays[0].shape[2])
        step = jax.shard_map(functools.partial(body, tables), mesh=mesh, in_specs=in_specs, out_specs=out_specs, check_vma=False)
        return step(*arrays)

    return whole
```

```python
import functools
import math

import ml_dtypes
import numpy as np
import jax
import jax.numpy as jnp
from jax import lax
from jax.experimental import pallas as pl
from jax.experimental.pallas import tpu as pltpu
from jax.sharding import PartitionSpec as P

SUBSTEPS = 2
FUSED_VMEM = 40 * 2 ** 20
FINISH_VMEM = 4 * 2 ** 20


def extended(block, sides, width):
    for axis, dim in sides:
        count = lax.axis_size(axis)
        forward = [(i, i + 1) for i in range(count - 1)]
        forward.append((count - 1, 0))
        backward = [(target, source) for source, target in forward]
        low = lax.ppermute(
            lax.slice_in_dim(block, block.shape[dim] - width, None, axis=dim), axis, forward
        )
        high = lax.ppermute(lax.slice_in_dim(block, 0, width, axis=dim), axis, backward)
        block = jnp.concatenate([low, block, high], axis=dim)
    return block


def rim_fix(padded, lat_dim):
    band_index = lax.axis_index("lat")
    bands = lax.axis_size("lat")
    extent = padded.shape[lat_dim]
    position = lax.broadcasted_iota(jnp.int32, padded.shape, lat_dim)
    first_edge = jnp.logical_and(position == 0, band_index == 0)
    final_edge = jnp.logical_and(position == extent - 1, band_index == bands - 1)
    return jnp.where(jnp.logical_or(first_edge, final_edge), 0.0, padded)


def dft_tables(length):
    half_len = length // 2
    sample = lax.broadcasted_iota(jnp.int32, (length, length), 0)
    column = lax.broadcasted_iota(jnp.int32, (length, length), 1)
    is_cosine = column <= half_len
    wavenum = jnp.where(is_cosine, column, column - half_len)
    phase = sample * wavenum % length
    angle = 2.0 * math.pi / length * phase.astype(jnp.float32)
    forward = jnp.where(is_cosine, jnp.cos(angle), jnp.sin(angle))
    single = jnp.logical_and(is_cosine, jnp.logical_or(wavenum == 0, wavenum == half_len))
    weight = jnp.where(single, 1.0, 2.0) / length
    inverse = jnp.transpose(forward * weight)
    wave_row = wavenum[0].astype(jnp.float32)
    return (forward, inverse, wave_row)


def damping(wave_row, limits):
    bound_col = limits[:, None]
    ratio = bound_col / jnp.maximum(wave_row[None, :], 1.0)
    return jnp.where(wave_row[None, :] > bound_col, ratio * ratio, 1.0)


def transform_band(block, limits, forward, inverse, wave_row):
    circles = lax.all_to_all(block, "lon", split_axis=1, concat_axis=3, tiled=True)
    spectra = jnp.einsum("vetj,jc->vetc", circles, forward, precision=lax.Precision.HIGHEST)
    scaled = spectra * damping(wave_row, limits)
    damped = jnp.einsum("vetc,cj->vetj", scaled, inverse, precision=lax.Precision.HIGHEST)
    return lax.all_to_all(damped, "lon", split_axis=3, concat_axis=1, tiled=True)


def filtered_increments(increments, own_flags, own_limits, forward, inverse, wave_row):
    flag_cols = own_flags[:, None]
    damped = transform_band(increments, own_limits, forward, inverse, wave_row)
    return jnp.where(flag_cols, damped, increments)


def column_solve(vertical_wind, pstar, level_coef, sound_coef):
    levels = vertical_wind.shape[0]
    zero_slab = jnp.zeros_like(vertical_wind[0])
    ratios = []
    values = []
    prev_ratio = zero_slab
    prev_value = zero_slab
    for level in range(levels):
        alpha = level_coef[level]
        below = alpha * sound_coef[level]
        if level + 1 < levels:
            above = alpha * sound_coef[level + 1]
            rhs = vertical_wind[level] - alpha * (pstar[level + 1] - pstar[level])
        else:
            above = zero_slab
            rhs = vertical_wind[level] + alpha * pstar[level]
        pivot = 1.0 + below + above + below * prev_ratio
        prev_ratio = -above / pivot
        prev_value = (rhs + below * prev_value) / pivot
        ratios.append(prev_ratio)
        values.append(prev_value)
    solved = [zero_slab] * levels
    upper_value = values[levels - 1]
    solved[levels - 1] = upper_value
    for level in range(levels - 2, -1, -1):
        upper_value = values[level] - ratios[level] * upper_value
        solved[level] = upper_value
    new_wind = jnp.stack(solved)
    wind_below = jnp.concatenate([zero_slab[None], new_wind[:-1]], axis=0)
    new_pressure = pstar - sound_coef * (new_wind - wind_below)
    return (new_wind, new_pressure)


def wide_body(
    zonal_wind,
    merid_wind,
    vertical_wind,
    pressure,
    zonal_coef,
    merid_coef,
    level_coef,
    sound_coef,
    cutoff,
    filter_mask,
):
    lat_rows = pressure.shape[1]
    start = lax.axis_index("lat") * lat_rows
    own_flags = lax.dynamic_slice_in_dim(filter_mask, start, lat_rows) > 0
    own_limits = lax.dynamic_slice_in_dim(cutoff, start, lat_rows).astype(jnp.float32)
    forward, inverse, wave_row = dft_tables(pressure.shape[2] * lax.axis_size("lon"))
    zonal_rows = zonal_coef[None, :, None]
    merid_rows = merid_coef[None, :, None]
    for step in range(SUBSTEPS):
        padded = extended(pressure, (("lat", 1), ("lon", 2)), 1)
        padded = rim_fix(padded, 1)
        zonal_step = -zonal_rows * (padded[:, 1:-1, 2:] - padded[:, 1:-1, :-2])
        merid_step = -merid_rows * (padded[:, 2:, 1:-1] - padded[:, :-2, 1:-1])
        increments = jnp.stack([zonal_step, merid_step])
        damped = filtered_increments(increments, own_flags, own_limits, forward, inverse, wave_row)
        winds = jnp.stack([zonal_wind, merid_wind]) + damped
        wind_pad = extended(winds, (("lat", 2), ("lon", 3)), 1)
        wind_pad = rim_fix(wind_pad, 2)
        diverge = zonal_rows * (wind_pad[0, :, 1:-1, 2:] - wind_pad[0, :, 1:-1, :-2])
        diverge = diverge + merid_rows * (wind_pad[1, :, 2:, 1:-1] - wind_pad[1, :, :-2, 1:-1])
        pstar = pressure - sound_coef * diverge
        vertical_wind, pressure = column_solve(vertical_wind, pstar, level_coef, sound_coef)
        zonal_wind = winds[0]
        merid_wind = winds[1]
    return (zonal_wind, merid_wind, vertical_wind, pressure)


LANE = 128
TILE = 2 * LANE


def circle_tables(length):
    blocks = length // LANE
    half = blocks // 2
    m = np.arange(LANE, dtype=np.float64)[:, None]
    c = np.arange(LANE)[None, :]
    angle = 2 * np.pi * ((m * c) % LANE) / LANE
    cos, sin = np.cos(angle) / np.sqrt(LANE), np.sin(angle) / np.sqrt(LANE)
    table = np.block([[cos, -sin], [sin, cos]])
    high = table.astype(ml_dtypes.bfloat16)
    rest = (table - high.astype(np.float64)).astype(ml_dtypes.bfloat16)
    rows = np.zeros((half + 1, 8, TILE), np.float32)
    for k1 in range(half + 1):
        k = k1 + blocks * c[0]
        waves = np.tile(np.minimum(k, length - k), 2)
        scale = (1.0 if k1 in (0, half) else 2.0) / blocks
        turn = 2 * np.pi * m[:, 0] * k1 / length
        rows[k1, 0] = waves
        rows[k1, 1] = 4.0 * np.sin(2 * np.pi * waves / length) ** 2
        rows[k1, 2] = np.where(np.arange(TILE) < LANE, scale, -scale)
        rows[k1, 3] = np.concatenate([np.cos(turn), np.sin(turn)])
    return np.stack([high, rest]), rows


def split_parts(value):
    high = value.astype(jnp.bfloat16)
    rest = (value - high.astype(jnp.float32)).astype(jnp.bfloat16)
    return high, rest


def three_products(value, table_ref):
    high, rest = split_parts(value)
    dims = (((1,), (0,)), ((), ()))
    rows = value.shape[0]
    table = table_ref[0]
    both = lax.dot_general(jnp.concatenate([high, rest], axis=0), table, dims, preferred_element_type=jnp.float32)
    corr = lax.dot_general(high, table_ref[1], dims, preferred_element_type=jnp.float32)
    return both[:rows] + (both[rows:] + corr)


def weighted(terms):
    total = None
    for coef, value in terms:
        if abs(coef) < 1e-12:
            continue
        if abs(abs(coef) - 1.0) < 1e-12:
            term = value
        else:
            term = abs(coef) * value
        if total is None:
            total = term if coef > 0 else -term
        else:
            total = total + term if coef > 0 else total - term
    return total


def coarse_forward(xs):
    count = len(xs)
    half = count // 2
    even = {b: xs[b] + xs[count - b] for b in range(1, half)}
    odd = {b: xs[b] - xs[count - b] for b in range(1, half)}
    real, imag = [], {}
    for k in range(half + 1):
        ends = xs[0] + xs[half] if k % 2 == 0 else xs[0] - xs[half]
        real.append(weighted([(1.0, ends)] + [(math.cos(2 * math.pi * b * k / count), even[b]) for b in range(1, half)]))
    for k in range(1, half):
        imag[k] = weighted([(-math.sin(2 * math.pi * b * k / count), odd[b]) for b in range(1, half)])
    pairs = [(real[0], real[half])] + [(real[k], imag[k]) for k in range(1, half)]
    return pairs


def coarse_inverse(pairs):
    half = len(pairs)
    count = 2 * half
    first, last = pairs[0]
    xs = [None] * count
    for b in range(half + 1):
        ends = first + last if b % 2 == 0 else first - last
        cos_part = weighted([(1.0, ends)] + [(math.cos(2 * math.pi * b * k / count), pairs[k][0]) for k in range(1, half)])
        if b in (0, half):
            xs[b] = cos_part
        else:
            sin_part = weighted([(-math.sin(2 * math.pi * b * k / count), pairs[k][1]) for k in range(1, half)])
            xs[b] = cos_part + sin_part
            xs[count - b] = cos_part - sin_part
    return xs


def whole_tiles(count):
    return -(-count // 16) * 16


def forward_fill(xs, rows_ref, work_ref, start):
    pairs = coarse_forward(xs)
    half = len(pairs)
    first, last = pairs[0]
    for t in range(half + 1):
        cos, sin = rows_ref[t, 3:4, :LANE], rows_ref[t, 3:4, LANE:]
        if t == 0:
            left, right = first, jnp.zeros_like(first)
        elif t == half:
            left, right = last * cos, -(last * sin)
        else:
            real, imag = pairs[t]
            left, right = real * cos + imag * sin, imag * cos - real * sin
        work_ref[start + 8 * t:start + 8 * t + 8, :LANE] = left
        work_ref[start + 8 * t:start + 8 * t + 8, LANE:] = right


def inverse_blocks(back_ref, rows_ref, start):
    half = rows_ref.shape[0] - 1
    pairs = []
    ends = []
    for t in range(half + 1):
        left = back_ref[start + 8 * t:start + 8 * t + 8, :LANE]
        right = back_ref[start + 8 * t:start + 8 * t + 8, LANE:]
        cos, sin = rows_ref[t, 3:4, :LANE], rows_ref[t, 3:4, LANE:]
        if t == 0:
            ends.append(left)
        elif t == half:
            ends.append(left * cos + right * sin)
        else:
            pairs.append((left * cos + right * sin, left * sin - right * cos))
    return coarse_inverse([tuple(ends)] + pairs)


def put_blocks(out_ref, xs, unit, units):
    split = out_ref.shape[2] // LANE
    for b, value in enumerate(xs):
        out_ref[(b // split) * units + unit, :, (b % split) * LANE:(b % split + 1) * LANE] = value


def circle_diff(xs):
    count = len(xs)
    lane = lax.broadcasted_iota(jnp.int32, xs[0].shape, 1)
    ahead = [pltpu.roll(x, LANE - 1, 1) for x in xs]
    behind = [pltpu.roll(x, 1, 1) for x in xs]
    out = []
    for b in range(count):
        nxt = jnp.where(lane == LANE - 1, ahead[(b + 1) % count], ahead[b])
        prv = jnp.where(lane == 0, behind[(b - 1) % count], behind[b])
        out.append(nxt - prv)
    return out


def border_rows(edge_ref, send_ref):
    for d in range(edge_ref.shape[0]):
        send_ref[d] = jnp.sum(pltpu.roll(edge_ref[d], 0, 1, stride=8, stride_axis=0), axis=0, keepdims=True)


def border_columns(row):
    value = jnp.broadcast_to(row, (8, LANE))
    place = lax.broadcasted_iota(jnp.int32, (8, LANE), 0)
    for bit in (1, 2, 4):
        value = jnp.where(place // bit % 2 == 1, pltpu.roll(value, LANE - 8 * bit, 1), value)
    return value


def border_tiles(edge_ref, xs, unit):
    count = len(xs)
    split = count // edge_ref.shape[0]
    lane = lax.broadcasted_iota(jnp.int32, xs[0].shape, 1)
    turned = [pltpu.roll(x, 2 * unit + 1, 1) for x in xs]
    for d in range(edge_ref.shape[0]):
        west, east = turned[(d * split - 1) % count], turned[(d * split + split) % count]
        kept = edge_ref[d] if unit else jnp.zeros_like(west)
        edge_ref[d] = jnp.where(lane == 2 * unit, west, jnp.where(lane == 2 * unit + 1, east, kept))


def filter_values(limit, wave, scale):
    quotient = limit / jnp.maximum(wave, 1.0)
    return jnp.where(wave > limit, quotient * quotient, 1.0) * scale


def filter_terms(rows_ref, own_ref, near_ref, filt_ref, side_ref):
    rows = own_ref.shape[1]
    zonal, merid, limit = own_ref[0, :, 0:1], own_ref[1, :, 0:1], own_ref[2, :, 0:1]
    for t in range(rows_ref.shape[0]):
        wave, sines, scale = rows_ref[t, 0:1, :], rows_ref[t, 1:2, :], rows_ref[t, 2:3, :]
        factor = filter_values(limit, wave, scale)
        filt_ref[t, 0] = factor
        filt_ref[t, 1] = merid * factor
        filt_ref[t, 2] = (zonal * zonal) * sines * factor
        south = near_ref[0, 1, rows - 1:rows, 0:1] * filter_values(near_ref[0, 2, rows - 1:rows, 0:1], wave, scale)
        north = near_ref[1, 1, 0:1, 0:1] * filter_values(near_ref[1, 2, 0:1, 0:1], wave, scale)
        side_ref[t, 0:1, :] = south
        side_ref[t, 1:2, :] = north


def merid_terms(spec_ref, unit, t, filt_ref, side_ref, south_ref, north_ref, at):
    tile = spec_ref.shape[1] // filt_ref.shape[0]
    own = spec_ref[unit, tile * t:tile * t + tile, :]
    row = lax.broadcasted_iota(jnp.int32, own.shape, 0)
    below_far, below = south_ref[at:at + 1, :], south_ref[at + 1:at + 2, :]
    above, above_far = north_ref[at:at + 1, :], north_ref[at + 1:at + 2, :]
    upper = jnp.where(row == tile - 1, above, pltpu.roll(own, tile - 1, 0))
    lower = jnp.where(row == 0, below, pltpu.roll(own, 1, 0))
    mid = -filt_ref[t, 1] * (upper - lower)
    v_south = -side_ref[t, 0:1, :] * (own[0:1] - below_far)
    v_north = -side_ref[t, 1:2, :] * (above_far - own[tile - 1:tile])
    return own, row, mid, v_south, v_north


def factor_columns(a_ref, s_ref, ratio_ref, inv_ref, gain_ref, carry_ref):
    levels = s_ref.shape[0]
    prev = jnp.zeros(s_ref.shape[1:], jnp.float32)
    for level in range(levels):
        alpha = a_ref[level]
        below = alpha * s_ref[level]
        above = alpha * s_ref[level + 1] if level + 1 < levels else jnp.zeros_like(below)
        inv = 1.0 / (1.0 + below + above + below * prev)
        prev = -above * inv
        ratio_ref[level] = prev
        inv_ref[level] = inv
        gain_ref[level] = alpha * inv
        carry_ref[level] = below * inv


def solve_columns(s_ref, winv_ref, p_ref, spread, ratio_ref, gain_ref, carry_ref, w_out, p_out):
    levels = s_ref.shape[0]

    def star(level):
        return p_ref[level] - s_ref[level] * spread(level)

    here = star(0)
    prev = jnp.zeros_like(here)
    for level in range(levels):
        p_out[level] = here
        nxt = star(level + 1) if level + 1 < levels else jnp.zeros_like(here)
        prev = (winv_ref[level] - gain_ref[level] * (nxt - here)) + carry_ref[level] * prev
        w_out[level] = prev
        here = nxt
    upper = w_out[levels - 1]
    for level in range(levels - 1, 0, -1):
        lower = w_out[level - 1] - ratio_ref[level - 1] * upper
        w_out[level - 1] = lower
        p_out[level] = p_out[level] - s_ref[level] * (upper - lower)
        upper = lower
    p_out[0] = p_out[0] - s_ref[0] * upper


def paired_rows(first, second, inner):
    row = lax.broadcasted_iota(jnp.int32, first.shape, 0)
    rows = first.shape[0]
    shift = 2 if not inner else rows - 2
    return jnp.where(row < rows // 2, pltpu.roll(first, shift, 0), pltpu.roll(second, rows - shift, 0))


def unpaired_rows(tile, second, inner):
    rows = tile.shape[0]
    row = lax.broadcasted_iota(jnp.int32, tile.shape, 0)
    middle = jnp.logical_and(row >= 2, row < rows - 2)
    shift = rows - 2 if second == inner else 2
    moved = pltpu.roll(tile, shift, 0)
    return jnp.where(middle, moved, 0.0) if inner else jnp.where(middle, 0.0, moved)


def divergence(u, v, zonal, merid, west, east, south, north):
    rows, width = u.shape
    lane = lax.broadcasted_iota(jnp.int32, (rows, width), 1)
    row = lax.broadcasted_iota(jnp.int32, (rows, width), 0)
    ahead = jnp.where(lane == width - 1, east, pltpu.roll(u, width - 1, 1))
    behind = jnp.where(lane == 0, west, pltpu.roll(u, 1, 1))
    upper = jnp.where(row == rows - 1, north, pltpu.roll(v, rows - 1, 0))
    lower = jnp.where(row == 0, south, pltpu.roll(v, 1, 0))
    return zonal * (ahead - behind) + merid * (upper - lower)


def base_divergence(u_ref, v_ref, own_ref, west_ref, east_ref, south_ref, north_ref, base_ref, is_first, is_last):
    zonal, merid = own_ref[0, :, 0:1], own_ref[1, :, 0:1]
    keep_south = jnp.where(is_first, 0.0, 1.0)
    keep_north = jnp.where(is_last, 0.0, 1.0)
    west = west_ref[...]
    east = east_ref[...]
    for level in range(u_ref.shape[0]):
        base_ref[level] = divergence(
            u_ref[level], v_ref[level], zonal, merid, west[:, level:level + 1], east[:, level:level + 1],
            keep_south * south_ref[level:level + 1, :], keep_north * north_ref[level:level + 1, :],
        )


def added_divergence(ur, vr, own_ref, base_ref, levels):
    zonal, merid = own_ref[0, :, 0:1], own_ref[1, :, 0:1]
    for level in levels:
        base_ref[level] = base_ref[level] + divergence(ur[level], vr[level], zonal, merid, 0.0, 0.0, 0.0, 0.0)


def added_borders(own_ref, border_ref, base_ref, units):
    zonal = own_ref[0, :, 0:1]
    width = base_ref.shape[2]
    lane = lax.broadcasted_iota(jnp.int32, (8, LANE), 1)
    for d in range(border_ref.shape[0]):
        border = border_columns(border_ref[d])
        for l in range(units):
            level = d * units + l
            west = jnp.where(lane == 0, zonal * border[:, 2 * l:2 * l + 1], 0.0)
            east = jnp.where(lane == LANE - 1, zonal * border[:, 2 * l + 1:2 * l + 2], 0.0)
            base_ref[level, :, :LANE] = base_ref[level, :, :LANE] - west
            base_ref[level, :, width - LANE:] = base_ref[level, :, width - LANE:] + east


def pack_edges(u_ref, v_ref, first_col, last_col, first_row, last_row):
    rows, width = u_ref.shape[1:]
    lane = lax.broadcasted_iota(jnp.int32, (rows, LANE), 1)
    first = jnp.zeros((rows, LANE), jnp.float32)
    last = jnp.zeros((rows, LANE), jnp.float32)
    for level in range(u_ref.shape[0]):
        first = jnp.where(lane == level, u_ref[level, :, 0:1], first)
        last = jnp.where(lane == level, u_ref[level, :, width - 1:width], last)
        first_row[level:level + 1, :] = v_ref[level, 0:1, :]
        last_row[level:level + 1, :] = v_ref[level, rows - 1:rows, :]
    first_col[...] = first
    last_col[...] = last


def pack_halo(source, low, high, units):
    rows = source.shape[1]
    for g in range(low.shape[0]):
        for l in range(units):
            low[g, 2 * l:2 * l + 2, :] = source[g * units + l, 0:2, :]
            high[g, 2 * l:2 * l + 2, :] = source[g * units + l, rows - 2:rows, :]


def own_coefs(zc_ref, mc_ref, cutoff_ref, mask_ref, own_ref, first_lat, unfiltered):
    rows = own_ref.shape[1]
    row = lax.broadcasted_iota(jnp.int32, own_ref.shape[1:], 0)
    zonal = jnp.zeros(own_ref.shape[1:], jnp.float32)
    merid = jnp.zeros(own_ref.shape[1:], jnp.float32)
    limit = jnp.zeros(own_ref.shape[1:], jnp.int32)
    for r in range(rows):
        zonal = jnp.where(row == r, zc_ref[r], zonal)
        merid = jnp.where(row == r, mc_ref[r], merid)
        filtered = mask_ref[first_lat + r]
        bound = filtered * cutoff_ref[first_lat + r] + (1 - filtered) * unfiltered
        limit = jnp.where(row == r, bound, limit)
    own_ref[0] = zonal
    own_ref[1] = merid
    own_ref[2] = limit.astype(jnp.float32)


def flipped(index, mask):
    bit = 1
    while bit <= mask:
        if mask & bit:
            index = index + bit * (1 - 2 * (index // bit % 2))
        bit *= 2
    return index


def partner_masks(count):
    return sorted(range(1, count), key=lambda mask: (-bin(mask // 2).count("1"), -(mask % 2), -mask))


def fused_kernel(
    bands, per_band, a_far, zc_far, mc_far, cutoff_far, mask_far, u_far, v_far, w_far, p_far, s_far, table_far, rows_far,
    u_out, v_out, base, winv, p_mid, s_ref, ratio, gain, carry, own_ref, rim_recv,
    x1, x2, d1, ur, vr, ds1, us, vs, w_mid, inv, u_ref, v_ref, w_ref, p_ref,
    halo1, low, high, chain_send, chain_recv, table_ref, rows_ref, spec, work, back, filt, sides,
    near, cols_send, cols_recv, rows_send, rows_recv, border_tile, border_send, border_recv, rim_send,
    a_ref, zc_ref, mc_ref, cutoff_ref, mask_ref,
    load_sems, send_sems, recv_sems, edge_send, edge_recv, halo_send, halo_recv, last_send, last_recv, chain_out, chain_in, band_in,
):
    band_me = lax.axis_index("lat")
    lon_me = lax.axis_index("lon")
    lat_rows = u_ref.shape[1]
    units = u_ref.shape[0] // per_band
    channels = rows_ref.shape[0]
    half = channels - 1
    per_unit = channels * lat_rows
    split = u_ref.shape[2] // LANE
    mesh_id = pl.DeviceIdType.MESH
    is_first = band_me == 0
    is_last = band_me == bands - 1
    not_first = jnp.logical_not(is_first)
    not_last = jnp.logical_not(is_last)
    masks = partner_masks(per_band)
    partners = [flipped(lon_me, mask) for mask in masks]

    pairs = (
        (p_far, p_ref), (zc_far, zc_ref), (mc_far, mc_ref), (cutoff_far, cutoff_ref), (mask_far, mask_ref), (a_far, a_ref),
        (rows_far, rows_ref), (u_far, u_ref), (v_far, v_ref), (table_far, table_ref), (s_far, s_ref), (w_far, w_ref),
    )
    loads = [pltpu.make_async_copy(far, here, load_sems.at[n]) for n, (far, here) in enumerate(pairs)]
    for load in loads:
        load.start()
    barrier = pltpu.get_barrier_semaphore()

    def greet(band, lon):
        pl.semaphore_signal(barrier, inc=1, device_id=(band, lon), device_id_type=mesh_id)

    for partner in partners:
        greet(band_me, partner)
    for there, step in ((not_first, -1), (not_last, 1)):
        @pl.when(there)
        def _():
            greet(band_me + step, lon_me)

    loads[0].wait()
    pack_halo(p_ref, low, high, units)
    pl.semaphore_wait(barrier, per_band - 1 + jnp.where(is_first, 0, 1) + jnp.where(is_last, 0, 1))
    for there, step, place in ((not_first, -1, 1), (not_last, 1, 0)):
        @pl.when(there)
        def _():
            pl.semaphore_signal(band_in.at[place], inc=1, device_id=(band_me + step, lon_me), device_id_type=mesh_id)


    def scatter(source, target, sem, unit, count=1):
        for g in partners:
            pltpu.make_async_remote_copy(
                src_ref=source.at[pl.ds(g * units + unit, count)], dst_ref=target.at[pl.ds(lon_me * units + unit, count)],
                send_sem=send_sems.at[sem], recv_sem=recv_sems.at[sem, unit],
                device_id=(band_me, g), device_id_type=mesh_id,
            ).start()
        for n in range(count):
            target[lon_me * units + unit + n] = source[lon_me * units + unit + n]

    def gathered(target, sem, unit, count=1):
        block = target.at[pl.ds(0, (per_band - 1) * count)]
        pltpu.make_async_copy(block, block, recv_sems.at[sem, unit]).wait()

    def sent(source, sem):
        block = source.at[pl.ds(0, (per_band - 1) * units)]
        pltpu.make_async_copy(block, block, send_sems.at[sem]).wait()

    def spread_halo(target):
        def one(source, slot, sem, other):
            for g in partners + [lon_me]:
                pltpu.make_async_remote_copy(
                    src_ref=source.at[g], dst_ref=target.at[slot, lon_me],
                    send_sem=halo_send.at[sem], recv_sem=halo_recv.at[sem],
                    device_id=(other, g), device_id_type=mesh_id,
                ).start()

        @pl.when(not_first)
        def _():
            pl.semaphore_wait(band_in.at[0], 1)
            one(low, 1, 0, band_me - 1)

        @pl.when(not_last)
        def _():
            pl.semaphore_wait(band_in.at[1], 1)
            one(high, 0, 1, band_me + 1)

    def halo_wait(sems, upward):
        @pl.when(not_first)
        def _():
            pltpu.make_async_copy(low, low, sems.at[0 if upward else 1]).wait()

        @pl.when(not_last)
        def _():
            pltpu.make_async_copy(low, low, sems.at[1 if upward else 0]).wait()

    def chain_copy(unit, side):
        return pltpu.make_async_remote_copy(
            src_ref=chain_send.at[side, unit], dst_ref=chain_recv.at[side, unit],
            send_sem=chain_out.at[side], recv_sem=chain_in.at[side, unit],
            device_id=((band_me + bands + 1 - 2 * side) % bands, lon_me), device_id_type=mesh_id,
        )

    def coef_copy(step, side):
        return pltpu.make_async_remote_copy(
            src_ref=own_ref, dst_ref=near.at[side], send_sem=edge_send.at[4 + side], recv_sem=edge_recv.at[4 + side],
            device_id=((band_me + bands + step) % bands, lon_me), device_id_type=mesh_id,
        )

    for unit in range(units):
        scatter(p_ref, x1, 0, unit)
    spread_halo(halo1)

    for load in loads[1:7]:
        load.wait()
    own_coefs(zc_ref, mc_ref, cutoff_ref, mask_ref, own_ref, band_me * lat_rows, half * TILE)

    @pl.when(not_first)
    def _():
        coef_copy(-1, 1).start()

    @pl.when(not_last)
    def _():
        coef_copy(1, 0).start()

    @pl.when(is_first)
    def _():
        near[0] = jnp.zeros(near.shape[1:], jnp.float32)
        chain_recv[0] = jnp.zeros(chain_recv.shape[1:], jnp.float32)
        for g in range(per_band):
            halo1[0, g] = jnp.zeros(halo1.shape[2:], jnp.float32)

    @pl.when(is_last)
    def _():
        near[1] = jnp.zeros(near.shape[1:], jnp.float32)
        chain_recv[1] = jnp.zeros(chain_recv.shape[1:], jnp.float32)
        for g in range(per_band):
            halo1[1, g] = jnp.zeros(halo1.shape[2:], jnp.float32)

    work[...] = jnp.zeros(work.shape, jnp.float32)
    for load in loads[7:9]:
        load.wait()
    pack_edges(u_ref, v_ref, cols_send.at[0], cols_send.at[1], rows_send.at[0], rows_send.at[1])
    edge_copies = []
    for side, step in ((0, -1), (1, 1)):
        edge_copies.append(pltpu.make_async_remote_copy(
            src_ref=cols_send.at[side], dst_ref=cols_recv.at[side], send_sem=edge_send.at[side], recv_sem=edge_recv.at[side],
            device_id=(band_me, (lon_me + per_band + step) % per_band), device_id_type=mesh_id,
        ))
    for copy in edge_copies:
        copy.start()

    def row_copy(step, side):
        return pltpu.make_async_remote_copy(
            src_ref=rows_send.at[side], dst_ref=rows_recv.at[side], send_sem=edge_send.at[2 + side], recv_sem=edge_recv.at[2 + side],
            device_id=((band_me + bands + step) % bands, lon_me), device_id_type=mesh_id,
        )

    @pl.when(not_first)
    def _():
        row_copy(-1, 0).start()

    @pl.when(not_last)
    def _():
        row_copy(1, 1).start()

    @pl.when(is_first)
    def _():
        rows_recv[1] = jnp.zeros(rows_recv.shape[1:], jnp.float32)

    @pl.when(is_last)
    def _():
        rows_recv[0] = jnp.zeros(rows_recv.shape[1:], jnp.float32)

    for load in loads[9:]:
        load.wait()
    factor_columns(a_ref, s_ref, ratio, inv, gain, carry)
    for level in range(s_ref.shape[0]):
        winv[level] = w_ref[level] * inv[level]

    @pl.when(not_first)
    def _():
        coef_copy(1, 0).wait_recv()

    @pl.when(not_last)
    def _():
        coef_copy(-1, 1).wait_recv()

    filter_terms(rows_ref, own_ref, near, filt, sides)

    def circles(source, first, count, stride):
        return [
            [source[d * stride + first + n, :, h * LANE:(h + 1) * LANE] for d in range(per_band) for h in range(split)]
            for n in range(count)
        ]

    def forward(tiles, places, accumulate):
        for n, xs in enumerate(tiles):
            forward_fill(xs, rows_ref, work, n * per_unit)
        used = len(tiles) * per_unit
        value = three_products(work[0:whole_tiles(used), :], table_ref)
        for n, place in enumerate(places):
            part = value[n * per_unit:(n + 1) * per_unit]
            spec[place] = spec[place] + part if accumulate else part

    def inverse(count):
        back[0:whole_tiles(count * per_unit), :] = three_products(work[0:whole_tiles(count * per_unit), :], table_ref)

    halo_wait(halo_recv, False)
    forward([
        [halo1[slot, d, :, h * LANE:(h + 1) * LANE] for d in range(per_band) for h in range(split)] for slot in range(2)
    ], [units, units + 1], False)
    for unit in range(units):
        gathered(x1, 0, unit)
        forward(circles(x1, unit, 1, units), [unit], False)
        for t in range(channels):
            at = lat_rows * t + 2 * unit
            own, row, mid, v_south, v_north = merid_terms(spec, unit, t, filt, sides, spec.at[units], spec.at[units + 1], at)
            upper = jnp.where(row == lat_rows - 1, v_north, pltpu.roll(mid, lat_rows - 1, 0))
            lower = jnp.where(row == 0, v_south, pltpu.roll(mid, 1, 0))
            merid = own_ref[1, :, 0:1]
            work[lat_rows * t:lat_rows * (t + 1), :] = filt[t, 2] * own + merid * (upper - lower)
        inverse(1)
        put_blocks(ds1, inverse_blocks(back, rows_ref, 0), unit, units)
        scatter(ds1, d1, 1, unit)

    for copy in edge_copies:
        copy.wait_recv()

    @pl.when(not_first)
    def _():
        row_copy(1, 1).wait_recv()

    @pl.when(not_last)
    def _():
        row_copy(-1, 0).wait_recv()

    base_divergence(
        u_ref, v_ref, own_ref, cols_recv.at[1], cols_recv.at[0], rows_recv.at[1], rows_recv.at[0], base,
        is_first, is_last,
    )
    for unit in range(units):
        gathered(d1, 1, unit)

    def first_spread(level):
        return base[level] + d1[level]

    solve_columns(s_ref, winv, p_ref, first_spread, ratio, gain, carry, vs, p_mid)
    for unit in range(units):
        scatter(p_mid, x2, 2, unit)
    for level in range(s_ref.shape[0]):
        winv[level] = vs[level] * inv[level]

    zonal = own_ref[0, :, 0:1]
    for unit in range(units):
        gathered(x2, 2, unit)
        forward(circles(x2, unit, 1, units), [unit], True)
        for t in range(channels):
            at = lat_rows * t
            chain_send[0, unit, 2 * t:2 * t + 2, :] = spec[unit, at + lat_rows - 2:at + lat_rows, :]
            chain_send[1, unit, 2 * t:2 * t + 2, :] = spec[unit, at:at + 2, :]

        @pl.when(not_last)
        def _():
            chain_copy(unit, 0).start()

        @pl.when(not_first)
        def _():
            chain_copy(unit, 1).start()

        for t in range(channels):
            at = lat_rows * t
            work[at:at + lat_rows, :] = filt[t, 0] * spec[unit, at:at + lat_rows, :]
        inverse(1)
        moved = [-zonal * x for x in circle_diff(inverse_blocks(back, rows_ref, 0))]
        put_blocks(us, moved, unit, units)
        scatter(us, ur, 3, unit)
        border_tiles(border_tile, moved, unit)
    border_rows(border_tile, border_send)

    def last_copy(source, target, n, g):
        return pltpu.make_async_remote_copy(
            src_ref=source.at[pl.ds(g, 1)], dst_ref=target.at[pl.ds(lon_me, 1)], send_sem=last_send.at[n], recv_sem=last_recv.at[n],
            device_id=(band_me, g), device_id_type=mesh_id,
        )

    def last_scatter(source, target, n):
        for g in partners:
            last_copy(source, target, n, g).start()
        target[lon_me] = source[lon_me]

    last_scatter(border_send, border_recv, 0)
    rim_at = per_unit
    for unit in range(units):
        @pl.when(not_first)
        def _():
            chain_copy(unit, 0).wait_recv()

        @pl.when(not_last)
        def _():
            chain_copy(unit, 1).wait_recv()

        for t in range(channels):
            own, row, mid, v_south, v_north = merid_terms(
                spec, unit, t, filt, sides, chain_recv.at[0, unit], chain_recv.at[1, unit], 2 * t,
            )
            work[lat_rows * t:lat_rows * (t + 1), :] = mid
            rim = rim_at + lat_rows * t + 2 * unit
            work[rim:rim + 1, :] = v_south
            work[rim + 1:rim + 2, :] = v_north
        inverse(2 if unit == units - 1 else 1)
        put_blocks(vs, inverse_blocks(back, rows_ref, 0), unit, units)
        scatter(vs, vr, 4, unit)
    rims = inverse_blocks(back, rows_ref, rim_at)
    for b, value in enumerate(rims):
        rim_send[b // split, :, (b % split) * LANE:(b % split + 1) * LANE] = value

    last_scatter(rim_send, rim_recv, 1)

    def last_wait(target, sems, n):
        block = target.at[pl.ds(0, per_band - 1)]
        pltpu.make_async_copy(block, block, sems.at[n]).wait()

    for unit in range(units):
        gathered(ur, 3, unit)
        for d in range(per_band):
            level = d * units + unit
            u_out[level] = u_ref[level] + ur[level]
    last_wait(border_recv, last_recv, 0)
    added_borders(own_ref, border_recv, base, units)
    for unit in range(units):
        gathered(vr, 4, unit)
        own_levels = [d * units + unit for d in range(per_band)]
        for level in own_levels:
            v_out[level] = v_ref[level] + vr[level]
        added_divergence(ur, vr, own_ref, base, own_levels)
    last_wait(rim_recv, last_recv, 1)
    for source, sem in ((p_ref, 0), (ds1, 1), (p_mid, 2), (us, 3), (vs, 4)):
        sent(source, sem)
    last_wait(border_send, last_send, 0)
    last_wait(rim_send, last_send, 1)
    halo_wait(halo_send, True)
    for copy in edge_copies:
        copy.wait_send()

    @pl.when(not_first)
    def _():
        pltpu.make_async_copy(chain_send.at[1], chain_send.at[1], chain_out.at[1]).wait()
        coef_copy(-1, 1).wait_send()
        row_copy(-1, 0).wait_send()

    @pl.when(not_last)
    def _():
        pltpu.make_async_copy(chain_send.at[0], chain_send.at[0], chain_out.at[0]).wait()
        coef_copy(1, 0).wait_send()
        row_copy(1, 1).wait_send()


def deliver_kernel(
    units, u_ref, v_ref, base, winv, p_mid, s_ref, ratio, gain, carry, own_ref, rim_ref, u_out, v_out, w_out, p_out, w_end, p_end, sems,
):
    copies = [
        pltpu.make_async_copy(source, target, sems.at[n])
        for n, (source, target) in enumerate(((u_ref, u_out), (v_ref, v_out), (w_end, w_out), (p_end, p_out)))
    ]
    copies[0].start()
    copies[1].start()
    row = lax.broadcasted_iota(jnp.int32, u_ref.shape[1:], 0)
    rows = u_ref.shape[1]
    merid = own_ref[1, :, 0:1]
    south = jnp.where(row == 0, -merid, 0.0)
    north = jnp.where(row == rows - 1, merid, 0.0)

    def spread(level):
        d, l = level // units, 2 * (level % units)
        return base[level] + south * rim_ref[d, l:l + 1, :] + north * rim_ref[d, l + 1:l + 2, :]

    solve_columns(s_ref, winv, p_mid, spread, ratio, gain, carry, w_end, p_end)
    copies[2].start()
    copies[3].start()
    for copy in copies:
        copy.wait()


def deliver(units, arrays):
    shape = arrays[0].shape
    return pl.pallas_call(
        functools.partial(deliver_kernel, units),
        out_shape=(jax.ShapeDtypeStruct(shape, jnp.float32),) * 4,
        in_specs=[pl.BlockSpec(memory_space=pltpu.VMEM)] * len(arrays),
        out_specs=(pl.BlockSpec(memory_space=pl.ANY),) * 4,
        scratch_shapes=[pltpu.VMEM(shape, jnp.float32)] * 2 + [pltpu.SemaphoreType.DMA((4,))],
        compiler_params=pltpu.CompilerParams(vmem_limit_bytes=FINISH_VMEM),
    )(*arrays)


def level_body(
    tables,
    zonal_wind,
    merid_wind,
    vertical_wind,
    pressure,
    zonal_coef,
    merid_coef,
    level_coef,
    sound_coef,
    cutoff,
    filter_mask,
):
    table, rows = (jnp.asarray(t) for t in tables)
    channels = rows.shape[0]
    bands = lax.axis_size("lat")
    per_band = lax.axis_size("lon")
    levels, lat_rows, width = pressure.shape
    units = levels // per_band
    per_unit = channels * lat_rows
    vmem = pl.BlockSpec(memory_space=pltpu.VMEM)
    far = pl.BlockSpec(memory_space=pl.ANY)

    def scratch(*shape):
        return pltpu.VMEM(shape, jnp.float32)

    field = scratch(*pressure.shape)
    halo = scratch(2, per_band, lat_rows, width)
    chain = scratch(2, units, -(-2 * channels // 8) * 8, TILE)
    spare = scratch(whole_tiles(2 * per_unit), TILE)
    dma = pltpu.SemaphoreType.DMA
    operands = (
        level_coef, zonal_coef, merid_coef, cutoff, filter_mask,
        zonal_wind, merid_wind, vertical_wind, pressure, sound_coef, table, rows,
    )
    results = pl.pallas_call(
        functools.partial(fused_kernel, bands, per_band),
        out_shape=(pltpu.VMEM(pressure.shape, jnp.float32),) * 9 + (
            pltpu.VMEM((3, lat_rows, LANE), jnp.float32), pltpu.VMEM((per_band, lat_rows, width), jnp.float32),
        ),
        in_specs=[far] * len(operands),
        out_specs=(vmem,) * 11,
        scratch_shapes=[field] * 14 + [halo, scratch(per_band, lat_rows, width), scratch(per_band, lat_rows, width), chain, chain] + [
            pltpu.VMEM(table.shape, table.dtype), scratch(*rows.shape),
            scratch(units + 2, per_unit, TILE), spare, spare,
            scratch(channels, 3, lat_rows, TILE), scratch(channels, 8, TILE),
            scratch(2, 3, lat_rows, LANE),
            scratch(2, lat_rows, LANE), scratch(2, lat_rows, LANE),
            scratch(2, levels, width), scratch(2, levels, width),
            scratch(per_band, lat_rows, LANE), scratch(per_band, 1, LANE), scratch(per_band, 1, LANE),
            scratch(per_band, lat_rows, width),
            pltpu.SMEM(level_coef.shape, jnp.float32), pltpu.SMEM(zonal_coef.shape, jnp.float32),
            pltpu.SMEM(merid_coef.shape, jnp.float32), pltpu.SMEM(cutoff.shape, jnp.int32),
            pltpu.SMEM(filter_mask.shape, jnp.int32),
            dma((len(operands),)), dma((5,)), dma((5, units)), dma((6,)), dma((6,)), dma((2,)), dma((2,)), dma((2,)), dma((2,)), dma((2,)), dma((2, units)),
            pltpu.SemaphoreType.REGULAR((2,)),
        ],
        compiler_params=pltpu.CompilerParams(collective_id=0, has_side_effects=True, vmem_limit_bytes=FUSED_VMEM),
    )(*[pltpu.with_memory_space_constraint(x, pltpu.HBM) for x in operands])
    return deliver(units, results)


def body(tables, *arrays):
    pressure = arrays[3]
    per_band = lax.axis_size("lon")
    levels, lat_rows, width = pressure.shape
    fits = lat_rows == 8 and levels == 4 * per_band and levels <= LANE and width % LANE == 0 and per_band & (per_band - 1) == 0
    if fits:
        return level_body(tables, *arrays)
    return wide_body(*arrays)


def solution(mesh):
    in_specs = (
        P(None, "lat", "lon"),
        P(None, "lat", "lon"),
        P(None, "lat", "lon"),
        P(None, "lat", "lon"),
        P("lat"),
        P("lat"),
        P(),
        P(None, "lat", "lon"),
        P(),
        P(),
    )
    out_specs = (
        P(None, "lat", "lon"),
        P(None, "lat", "lon"),
        P(None, "lat", "lon"),
        P(None, "lat", "lon"),
    )

    def whole(*arrays):
        tables = circle_tables(arrays[0].shape[2])
        step = jax.shard_map(functools.partial(body, tables), mesh=mesh, in_specs=in_specs, out_specs=out_specs, check_vma=False)
        return step(*arrays)

    return whole
```

```python
import functools
import math

import ml_dtypes
import numpy as np
import jax
import jax.numpy as jnp
from jax import lax
from jax.experimental import pallas as pl
from jax.experimental.pallas import tpu as pltpu
from jax.sharding import PartitionSpec as P

SUBSTEPS = 2
FUSED_VMEM = 40 * 2 ** 20
FINISH_VMEM = 4 * 2 ** 20


def extended(block, sides, width):
    for axis, dim in sides:
        count = lax.axis_size(axis)
        forward = [(i, i + 1) for i in range(count - 1)]
        forward.append((count - 1, 0))
        backward = [(target, source) for source, target in forward]
        low = lax.ppermute(
            lax.slice_in_dim(block, block.shape[dim] - width, None, axis=dim), axis, forward
        )
        high = lax.ppermute(lax.slice_in_dim(block, 0, width, axis=dim), axis, backward)
        block = jnp.concatenate([low, block, high], axis=dim)
    return block


def rim_fix(padded, lat_dim):
    band_index = lax.axis_index("lat")
    bands = lax.axis_size("lat")
    extent = padded.shape[lat_dim]
    position = lax.broadcasted_iota(jnp.int32, padded.shape, lat_dim)
    first_edge = jnp.logical_and(position == 0, band_index == 0)
    final_edge = jnp.logical_and(position == extent - 1, band_index == bands - 1)
    return jnp.where(jnp.logical_or(first_edge, final_edge), 0.0, padded)


def dft_tables(length):
    half_len = length // 2
    sample = lax.broadcasted_iota(jnp.int32, (length, length), 0)
    column = lax.broadcasted_iota(jnp.int32, (length, length), 1)
    is_cosine = column <= half_len
    wavenum = jnp.where(is_cosine, column, column - half_len)
    phase = sample * wavenum % length
    angle = 2.0 * math.pi / length * phase.astype(jnp.float32)
    forward = jnp.where(is_cosine, jnp.cos(angle), jnp.sin(angle))
    single = jnp.logical_and(is_cosine, jnp.logical_or(wavenum == 0, wavenum == half_len))
    weight = jnp.where(single, 1.0, 2.0) / length
    inverse = jnp.transpose(forward * weight)
    wave_row = wavenum[0].astype(jnp.float32)
    return (forward, inverse, wave_row)


def damping(wave_row, limits):
    bound_col = limits[:, None]
    ratio = bound_col / jnp.maximum(wave_row[None, :], 1.0)
    return jnp.where(wave_row[None, :] > bound_col, ratio * ratio, 1.0)


def transform_band(block, limits, forward, inverse, wave_row):
    circles = lax.all_to_all(block, "lon", split_axis=1, concat_axis=3, tiled=True)
    spectra = jnp.einsum("vetj,jc->vetc", circles, forward, precision=lax.Precision.HIGHEST)
    scaled = spectra * damping(wave_row, limits)
    damped = jnp.einsum("vetc,cj->vetj", scaled, inverse, precision=lax.Precision.HIGHEST)
    return lax.all_to_all(damped, "lon", split_axis=3, concat_axis=1, tiled=True)


def filtered_increments(increments, own_flags, own_limits, forward, inverse, wave_row):
    flag_cols = own_flags[:, None]
    damped = transform_band(increments, own_limits, forward, inverse, wave_row)
    return jnp.where(flag_cols, damped, increments)


def column_solve(vertical_wind, pstar, level_coef, sound_coef):
    levels = vertical_wind.shape[0]
    zero_slab = jnp.zeros_like(vertical_wind[0])
    ratios = []
    values = []
    prev_ratio = zero_slab
    prev_value = zero_slab
    for level in range(levels):
        alpha = level_coef[level]
        below = alpha * sound_coef[level]
        if level + 1 < levels:
            above = alpha * sound_coef[level + 1]
            rhs = vertical_wind[level] - alpha * (pstar[level + 1] - pstar[level])
        else:
            above = zero_slab
            rhs = vertical_wind[level] + alpha * pstar[level]
        pivot = 1.0 + below + above + below * prev_ratio
        prev_ratio = -above / pivot
        prev_value = (rhs + below * prev_value) / pivot
        ratios.append(prev_ratio)
        values.append(prev_value)
    solved = [zero_slab] * levels
    upper_value = values[levels - 1]
    solved[levels - 1] = upper_value
    for level in range(levels - 2, -1, -1):
        upper_value = values[level] - ratios[level] * upper_value
        solved[level] = upper_value
    new_wind = jnp.stack(solved)
    wind_below = jnp.concatenate([zero_slab[None], new_wind[:-1]], axis=0)
    new_pressure = pstar - sound_coef * (new_wind - wind_below)
    return (new_wind, new_pressure)


def wide_body(
    zonal_wind,
    merid_wind,
    vertical_wind,
    pressure,
    zonal_coef,
    merid_coef,
    level_coef,
    sound_coef,
    cutoff,
    filter_mask,
):
    lat_rows = pressure.shape[1]
    start = lax.axis_index("lat") * lat_rows
    own_flags = lax.dynamic_slice_in_dim(filter_mask, start, lat_rows) > 0
    own_limits = lax.dynamic_slice_in_dim(cutoff, start, lat_rows).astype(jnp.float32)
    forward, inverse, wave_row = dft_tables(pressure.shape[2] * lax.axis_size("lon"))
    zonal_rows = zonal_coef[None, :, None]
    merid_rows = merid_coef[None, :, None]
    for step in range(SUBSTEPS):
        padded = extended(pressure, (("lat", 1), ("lon", 2)), 1)
        padded = rim_fix(padded, 1)
        zonal_step = -zonal_rows * (padded[:, 1:-1, 2:] - padded[:, 1:-1, :-2])
        merid_step = -merid_rows * (padded[:, 2:, 1:-1] - padded[:, :-2, 1:-1])
        increments = jnp.stack([zonal_step, merid_step])
        damped = filtered_increments(increments, own_flags, own_limits, forward, inverse, wave_row)
        winds = jnp.stack([zonal_wind, merid_wind]) + damped
        wind_pad = extended(winds, (("lat", 2), ("lon", 3)), 1)
        wind_pad = rim_fix(wind_pad, 2)
        diverge = zonal_rows * (wind_pad[0, :, 1:-1, 2:] - wind_pad[0, :, 1:-1, :-2])
        diverge = diverge + merid_rows * (wind_pad[1, :, 2:, 1:-1] - wind_pad[1, :, :-2, 1:-1])
        pstar = pressure - sound_coef * diverge
        vertical_wind, pressure = column_solve(vertical_wind, pstar, level_coef, sound_coef)
        zonal_wind = winds[0]
        merid_wind = winds[1]
    return (zonal_wind, merid_wind, vertical_wind, pressure)


LANE = 128
TILE = 2 * LANE


def circle_tables(length):
    blocks = length // LANE
    half = blocks // 2
    m = np.arange(LANE, dtype=np.float64)[:, None]
    c = np.arange(LANE)[None, :]
    angle = 2 * np.pi * ((m * c) % LANE) / LANE
    cos, sin = np.cos(angle) / np.sqrt(LANE), np.sin(angle) / np.sqrt(LANE)
    table = np.block([[cos, -sin], [sin, cos]])
    high = table.astype(ml_dtypes.bfloat16)
    rest = (table - high.astype(np.float64)).astype(ml_dtypes.bfloat16)
    rows = np.zeros((half + 1, 8, TILE), np.float32)
    for k1 in range(half + 1):
        k = k1 + blocks * c[0]
        waves = np.tile(np.minimum(k, length - k), 2)
        scale = (1.0 if k1 in (0, half) else 2.0) / blocks
        turn = 2 * np.pi * m[:, 0] * k1 / length
        rows[k1, 0] = waves
        rows[k1, 1] = 4.0 * np.sin(2 * np.pi * waves / length) ** 2
        rows[k1, 2] = np.where(np.arange(TILE) < LANE, scale, -scale)
        rows[k1, 3] = np.concatenate([np.cos(turn), np.sin(turn)])
    return np.stack([high, rest]), rows


def split_parts(value):
    high = value.astype(jnp.bfloat16)
    rest = (value - high.astype(jnp.float32)).astype(jnp.bfloat16)
    return high, rest


def three_products(value, table_ref):
    high, rest = split_parts(value)
    dims = (((1,), (0,)), ((), ()))
    rows = value.shape[0]
    table = table_ref[0]
    both = lax.dot_general(jnp.concatenate([high, rest], axis=0), table, dims, preferred_element_type=jnp.float32)
    corr = lax.dot_general(high, table_ref[1], dims, preferred_element_type=jnp.float32)
    return both[:rows] + (both[rows:] + corr)


def weighted(terms):
    total = None
    for coef, value in terms:
        if abs(coef) < 1e-12:
            continue
        if abs(abs(coef) - 1.0) < 1e-12:
            term = value
        else:
            term = abs(coef) * value
        if total is None:
            total = term if coef > 0 else -term
        else:
            total = total + term if coef > 0 else total - term
    return total


def coarse_forward(xs):
    count = len(xs)
    half = count // 2
    even = {b: xs[b] + xs[count - b] for b in range(1, half)}
    odd = {b: xs[b] - xs[count - b] for b in range(1, half)}
    real, imag = [], {}
    for k in range(half + 1):
        ends = xs[0] + xs[half] if k % 2 == 0 else xs[0] - xs[half]
        real.append(weighted([(1.0, ends)] + [(math.cos(2 * math.pi * b * k / count), even[b]) for b in range(1, half)]))
    for k in range(1, half):
        imag[k] = weighted([(-math.sin(2 * math.pi * b * k / count), odd[b]) for b in range(1, half)])
    pairs = [(real[0], real[half])] + [(real[k], imag[k]) for k in range(1, half)]
    return pairs


def coarse_inverse(pairs):
    half = len(pairs)
    count = 2 * half
    first, last = pairs[0]
    xs = [None] * count
    for b in range(half + 1):
        ends = first + last if b % 2 == 0 else first - last
        cos_part = weighted([(1.0, ends)] + [(math.cos(2 * math.pi * b * k / count), pairs[k][0]) for k in range(1, half)])
        if b in (0, half):
            xs[b] = cos_part
        else:
            sin_part = weighted([(-math.sin(2 * math.pi * b * k / count), pairs[k][1]) for k in range(1, half)])
            xs[b] = cos_part + sin_part
            xs[count - b] = cos_part - sin_part
    return xs


def whole_tiles(count):
    return -(-count // 16) * 16


def forward_fill(xs, rows_ref, work_ref, start):
    pairs = coarse_forward(xs)
    half = len(pairs)
    first, last = pairs[0]
    for t in range(half + 1):
        cos, sin = rows_ref[t, 3:4, :LANE], rows_ref[t, 3:4, LANE:]
        if t == 0:
            left, right = first, jnp.zeros_like(first)
        elif t == half:
            left, right = last * cos, -(last * sin)
        else:
            real, imag = pairs[t]
            left, right = real * cos + imag * sin, imag * cos - real * sin
        work_ref[start + 8 * t:start + 8 * t + 8, :LANE] = left
        work_ref[start + 8 * t:start + 8 * t + 8, LANE:] = right


def inverse_blocks(back_ref, rows_ref, start):
    half = rows_ref.shape[0] - 1
    pairs = []
    ends = []
    for t in range(half + 1):
        left = back_ref[start + 8 * t:start + 8 * t + 8, :LANE]
        right = back_ref[start + 8 * t:start + 8 * t + 8, LANE:]
        cos, sin = rows_ref[t, 3:4, :LANE], rows_ref[t, 3:4, LANE:]
        if t == 0:
            ends.append(left)
        elif t == half:
            ends.append(left * cos + right * sin)
        else:
            pairs.append((left * cos + right * sin, left * sin - right * cos))
    return coarse_inverse([tuple(ends)] + pairs)


def put_blocks(out_ref, xs, unit, units):
    split = out_ref.shape[2] // LANE
    for b, value in enumerate(xs):
        out_ref[(b // split) * units + unit, :, (b % split) * LANE:(b % split + 1) * LANE] = value


def circle_diff(xs):
    count = len(xs)
    lane = lax.broadcasted_iota(jnp.int32, xs[0].shape, 1)
    ahead = [pltpu.roll(x, LANE - 1, 1) for x in xs]
    behind = [pltpu.roll(x, 1, 1) for x in xs]
    out = []
    for b in range(count):
        nxt = jnp.where(lane == LANE - 1, ahead[(b + 1) % count], ahead[b])
        prv = jnp.where(lane == 0, behind[(b - 1) % count], behind[b])
        out.append(nxt - prv)
    return out


def border_rows(edge_ref, send_ref):
    for d in range(edge_ref.shape[0]):
        send_ref[d] = jnp.sum(pltpu.roll(edge_ref[d], 0, 1, stride=8, stride_axis=0), axis=0, keepdims=True)


def border_columns(row):
    value = jnp.broadcast_to(row, (8, LANE))
    place = lax.broadcasted_iota(jnp.int32, (8, LANE), 0)
    for bit in (1, 2, 4):
        value = jnp.where(place // bit % 2 == 1, pltpu.roll(value, LANE - 8 * bit, 1), value)
    return value


def border_tiles(edge_ref, xs, unit):
    count = len(xs)
    split = count // edge_ref.shape[0]
    lane = lax.broadcasted_iota(jnp.int32, xs[0].shape, 1)
    turned = [pltpu.roll(x, 2 * unit + 1, 1) for x in xs]
    for d in range(edge_ref.shape[0]):
        west, east = turned[(d * split - 1) % count], turned[(d * split + split) % count]
        kept = edge_ref[d] if unit else jnp.zeros_like(west)
        edge_ref[d] = jnp.where(lane == 2 * unit, west, jnp.where(lane == 2 * unit + 1, east, kept))


def filter_values(limit, wave, scale):
    quotient = limit / jnp.maximum(wave, 1.0)
    return jnp.where(wave > limit, quotient * quotient, 1.0) * scale


def filter_terms(rows_ref, own_ref, near_ref, filt_ref, side_ref):
    rows = own_ref.shape[1]
    zonal, merid, limit = own_ref[0, :, 0:1], own_ref[1, :, 0:1], own_ref[2, :, 0:1]
    for t in range(rows_ref.shape[0]):
        wave, sines, scale = rows_ref[t, 0:1, :], rows_ref[t, 1:2, :], rows_ref[t, 2:3, :]
        factor = filter_values(limit, wave, scale)
        filt_ref[t, 0] = factor
        filt_ref[t, 1] = merid * factor
        filt_ref[t, 2] = (zonal * zonal) * sines * factor
        filt_ref[t, 3] = packed_half(factor, factor, False)
        filt_ref[t, 4] = packed_half(factor, factor, True)
        south = near_ref[0, 1, rows - 1:rows, 0:1] * filter_values(near_ref[0, 2, rows - 1:rows, 0:1], wave, scale)
        north = near_ref[1, 1, 0:1, 0:1] * filter_values(near_ref[1, 2, 0:1, 0:1], wave, scale)
        side_ref[t, 0:1, :] = south
        side_ref[t, 1:2, :] = north


def merid_terms(spec_ref, unit, t, filt_ref, side_ref, south_ref, north_ref, at):
    tile = spec_ref.shape[1] // filt_ref.shape[0]
    own = spec_ref[unit, tile * t:tile * t + tile, :]
    row = lax.broadcasted_iota(jnp.int32, own.shape, 0)
    below_far, below = south_ref[at:at + 1, :], south_ref[at + 1:at + 2, :]
    above, above_far = north_ref[at:at + 1, :], north_ref[at + 1:at + 2, :]
    upper = jnp.where(row == tile - 1, above, pltpu.roll(own, tile - 1, 0))
    lower = jnp.where(row == 0, below, pltpu.roll(own, 1, 0))
    mid = -filt_ref[t, 1] * (upper - lower)
    v_south = -side_ref[t, 0:1, :] * (own[0:1] - below_far)
    v_north = -side_ref[t, 1:2, :] * (above_far - own[tile - 1:tile])
    return own, row, mid, v_south, v_north


def factor_columns(a_ref, s_ref, ratio_ref, inv_ref, gain_ref, carry_ref):
    levels = s_ref.shape[0]
    prev = jnp.zeros(s_ref.shape[1:], jnp.float32)
    for level in range(levels):
        alpha = a_ref[level]
        below = alpha * s_ref[level]
        above = alpha * s_ref[level + 1] if level + 1 < levels else jnp.zeros_like(below)
        inv = 1.0 / (1.0 + below + above + below * prev)
        prev = -above * inv
        ratio_ref[level] = prev
        inv_ref[level] = inv
        gain_ref[level] = alpha * inv
        carry_ref[level] = below * inv


def solve_columns(s_ref, winv_ref, p_ref, spread, ratio_ref, gain_ref, carry_ref, w_out, p_out):
    levels = s_ref.shape[0]

    def star(level):
        return p_ref[level] - s_ref[level] * spread(level)

    here = star(0)
    prev = jnp.zeros_like(here)
    for level in range(levels):
        p_out[level] = here
        nxt = star(level + 1) if level + 1 < levels else jnp.zeros_like(here)
        prev = (winv_ref[level] - gain_ref[level] * (nxt - here)) + carry_ref[level] * prev
        w_out[level] = prev
        here = nxt
    upper = w_out[levels - 1]
    for level in range(levels - 1, 0, -1):
        lower = w_out[level - 1] - ratio_ref[level - 1] * upper
        w_out[level - 1] = lower
        p_out[level] = p_out[level] - s_ref[level] * (upper - lower)
        upper = lower
    p_out[0] = p_out[0] - s_ref[0] * upper


def packed_half(first, second, inner):
    rows = first.shape[0]
    row = lax.broadcasted_iota(jnp.int32, first.shape, 0)
    shift = rows - 2 if inner else 2
    return jnp.where(row < rows // 2, pltpu.roll(first, shift, 0), pltpu.roll(second, rows - shift, 0))


def unpacked(outer, inner, second):
    rows = outer.shape[0]
    row = lax.broadcasted_iota(jnp.int32, outer.shape, 0)
    shift = rows - 2 if second else 2
    middle = jnp.logical_and(row >= 2, row < rows - 2)
    return jnp.where(middle, pltpu.roll(inner, shift, 0), pltpu.roll(outer, rows - shift, 0))


def divergence(u, v, zonal, merid, west, east, south, north):
    rows, width = u.shape
    lane = lax.broadcasted_iota(jnp.int32, (rows, width), 1)
    row = lax.broadcasted_iota(jnp.int32, (rows, width), 0)
    ahead = jnp.where(lane == width - 1, east, pltpu.roll(u, width - 1, 1))
    behind = jnp.where(lane == 0, west, pltpu.roll(u, 1, 1))
    upper = jnp.where(row == rows - 1, north, pltpu.roll(v, rows - 1, 0))
    lower = jnp.where(row == 0, south, pltpu.roll(v, 1, 0))
    return zonal * (ahead - behind) + merid * (upper - lower)


def base_divergence(u_ref, v_ref, own_ref, west_ref, east_ref, south_ref, north_ref, base_ref, is_first, is_last):
    zonal, merid = own_ref[0, :, 0:1], own_ref[1, :, 0:1]
    keep_south = jnp.where(is_first, 0.0, 1.0)
    keep_north = jnp.where(is_last, 0.0, 1.0)
    west = west_ref[...]
    east = east_ref[...]
    for level in range(u_ref.shape[0]):
        base_ref[level] = divergence(
            u_ref[level], v_ref[level], zonal, merid, west[:, level:level + 1], east[:, level:level + 1],
            keep_south * south_ref[level:level + 1, :], keep_north * north_ref[level:level + 1, :],
        )


def added_divergence(ur, vr, own_ref, base_ref, levels):
    zonal, merid = own_ref[0, :, 0:1], own_ref[1, :, 0:1]
    for level in levels:
        base_ref[level] = base_ref[level] + divergence(ur[level], vr[level], zonal, merid, 0.0, 0.0, 0.0, 0.0)


def added_borders(own_ref, border_ref, base_ref, units):
    zonal = own_ref[0, :, 0:1]
    width = base_ref.shape[2]
    lane = lax.broadcasted_iota(jnp.int32, (8, LANE), 1)
    for d in range(border_ref.shape[0]):
        border = border_columns(border_ref[d])
        higher = pltpu.roll(border, LANE - units, 1)
        sides = [unpacked(border, higher, l == 1) for l in range(2)]
        for l in range(units):
            level = d * units + l
            at = l // 2 * 2
            west = jnp.where(lane == 0, zonal * sides[l % 2][:, at:at + 1], 0.0)
            east = jnp.where(lane == LANE - 1, zonal * sides[l % 2][:, at + 1:at + 2], 0.0)
            base_ref[level, :, :LANE] = base_ref[level, :, :LANE] - west
            base_ref[level, :, width - LANE:] = base_ref[level, :, width - LANE:] + east


def pack_edges(u_ref, v_ref, first_col, last_col, first_row, last_row):
    rows, width = u_ref.shape[1:]
    lane = lax.broadcasted_iota(jnp.int32, (rows, LANE), 1)
    first = jnp.zeros((rows, LANE), jnp.float32)
    last = jnp.zeros((rows, LANE), jnp.float32)
    for level in range(u_ref.shape[0]):
        first = jnp.where(lane == level, u_ref[level, :, 0:1], first)
        last = jnp.where(lane == level, u_ref[level, :, width - 1:width], last)
        first_row[level:level + 1, :] = v_ref[level, 0:1, :]
        last_row[level:level + 1, :] = v_ref[level, rows - 1:rows, :]
    first_col[...] = first
    last_col[...] = last


def pack_halo(source, low, high, units):
    rows = source.shape[1]
    for g in range(low.shape[0]):
        for l in range(units):
            low[g, 2 * l:2 * l + 2, :] = source[g * units + l, 0:2, :]
            high[g, 2 * l:2 * l + 2, :] = source[g * units + l, rows - 2:rows, :]


def own_coefs(zc_ref, mc_ref, cutoff_ref, mask_ref, own_ref, first_lat, unfiltered):
    rows = own_ref.shape[1]
    row = lax.broadcasted_iota(jnp.int32, own_ref.shape[1:], 0)
    zonal = jnp.zeros(own_ref.shape[1:], jnp.float32)
    merid = jnp.zeros(own_ref.shape[1:], jnp.float32)
    limit = jnp.zeros(own_ref.shape[1:], jnp.int32)
    for r in range(rows):
        zonal = jnp.where(row == r, zc_ref[r], zonal)
        merid = jnp.where(row == r, mc_ref[r], merid)
        filtered = mask_ref[first_lat + r]
        bound = filtered * cutoff_ref[first_lat + r] + (1 - filtered) * unfiltered
        limit = jnp.where(row == r, bound, limit)
    own_ref[0] = zonal
    own_ref[1] = merid
    own_ref[2] = limit.astype(jnp.float32)


def flipped(index, mask):
    bit = 1
    while bit <= mask:
        if mask & bit:
            index = index + bit * (1 - 2 * (index // bit % 2))
        bit *= 2
    return index


def partner_masks(count):
    return sorted(range(1, count), key=lambda mask: (-bin(mask // 2).count("1"), -(mask % 2), -mask))


def fused_kernel(
    bands, per_band, a_far, zc_far, mc_far, cutoff_far, mask_far, u_far, v_far, w_far, p_far, s_far, table_far, rows_far,
    u_out, v_out, base, winv, p_mid, s_ref, ratio, gain, carry, own_ref, rim_recv,
    x1, x2, d1, ur, vr, ds1, us, vs, w_mid, packed_p, inv, u_ref, v_ref, w_ref, p_ref,
    halo1, low, high, chain_send, chain_recv, table_ref, rows_ref, spec, packed_spec, work, back, filt, sides,
    near, cols_send, cols_recv, rows_send, rows_recv, border_tile, border_send, border_recv, rim_send,
    a_ref, zc_ref, mc_ref, cutoff_ref, mask_ref,
    load_sems, send_sems, recv_sems, edge_send, edge_recv, halo_send, halo_recv, last_send, last_recv, chain_out, chain_in, band_in,
):
    band_me = lax.axis_index("lat")
    lon_me = lax.axis_index("lon")
    lat_rows = u_ref.shape[1]
    units = u_ref.shape[0] // per_band
    channels = rows_ref.shape[0]
    half = channels - 1
    per_unit = channels * lat_rows
    split = u_ref.shape[2] // LANE
    mesh_id = pl.DeviceIdType.MESH
    is_first = band_me == 0
    is_last = band_me == bands - 1
    not_first = jnp.logical_not(is_first)
    not_last = jnp.logical_not(is_last)
    masks = partner_masks(per_band)
    partners = [flipped(lon_me, mask) for mask in masks]

    pairs = (
        (p_far, p_ref), (zc_far, zc_ref), (mc_far, mc_ref), (cutoff_far, cutoff_ref), (mask_far, mask_ref), (a_far, a_ref),
        (rows_far, rows_ref), (u_far, u_ref), (v_far, v_ref), (table_far, table_ref), (s_far, s_ref), (w_far, w_ref),
    )
    loads = [pltpu.make_async_copy(far, here, load_sems.at[n]) for n, (far, here) in enumerate(pairs)]
    loads[0].start()
    barrier = pltpu.get_barrier_semaphore()

    def greet(band, lon):
        pl.semaphore_signal(barrier, inc=1, device_id=(band, lon), device_id_type=mesh_id)

    for partner in partners:
        greet(band_me, partner)
    for there, step in ((not_first, -1), (not_last, 1)):
        @pl.when(there)
        def _():
            greet(band_me + step, lon_me)

    for load in loads[1:]:
        load.start()
    loads[0].wait()
    pl.semaphore_wait(barrier, per_band - 1 + jnp.where(is_first, 0, 1) + jnp.where(is_last, 0, 1))
    for there, step, place in ((not_first, -1, 1), (not_last, 1, 0)):
        @pl.when(there)
        def _():
            pl.semaphore_signal(band_in.at[place], inc=1, device_id=(band_me + step, lon_me), device_id_type=mesh_id)


    def scatter(source, target, sem, unit, count=1):
        for g in partners:
            pltpu.make_async_remote_copy(
                src_ref=source.at[pl.ds(g * units + unit, count)], dst_ref=target.at[pl.ds(lon_me * units + unit, count)],
                send_sem=send_sems.at[sem], recv_sem=recv_sems.at[sem, unit],
                device_id=(band_me, g), device_id_type=mesh_id,
            ).start()
        for n in range(count):
            target[lon_me * units + unit + n] = source[lon_me * units + unit + n]

    def gathered(target, sem, unit, count=1):
        block = target.at[pl.ds(0, (per_band - 1) * count)]
        pltpu.make_async_copy(block, block, recv_sems.at[sem, unit]).wait()

    def sent(source, sem):
        block = source.at[pl.ds(0, (per_band - 1) * units)]
        pltpu.make_async_copy(block, block, send_sems.at[sem]).wait()

    def spread_halo(target):
        def one(source, slot, sem, other):
            for g in partners + [lon_me]:
                pltpu.make_async_remote_copy(
                    src_ref=source.at[g], dst_ref=target.at[slot, lon_me],
                    send_sem=halo_send.at[sem], recv_sem=halo_recv.at[sem],
                    device_id=(other, g), device_id_type=mesh_id,
                ).start()

        @pl.when(not_first)
        def _():
            pl.semaphore_wait(band_in.at[0], 1)
            one(low, 1, 0, band_me - 1)

        @pl.when(not_last)
        def _():
            pl.semaphore_wait(band_in.at[1], 1)
            one(high, 0, 1, band_me + 1)

    def halo_wait(sems, upward):
        @pl.when(not_first)
        def _():
            pltpu.make_async_copy(low, low, sems.at[0 if upward else 1]).wait()

        @pl.when(not_last)
        def _():
            pltpu.make_async_copy(low, low, sems.at[1 if upward else 0]).wait()

    def chain_copy(unit, side):
        return pltpu.make_async_remote_copy(
            src_ref=chain_send.at[side, unit], dst_ref=chain_recv.at[side, unit],
            send_sem=chain_out.at[side], recv_sem=chain_in.at[side, unit],
            device_id=((band_me + bands + 1 - 2 * side) % bands, lon_me), device_id_type=mesh_id,
        )

    def chain_start(unit, tile, place):
        for t in range(channels):
            at = lat_rows * t + place
            chain_send[0, unit, 2 * t:2 * t + 2, :] = packed_spec[tile, at:at + 2, :]
            chain_send[1, unit, 2 * t:2 * t + 2, :] = packed_spec[tile, at + 2:at + 4, :]

        @pl.when(not_last)
        def _():
            chain_copy(unit, 0).start()

        @pl.when(not_first)
        def _():
            chain_copy(unit, 1).start()

    def coef_copy(step, side):
        return pltpu.make_async_remote_copy(
            src_ref=own_ref, dst_ref=near.at[side], send_sem=edge_send.at[4 + side], recv_sem=edge_recv.at[4 + side],
            device_id=((band_me + bands + step) % bands, lon_me), device_id_type=mesh_id,
        )

    for unit in range(0, units, 2):
        scatter(p_ref, x1, 0, unit, 2)
    pack_halo(p_ref, low, high, units)
    spread_halo(halo1)

    for load in loads[1:7]:
        load.wait()
    own_coefs(zc_ref, mc_ref, cutoff_ref, mask_ref, own_ref, band_me * lat_rows, half * TILE)

    @pl.when(not_first)
    def _():
        coef_copy(-1, 1).start()

    @pl.when(not_last)
    def _():
        coef_copy(1, 0).start()

    @pl.when(is_first)
    def _():
        near[0] = jnp.zeros(near.shape[1:], jnp.float32)
        chain_recv[0] = jnp.zeros(chain_recv.shape[1:], jnp.float32)
        for g in range(per_band):
            halo1[0, g] = jnp.zeros(halo1.shape[2:], jnp.float32)

    @pl.when(is_last)
    def _():
        near[1] = jnp.zeros(near.shape[1:], jnp.float32)
        chain_recv[1] = jnp.zeros(chain_recv.shape[1:], jnp.float32)
        for g in range(per_band):
            halo1[1, g] = jnp.zeros(halo1.shape[2:], jnp.float32)

    work[...] = jnp.zeros(work.shape, jnp.float32)
    for load in loads[7:9]:
        load.wait()
    pack_edges(u_ref, v_ref, cols_send.at[0], cols_send.at[1], rows_send.at[0], rows_send.at[1])
    edge_copies = []
    for side, step in ((0, -1), (1, 1)):
        edge_copies.append(pltpu.make_async_remote_copy(
            src_ref=cols_send.at[side], dst_ref=cols_recv.at[side], send_sem=edge_send.at[side], recv_sem=edge_recv.at[side],
            device_id=(band_me, (lon_me + per_band + step) % per_band), device_id_type=mesh_id,
        ))
    for copy in edge_copies:
        copy.start()

    def row_copy(step, side):
        return pltpu.make_async_remote_copy(
            src_ref=rows_send.at[side], dst_ref=rows_recv.at[side], send_sem=edge_send.at[2 + side], recv_sem=edge_recv.at[2 + side],
            device_id=((band_me + bands + step) % bands, lon_me), device_id_type=mesh_id,
        )

    @pl.when(not_first)
    def _():
        row_copy(-1, 0).start()

    @pl.when(not_last)
    def _():
        row_copy(1, 1).start()

    @pl.when(is_first)
    def _():
        rows_recv[1] = jnp.zeros(rows_recv.shape[1:], jnp.float32)

    @pl.when(is_last)
    def _():
        rows_recv[0] = jnp.zeros(rows_recv.shape[1:], jnp.float32)

    for load in loads[9:]:
        load.wait()
    factor_columns(a_ref, s_ref, ratio, inv, gain, carry)
    for level in range(s_ref.shape[0]):
        winv[level] = w_ref[level] * inv[level]

    @pl.when(not_first)
    def _():
        coef_copy(1, 0).wait_recv()

    @pl.when(not_last)
    def _():
        coef_copy(-1, 1).wait_recv()

    filter_terms(rows_ref, own_ref, near, filt, sides)

    def circles(source, first, count, stride):
        return [
            [source[d * stride + first + n, :, h * LANE:(h + 1) * LANE] for d in range(per_band) for h in range(split)]
            for n in range(count)
        ]

    def forward(tiles, places):
        for n, xs in enumerate(tiles):
            forward_fill(xs, rows_ref, work, n * per_unit)
        used = len(tiles) * per_unit
        value = three_products(work[0:whole_tiles(used), :], table_ref)
        for n, place in enumerate(places):
            spec[place] = value[n * per_unit:(n + 1) * per_unit]
        return value

    def inverse(count):
        back[0:whole_tiles(count * per_unit), :] = three_products(work[0:whole_tiles(count * per_unit), :], table_ref)

    merid = own_ref[1, :, 0:1]
    pair_count = units // 2
    halo_wait(halo_recv, False)
    forward([
        [halo1[slot, d, :, h * LANE:(h + 1) * LANE] for d in range(per_band) for h in range(split)] for slot in range(2)
    ], [units, units + 1])
    for pair in range(pair_count):
        gathered(x1, 0, 2 * pair, 2)
        forward(circles(x1, 2 * pair, 2, units), [2 * pair, 2 * pair + 1])
        for t in range(channels):
            both = []
            for l in (2 * pair, 2 * pair + 1):
                at = lat_rows * t + 2 * l
                own, row, mid, v_south, v_north = merid_terms(spec, l, t, filt, sides, spec.at[units], spec.at[units + 1], at)
                upper = jnp.where(row == lat_rows - 1, v_north, pltpu.roll(mid, lat_rows - 1, 0))
                lower = jnp.where(row == 0, v_south, pltpu.roll(mid, 1, 0))
                both.append(filt[t, 2] * own + merid * (upper - lower))
            for half_at in range(2):
                at = half_at * per_unit + lat_rows * t
                work[at:at + lat_rows, :] = packed_half(*both, half_at == 1)
        inverse(2)
        put_blocks(ds1, inverse_blocks(back, rows_ref, 0), pair, units)
        scatter(ds1, d1, 1, pair)
        put_blocks(ds1, inverse_blocks(back, rows_ref, per_unit), pair_count + pair, units)
        scatter(ds1, d1, 1, pair_count + pair)

    for copy in edge_copies:
        copy.wait_recv()

    @pl.when(not_first)
    def _():
        row_copy(1, 1).wait_recv()

    @pl.when(not_last)
    def _():
        row_copy(-1, 0).wait_recv()

    base_divergence(
        u_ref, v_ref, own_ref, cols_recv.at[1], cols_recv.at[0], rows_recv.at[1], rows_recv.at[0], base,
        is_first, is_last,
    )
    def first_spread(level):
        tile = d1[level // units * units + level % units // 2]
        return base[level] + (pltpu.roll(tile, 2 if level % 2 else lat_rows - 2, 0))

    def second_spread(level):
        place = level // units * units + level % units // 2
        return base[level] + unpacked(d1[place], d1[place + pair_count], level % 2 == 1)

    for half_at, spread in enumerate((first_spread, second_spread)):
        for pair in range(pair_count):
            gathered(d1, 1, half_at * pair_count + pair)
        solve_columns(s_ref, winv, p_ref, spread, ratio, gain, carry, vs, p_mid)
        for pair in range(pair_count):
            for d in range(per_band):
                level = d * units + 2 * pair
                packed_p[d * units + half_at * pair_count + pair] = packed_half(p_mid[level], p_mid[level + 1], half_at == 1)
            scatter(packed_p, x2, 2, half_at * pair_count + pair)
    for level in range(s_ref.shape[0]):
        winv[level] = vs[level] * inv[level]

    for tile in range(units):
        pair, half_at = tile % pair_count, tile // pair_count
        gathered(x2, 2, tile)
        value = forward(circles(x2, tile, 1, units), [])
        for t in range(channels):
            rows = slice(lat_rows * t, lat_rows * (t + 1))
            total = packed_half(spec[2 * pair, rows, :], spec[2 * pair + 1, rows, :], half_at == 1) + value[rows]
            packed_spec[tile, rows, :] = total
            work[rows, :] = filt[t, 3 + half_at] * total
        for l in range(2):
            if not half_at:
                chain_start(2 * pair + l, tile, 4 * l)
                continue
            for t in range(channels):
                rows = slice(lat_rows * t, lat_rows * (t + 1))
                spec[2 * pair + l, rows, :] = unpacked(packed_spec[pair, rows, :], packed_spec[tile, rows, :], l == 1)
        zonal = packed_half(own_ref[0], own_ref[0], half_at == 1)
        inverse(1)
        moved = [-zonal * x for x in circle_diff(inverse_blocks(back, rows_ref, 0))]
        put_blocks(us, moved, tile, units)
        scatter(us, ur, 3, tile)
        border_tiles(border_tile, moved, tile)
    border_rows(border_tile, border_send)

    def last_copy(source, target, n, g):
        return pltpu.make_async_remote_copy(
            src_ref=source.at[pl.ds(g, 1)], dst_ref=target.at[pl.ds(lon_me, 1)], send_sem=last_send.at[n], recv_sem=last_recv.at[n],
            device_id=(band_me, g), device_id_type=mesh_id,
        )

    def last_scatter(source, target, n):
        for g in partners:
            last_copy(source, target, n, g).start()
        target[lon_me] = source[lon_me]

    last_scatter(border_send, border_recv, 0)
    rim_at = per_unit
    for unit in range(units):
        @pl.when(not_first)
        def _():
            chain_copy(unit, 0).wait_recv()

        @pl.when(not_last)
        def _():
            chain_copy(unit, 1).wait_recv()

        for t in range(channels):
            own, row, mid, v_south, v_north = merid_terms(
                spec, unit, t, filt, sides, chain_recv.at[0, unit], chain_recv.at[1, unit], 2 * t,
            )
            work[lat_rows * t:lat_rows * (t + 1), :] = mid
            rim = rim_at + lat_rows * t + 2 * unit
            work[rim:rim + 1, :] = v_south
            work[rim + 1:rim + 2, :] = v_north
        inverse(2 if unit == units - 1 else 1)
        put_blocks(vs, inverse_blocks(back, rows_ref, 0), unit, units)
        scatter(vs, vr, 4, unit)
    rims = inverse_blocks(back, rows_ref, rim_at)
    for b, value in enumerate(rims):
        rim_send[b // split, :, (b % split) * LANE:(b % split + 1) * LANE] = value

    last_scatter(rim_send, rim_recv, 1)

    def last_wait(target, sems, n):
        block = target.at[pl.ds(0, per_band - 1)]
        pltpu.make_async_copy(block, block, sems.at[n]).wait()

    for tile in range(units):
        gathered(ur, 3, tile)
        for d in range(per_band if tile >= pair_count else 0):
            for l in range(2):
                level = d * units + 2 * (tile - pair_count) + l
                moved = unpacked(ur[d * units + tile - pair_count], ur[d * units + tile], l == 1)
                u_out[level] = u_ref[level] + moved
                w_mid[level] = moved
    last_wait(border_recv, last_recv, 0)
    added_borders(own_ref, border_recv, base, units)
    for unit in range(units):
        gathered(vr, 4, unit)
        own_levels = [d * units + unit for d in range(per_band)]
        for level in own_levels:
            v_out[level] = v_ref[level] + vr[level]
        added_divergence(w_mid, vr, own_ref, base, own_levels)
    last_wait(rim_recv, last_recv, 1)
    for source, sem in ((p_ref, 0), (ds1, 1), (packed_p, 2), (us, 3), (vs, 4)):
        sent(source, sem)
    last_wait(border_send, last_send, 0)
    last_wait(rim_send, last_send, 1)
    halo_wait(halo_send, True)
    for copy in edge_copies:
        copy.wait_send()

    @pl.when(not_first)
    def _():
        pltpu.make_async_copy(chain_send.at[1], chain_send.at[1], chain_out.at[1]).wait()
        coef_copy(-1, 1).wait_send()
        row_copy(-1, 0).wait_send()

    @pl.when(not_last)
    def _():
        pltpu.make_async_copy(chain_send.at[0], chain_send.at[0], chain_out.at[0]).wait()
        coef_copy(1, 0).wait_send()
        row_copy(1, 1).wait_send()


def deliver_kernel(
    units, u_ref, v_ref, base, winv, p_mid, s_ref, ratio, gain, carry, own_ref, rim_ref, u_out, v_out, w_out, p_out, w_end, p_end, sems,
):
    copies = [
        pltpu.make_async_copy(source, target, sems.at[n])
        for n, (source, target) in enumerate(((u_ref, u_out), (v_ref, v_out), (w_end, w_out), (p_end, p_out)))
    ]
    copies[0].start()
    copies[1].start()
    row = lax.broadcasted_iota(jnp.int32, u_ref.shape[1:], 0)
    rows = u_ref.shape[1]
    merid = own_ref[1, :, 0:1]
    south = jnp.where(row == 0, -merid, 0.0)
    north = jnp.where(row == rows - 1, merid, 0.0)

    def spread(level):
        d, l = level // units, 2 * (level % units)
        return base[level] + south * rim_ref[d, l:l + 1, :] + north * rim_ref[d, l + 1:l + 2, :]

    solve_columns(s_ref, winv, p_mid, spread, ratio, gain, carry, w_end, p_end)
    copies[2].start()
    copies[3].start()
    for copy in copies:
        copy.wait()


def deliver(units, arrays):
    shape = arrays[0].shape
    return pl.pallas_call(
        functools.partial(deliver_kernel, units),
        out_shape=(jax.ShapeDtypeStruct(shape, jnp.float32),) * 4,
        in_specs=[pl.BlockSpec(memory_space=pltpu.VMEM)] * len(arrays),
        out_specs=(pl.BlockSpec(memory_space=pl.ANY),) * 4,
        scratch_shapes=[pltpu.VMEM(shape, jnp.float32)] * 2 + [pltpu.SemaphoreType.DMA((4,))],
        compiler_params=pltpu.CompilerParams(vmem_limit_bytes=FINISH_VMEM),
    )(*arrays)


def level_body(
    tables,
    zonal_wind,
    merid_wind,
    vertical_wind,
    pressure,
    zonal_coef,
    merid_coef,
    level_coef,
    sound_coef,
    cutoff,
    filter_mask,
):
    table, rows = (jnp.asarray(t) for t in tables)
    channels = rows.shape[0]
    bands = lax.axis_size("lat")
    per_band = lax.axis_size("lon")
    levels, lat_rows, width = pressure.shape
    units = levels // per_band
    per_unit = channels * lat_rows
    vmem = pl.BlockSpec(memory_space=pltpu.VMEM)
    far = pl.BlockSpec(memory_space=pl.ANY)

    def scratch(*shape):
        return pltpu.VMEM(shape, jnp.float32)

    field = scratch(*pressure.shape)
    halo = scratch(2, per_band, lat_rows, width)
    chain = scratch(2, units, -(-2 * channels // 8) * 8, TILE)
    spare = scratch(whole_tiles(2 * per_unit), TILE)
    dma = pltpu.SemaphoreType.DMA
    operands = (
        level_coef, zonal_coef, merid_coef, cutoff, filter_mask,
        zonal_wind, merid_wind, vertical_wind, pressure, sound_coef, table, rows,
    )
    results = pl.pallas_call(
        functools.partial(fused_kernel, bands, per_band),
        out_shape=(pltpu.VMEM(pressure.shape, jnp.float32),) * 9 + (
            pltpu.VMEM((3, lat_rows, LANE), jnp.float32), pltpu.VMEM((per_band, lat_rows, width), jnp.float32),
        ),
        in_specs=[far] * len(operands),
        out_specs=(vmem,) * 11,
        scratch_shapes=[field] * 15 + [halo, scratch(per_band, lat_rows, width), scratch(per_band, lat_rows, width), chain, chain] + [
            pltpu.VMEM(table.shape, table.dtype), scratch(*rows.shape),
            scratch(units + 2, per_unit, TILE), scratch(units, per_unit, TILE), spare, spare,
            scratch(channels, 5, lat_rows, TILE), scratch(channels, 8, TILE),
            scratch(2, 3, lat_rows, LANE),
            scratch(2, lat_rows, LANE), scratch(2, lat_rows, LANE),
            scratch(2, levels, width), scratch(2, levels, width),
            scratch(per_band, lat_rows, LANE), scratch(per_band, 1, LANE), scratch(per_band, 1, LANE),
            scratch(per_band, lat_rows, width),
            pltpu.SMEM(level_coef.shape, jnp.float32), pltpu.SMEM(zonal_coef.shape, jnp.float32),
            pltpu.SMEM(merid_coef.shape, jnp.float32), pltpu.SMEM(cutoff.shape, jnp.int32),
            pltpu.SMEM(filter_mask.shape, jnp.int32),
            dma((len(operands),)), dma((5,)), dma((5, units)), dma((6,)), dma((6,)), dma((2,)), dma((2,)), dma((2,)), dma((2,)), dma((2,)), dma((2, units)),
            pltpu.SemaphoreType.REGULAR((2,)),
        ],
        compiler_params=pltpu.CompilerParams(collective_id=0, has_side_effects=True, vmem_limit_bytes=FUSED_VMEM),
    )(*[pltpu.with_memory_space_constraint(x, pltpu.HBM) for x in operands])
    return deliver(units, results)


def body(tables, *arrays):
    pressure = arrays[3]
    per_band = lax.axis_size("lon")
    levels, lat_rows, width = pressure.shape
    fits = lat_rows == 8 and levels == 4 * per_band and levels <= LANE and width % LANE == 0 and per_band == 8
    if fits:
        return level_body(tables, *arrays)
    return wide_body(*arrays)


def solution(mesh):
    in_specs = (
        P(None, "lat", "lon"),
        P(None, "lat", "lon"),
        P(None, "lat", "lon"),
        P(None, "lat", "lon"),
        P("lat"),
        P("lat"),
        P(),
        P(None, "lat", "lon"),
        P(),
        P(),
    )
    out_specs = (
        P(None, "lat", "lon"),
        P(None, "lat", "lon"),
        P(None, "lat", "lon"),
        P(None, "lat", "lon"),
    )

    def whole(*arrays):
        tables = circle_tables(arrays[0].shape[2])
        step = jax.shard_map(functools.partial(body, tables), mesh=mesh, in_specs=in_specs, out_specs=out_specs, check_vma=False)
        return step(*arrays)

    return whole
```

```python
import functools
import math

import ml_dtypes
import numpy as np
import jax
import jax.numpy as jnp
from jax import lax
from jax.experimental import pallas as pl
from jax.experimental.pallas import tpu as pltpu
from jax.sharding import PartitionSpec as P

SUBSTEPS = 2
FUSED_VMEM = 40 * 2 ** 20
FINISH_VMEM = 4 * 2 ** 20


def extended(block, sides, width):
    for axis, dim in sides:
        count = lax.axis_size(axis)
        forward = [(i, i + 1) for i in range(count - 1)]
        forward.append((count - 1, 0))
        backward = [(target, source) for source, target in forward]
        low = lax.ppermute(
            lax.slice_in_dim(block, block.shape[dim] - width, None, axis=dim), axis, forward
        )
        high = lax.ppermute(lax.slice_in_dim(block, 0, width, axis=dim), axis, backward)
        block = jnp.concatenate([low, block, high], axis=dim)
    return block


def rim_fix(padded, lat_dim):
    band_index = lax.axis_index("lat")
    bands = lax.axis_size("lat")
    extent = padded.shape[lat_dim]
    position = lax.broadcasted_iota(jnp.int32, padded.shape, lat_dim)
    first_edge = jnp.logical_and(position == 0, band_index == 0)
    final_edge = jnp.logical_and(position == extent - 1, band_index == bands - 1)
    return jnp.where(jnp.logical_or(first_edge, final_edge), 0.0, padded)


def dft_tables(length):
    half_len = length // 2
    sample = lax.broadcasted_iota(jnp.int32, (length, length), 0)
    column = lax.broadcasted_iota(jnp.int32, (length, length), 1)
    is_cosine = column <= half_len
    wavenum = jnp.where(is_cosine, column, column - half_len)
    phase = sample * wavenum % length
    angle = 2.0 * math.pi / length * phase.astype(jnp.float32)
    forward = jnp.where(is_cosine, jnp.cos(angle), jnp.sin(angle))
    single = jnp.logical_and(is_cosine, jnp.logical_or(wavenum == 0, wavenum == half_len))
    weight = jnp.where(single, 1.0, 2.0) / length
    inverse = jnp.transpose(forward * weight)
    wave_row = wavenum[0].astype(jnp.float32)
    return (forward, inverse, wave_row)


def damping(wave_row, limits):
    bound_col = limits[:, None]
    ratio = bound_col / jnp.maximum(wave_row[None, :], 1.0)
    return jnp.where(wave_row[None, :] > bound_col, ratio * ratio, 1.0)


def transform_band(block, limits, forward, inverse, wave_row):
    circles = lax.all_to_all(block, "lon", split_axis=1, concat_axis=3, tiled=True)
    spectra = jnp.einsum("vetj,jc->vetc", circles, forward, precision=lax.Precision.HIGHEST)
    scaled = spectra * damping(wave_row, limits)
    damped = jnp.einsum("vetc,cj->vetj", scaled, inverse, precision=lax.Precision.HIGHEST)
    return lax.all_to_all(damped, "lon", split_axis=3, concat_axis=1, tiled=True)


def filtered_increments(increments, own_flags, own_limits, forward, inverse, wave_row):
    flag_cols = own_flags[:, None]
    damped = transform_band(increments, own_limits, forward, inverse, wave_row)
    return jnp.where(flag_cols, damped, increments)


def column_solve(vertical_wind, pstar, level_coef, sound_coef):
    levels = vertical_wind.shape[0]
    zero_slab = jnp.zeros_like(vertical_wind[0])
    ratios = []
    values = []
    prev_ratio = zero_slab
    prev_value = zero_slab
    for level in range(levels):
        alpha = level_coef[level]
        below = alpha * sound_coef[level]
        if level + 1 < levels:
            above = alpha * sound_coef[level + 1]
            rhs = vertical_wind[level] - alpha * (pstar[level + 1] - pstar[level])
        else:
            above = zero_slab
            rhs = vertical_wind[level] + alpha * pstar[level]
        pivot = 1.0 + below + above + below * prev_ratio
        prev_ratio = -above / pivot
        prev_value = (rhs + below * prev_value) / pivot
        ratios.append(prev_ratio)
        values.append(prev_value)
    solved = [zero_slab] * levels
    upper_value = values[levels - 1]
    solved[levels - 1] = upper_value
    for level in range(levels - 2, -1, -1):
        upper_value = values[level] - ratios[level] * upper_value
        solved[level] = upper_value
    new_wind = jnp.stack(solved)
    wind_below = jnp.concatenate([zero_slab[None], new_wind[:-1]], axis=0)
    new_pressure = pstar - sound_coef * (new_wind - wind_below)
    return (new_wind, new_pressure)


def wide_body(
    zonal_wind,
    merid_wind,
    vertical_wind,
    pressure,
    zonal_coef,
    merid_coef,
    level_coef,
    sound_coef,
    cutoff,
    filter_mask,
):
    lat_rows = pressure.shape[1]
    start = lax.axis_index("lat") * lat_rows
    own_flags = lax.dynamic_slice_in_dim(filter_mask, start, lat_rows) > 0
    own_limits = lax.dynamic_slice_in_dim(cutoff, start, lat_rows).astype(jnp.float32)
    forward, inverse, wave_row = dft_tables(pressure.shape[2] * lax.axis_size("lon"))
    zonal_rows = zonal_coef[None, :, None]
    merid_rows = merid_coef[None, :, None]
    for step in range(SUBSTEPS):
        padded = extended(pressure, (("lat", 1), ("lon", 2)), 1)
        padded = rim_fix(padded, 1)
        zonal_step = -zonal_rows * (padded[:, 1:-1, 2:] - padded[:, 1:-1, :-2])
        merid_step = -merid_rows * (padded[:, 2:, 1:-1] - padded[:, :-2, 1:-1])
        increments = jnp.stack([zonal_step, merid_step])
        damped = filtered_increments(increments, own_flags, own_limits, forward, inverse, wave_row)
        winds = jnp.stack([zonal_wind, merid_wind]) + damped
        wind_pad = extended(winds, (("lat", 2), ("lon", 3)), 1)
        wind_pad = rim_fix(wind_pad, 2)
        diverge = zonal_rows * (wind_pad[0, :, 1:-1, 2:] - wind_pad[0, :, 1:-1, :-2])
        diverge = diverge + merid_rows * (wind_pad[1, :, 2:, 1:-1] - wind_pad[1, :, :-2, 1:-1])
        pstar = pressure - sound_coef * diverge
        vertical_wind, pressure = column_solve(vertical_wind, pstar, level_coef, sound_coef)
        zonal_wind = winds[0]
        merid_wind = winds[1]
    return (zonal_wind, merid_wind, vertical_wind, pressure)


LANE = 128
TILE = 2 * LANE


def circle_tables(length):
    blocks = length // LANE
    half = blocks // 2
    m = np.arange(LANE, dtype=np.float64)[:, None]
    c = np.arange(LANE)[None, :]
    angle = 2 * np.pi * ((m * c) % LANE) / LANE
    cos, sin = np.cos(angle) / np.sqrt(LANE), np.sin(angle) / np.sqrt(LANE)
    table = np.block([[cos, -sin], [sin, cos]])
    high = table.astype(ml_dtypes.bfloat16)
    rest = (table - high.astype(np.float64)).astype(ml_dtypes.bfloat16)
    rows = np.zeros((half + 1, 8, TILE), np.float32)
    for k1 in range(half + 1):
        k = k1 + blocks * c[0]
        waves = np.tile(np.minimum(k, length - k), 2)
        scale = (1.0 if k1 in (0, half) else 2.0) / blocks
        turn = 2 * np.pi * m[:, 0] * k1 / length
        rows[k1, 0] = waves
        rows[k1, 1] = 4.0 * np.sin(2 * np.pi * waves / length) ** 2
        rows[k1, 2] = np.where(np.arange(TILE) < LANE, scale, -scale)
        rows[k1, 3] = np.concatenate([np.cos(turn), np.sin(turn)])
    return np.stack([high, rest]), rows


def split_parts(value):
    high = value.astype(jnp.bfloat16)
    rest = (value - high.astype(jnp.float32)).astype(jnp.bfloat16)
    return high, rest


def three_products(value, table_ref):
    high, rest = split_parts(value)
    dims = (((1,), (0,)), ((), ()))
    rows = value.shape[0]
    table = table_ref[0]
    both = lax.dot_general(jnp.concatenate([high, rest], axis=0), table, dims, preferred_element_type=jnp.float32)
    corr = lax.dot_general(high, table_ref[1], dims, preferred_element_type=jnp.float32)
    return both[:rows] + (both[rows:] + corr)


def weighted(terms):
    total = None
    for coef, value in terms:
        if abs(coef) < 1e-12:
            continue
        if abs(abs(coef) - 1.0) < 1e-12:
            term = value
        else:
            term = abs(coef) * value
        if total is None:
            total = term if coef > 0 else -term
        else:
            total = total + term if coef > 0 else total - term
    return total


def coarse_forward(xs):
    count = len(xs)
    half = count // 2
    even = {b: xs[b] + xs[count - b] for b in range(1, half)}
    odd = {b: xs[b] - xs[count - b] for b in range(1, half)}
    real, imag = [], {}
    for k in range(half + 1):
        ends = xs[0] + xs[half] if k % 2 == 0 else xs[0] - xs[half]
        real.append(weighted([(1.0, ends)] + [(math.cos(2 * math.pi * b * k / count), even[b]) for b in range(1, half)]))
    for k in range(1, half):
        imag[k] = weighted([(-math.sin(2 * math.pi * b * k / count), odd[b]) for b in range(1, half)])
    pairs = [(real[0], real[half])] + [(real[k], imag[k]) for k in range(1, half)]
    return pairs


def coarse_inverse(pairs):
    half = len(pairs)
    count = 2 * half
    first, last = pairs[0]
    xs = [None] * count
    for b in range(half + 1):
        ends = first + last if b % 2 == 0 else first - last
        cos_part = weighted([(1.0, ends)] + [(math.cos(2 * math.pi * b * k / count), pairs[k][0]) for k in range(1, half)])
        if b in (0, half):
            xs[b] = cos_part
        else:
            sin_part = weighted([(-math.sin(2 * math.pi * b * k / count), pairs[k][1]) for k in range(1, half)])
            xs[b] = cos_part + sin_part
            xs[count - b] = cos_part - sin_part
    return xs


def whole_tiles(count):
    return -(-count // 16) * 16


def forward_fill(xs, rows_ref, work_ref, start):
    pairs = coarse_forward(xs)
    half = len(pairs)
    first, last = pairs[0]
    for t in range(half + 1):
        cos, sin = rows_ref[t, 3:4, :LANE], rows_ref[t, 3:4, LANE:]
        if t == 0:
            left, right = first, jnp.zeros_like(first)
        elif t == half:
            left, right = last * cos, -(last * sin)
        else:
            real, imag = pairs[t]
            left, right = real * cos + imag * sin, imag * cos - real * sin
        work_ref[start + 8 * t:start + 8 * t + 8, :LANE] = left
        work_ref[start + 8 * t:start + 8 * t + 8, LANE:] = right


def inverse_blocks(back_ref, rows_ref, start):
    half = rows_ref.shape[0] - 1
    pairs = []
    ends = []
    for t in range(half + 1):
        left = back_ref[start + 8 * t:start + 8 * t + 8, :LANE]
        right = back_ref[start + 8 * t:start + 8 * t + 8, LANE:]
        cos, sin = rows_ref[t, 3:4, :LANE], rows_ref[t, 3:4, LANE:]
        if t == 0:
            ends.append(left)
        elif t == half:
            ends.append(left * cos + right * sin)
        else:
            pairs.append((left * cos + right * sin, left * sin - right * cos))
    return coarse_inverse([tuple(ends)] + pairs)


def put_blocks(out_ref, xs, unit, units):
    split = out_ref.shape[2] // LANE
    for b, value in enumerate(xs):
        out_ref[(b // split) * units + unit, :, (b % split) * LANE:(b % split + 1) * LANE] = value


def circle_diff(xs):
    count = len(xs)
    lane = lax.broadcasted_iota(jnp.int32, xs[0].shape, 1)
    ahead = [pltpu.roll(x, LANE - 1, 1) for x in xs]
    behind = [pltpu.roll(x, 1, 1) for x in xs]
    out = []
    for b in range(count):
        nxt = jnp.where(lane == LANE - 1, ahead[(b + 1) % count], ahead[b])
        prv = jnp.where(lane == 0, behind[(b - 1) % count], behind[b])
        out.append(nxt - prv)
    return out


def border_rows(edge_ref, send_ref):
    for d in range(edge_ref.shape[0]):
        send_ref[d] = jnp.sum(pltpu.roll(edge_ref[d], 0, 1, stride=8, stride_axis=0), axis=0, keepdims=True)


def border_columns(row):
    value = jnp.broadcast_to(row, (8, LANE))
    place = lax.broadcasted_iota(jnp.int32, (8, LANE), 0)
    for bit in (1, 2, 4):
        value = jnp.where(place // bit % 2 == 1, pltpu.roll(value, LANE - 8 * bit, 1), value)
    return value


def border_tiles(edge_ref, xs, unit):
    count = len(xs)
    split = count // edge_ref.shape[0]
    lane = lax.broadcasted_iota(jnp.int32, xs[0].shape, 1)
    turned = [pltpu.roll(x, 2 * unit + 1, 1) for x in xs]
    for d in range(edge_ref.shape[0]):
        west, east = turned[(d * split - 1) % count], turned[(d * split + split) % count]
        kept = edge_ref[d] if unit else jnp.zeros_like(west)
        edge_ref[d] = jnp.where(lane == 2 * unit, west, jnp.where(lane == 2 * unit + 1, east, kept))


def filter_values(limit, wave, scale):
    quotient = limit / jnp.maximum(wave, 1.0)
    return jnp.where(wave > limit, quotient * quotient, 1.0) * scale


def filter_terms(rows_ref, own_ref, near_ref, filt_ref, side_ref):
    rows = own_ref.shape[1]
    zonal, merid, limit = own_ref[0, :, 0:1], own_ref[1, :, 0:1], own_ref[2, :, 0:1]
    for t in range(rows_ref.shape[0]):
        wave, sines, scale = rows_ref[t, 0:1, :], rows_ref[t, 1:2, :], rows_ref[t, 2:3, :]
        factor = filter_values(limit, wave, scale)
        filt_ref[t, 0] = factor
        filt_ref[t, 1] = merid * factor
        filt_ref[t, 2] = (zonal * zonal) * sines * factor
        filt_ref[t, 3] = packed_half(factor, factor, False)
        filt_ref[t, 4] = packed_half(factor, factor, True)
        south = near_ref[0, 1, rows - 1:rows, 0:1] * filter_values(near_ref[0, 2, rows - 1:rows, 0:1], wave, scale)
        north = near_ref[1, 1, 0:1, 0:1] * filter_values(near_ref[1, 2, 0:1, 0:1], wave, scale)
        side_ref[t, 0:1, :] = south
        side_ref[t, 1:2, :] = north


def merid_terms(spec_ref, unit, t, filt_ref, side_ref, south_ref, north_ref, at):
    tile = spec_ref.shape[1] // filt_ref.shape[0]
    own = spec_ref[unit, tile * t:tile * t + tile, :]
    row = lax.broadcasted_iota(jnp.int32, own.shape, 0)
    below_far, below = south_ref[at:at + 1, :], south_ref[at + 1:at + 2, :]
    above, above_far = north_ref[at:at + 1, :], north_ref[at + 1:at + 2, :]
    upper = jnp.where(row == tile - 1, above, pltpu.roll(own, tile - 1, 0))
    lower = jnp.where(row == 0, below, pltpu.roll(own, 1, 0))
    mid = -filt_ref[t, 1] * (upper - lower)
    v_south = -side_ref[t, 0:1, :] * (own[0:1] - below_far)
    v_north = -side_ref[t, 1:2, :] * (above_far - own[tile - 1:tile])
    return own, row, mid, v_south, v_north


def factor_columns(a_ref, s_ref, ratio_ref, inv_ref, gain_ref, carry_ref):
    levels = s_ref.shape[0]
    prev = jnp.zeros(s_ref.shape[1:], jnp.float32)
    for level in range(levels):
        alpha = a_ref[level]
        below = alpha * s_ref[level]
        above = alpha * s_ref[level + 1] if level + 1 < levels else jnp.zeros_like(below)
        inv = 1.0 / (1.0 + below + above + below * prev)
        prev = -above * inv
        ratio_ref[level] = prev
        inv_ref[level] = inv
        gain_ref[level] = alpha * inv
        carry_ref[level] = below * inv


def solve_columns(s_ref, winv_ref, p_ref, spread, ratio_ref, gain_ref, carry_ref, w_out, p_out):
    levels = s_ref.shape[0]

    def star(level):
        return p_ref[level] - s_ref[level] * spread(level)

    here = star(0)
    prev = jnp.zeros_like(here)
    for level in range(levels):
        p_out[level] = here
        nxt = star(level + 1) if level + 1 < levels else jnp.zeros_like(here)
        prev = (winv_ref[level] - gain_ref[level] * (nxt - here)) + carry_ref[level] * prev
        w_out[level] = prev
        here = nxt
    upper = w_out[levels - 1]
    for level in range(levels - 1, 0, -1):
        lower = w_out[level - 1] - ratio_ref[level - 1] * upper
        w_out[level - 1] = lower
        p_out[level] = p_out[level] - s_ref[level] * (upper - lower)
        upper = lower
    p_out[0] = p_out[0] - s_ref[0] * upper


def packed_half(first, second, inner):
    rows = first.shape[0]
    row = lax.broadcasted_iota(jnp.int32, first.shape, 0)
    shift = rows - 2 if inner else 2
    return jnp.where(row < rows // 2, pltpu.roll(first, shift, 0), pltpu.roll(second, rows - shift, 0))


def unpacked(outer, inner, second):
    rows = outer.shape[0]
    row = lax.broadcasted_iota(jnp.int32, outer.shape, 0)
    shift = rows - 2 if second else 2
    middle = jnp.logical_and(row >= 2, row < rows - 2)
    return jnp.where(middle, pltpu.roll(inner, shift, 0), pltpu.roll(outer, rows - shift, 0))


def divergence(u, v, zonal, merid, west, east, south, north):
    rows, width = u.shape
    lane = lax.broadcasted_iota(jnp.int32, (rows, width), 1)
    row = lax.broadcasted_iota(jnp.int32, (rows, width), 0)
    ahead = jnp.where(lane == width - 1, east, pltpu.roll(u, width - 1, 1))
    behind = jnp.where(lane == 0, west, pltpu.roll(u, 1, 1))
    upper = jnp.where(row == rows - 1, north, pltpu.roll(v, rows - 1, 0))
    lower = jnp.where(row == 0, south, pltpu.roll(v, 1, 0))
    return zonal * (ahead - behind) + merid * (upper - lower)


def base_divergence(u_ref, v_ref, own_ref, west_ref, east_ref, south_ref, north_ref, base_ref, is_first, is_last):
    zonal, merid = own_ref[0, :, 0:1], own_ref[1, :, 0:1]
    keep_south = jnp.where(is_first, 0.0, 1.0)
    keep_north = jnp.where(is_last, 0.0, 1.0)
    west = west_ref[...]
    east = east_ref[...]
    for level in range(u_ref.shape[0]):
        base_ref[level] = divergence(
            u_ref[level], v_ref[level], zonal, merid, west[:, level:level + 1], east[:, level:level + 1],
            keep_south * south_ref[level:level + 1, :], keep_north * north_ref[level:level + 1, :],
        )


def added_divergence(ur, vr, own_ref, base_ref, levels):
    zonal, merid = own_ref[0, :, 0:1], own_ref[1, :, 0:1]
    for level in levels:
        base_ref[level] = base_ref[level] + divergence(ur[level], vr[level], zonal, merid, 0.0, 0.0, 0.0, 0.0)


def added_borders(own_ref, border_ref, base_ref, units):
    zonal = own_ref[0, :, 0:1]
    width = base_ref.shape[2]
    lane = lax.broadcasted_iota(jnp.int32, (8, LANE), 1)
    for d in range(border_ref.shape[0]):
        border = border_columns(border_ref[d])
        higher = pltpu.roll(border, LANE - units, 1)
        sides = [unpacked(border, higher, l == 1) for l in range(2)]
        for l in range(units):
            level = d * units + l
            at = l // 2 * 2
            west = jnp.where(lane == 0, zonal * sides[l % 2][:, at:at + 1], 0.0)
            east = jnp.where(lane == LANE - 1, zonal * sides[l % 2][:, at + 1:at + 2], 0.0)
            base_ref[level, :, :LANE] = base_ref[level, :, :LANE] - west
            base_ref[level, :, width - LANE:] = base_ref[level, :, width - LANE:] + east


def pack_edges(u_ref, v_ref, first_col, last_col, first_row, last_row):
    rows, width = u_ref.shape[1:]
    lane = lax.broadcasted_iota(jnp.int32, (rows, LANE), 1)
    first = jnp.zeros((rows, LANE), jnp.float32)
    last = jnp.zeros((rows, LANE), jnp.float32)
    for level in range(u_ref.shape[0]):
        first = jnp.where(lane == level, u_ref[level, :, 0:1], first)
        last = jnp.where(lane == level, u_ref[level, :, width - 1:width], last)
        first_row[level:level + 1, :] = v_ref[level, 0:1, :]
        last_row[level:level + 1, :] = v_ref[level, rows - 1:rows, :]
    first_col[...] = first
    last_col[...] = last


def pack_halo(source, low, high, units):
    rows = source.shape[1]
    for g in range(low.shape[0]):
        for l in range(units):
            low[g, 2 * l:2 * l + 2, :] = source[g * units + l, 0:2, :]
            high[g, 2 * l:2 * l + 2, :] = source[g * units + l, rows - 2:rows, :]


def own_coefs(zc_ref, mc_ref, cutoff_ref, mask_ref, own_ref, first_lat, unfiltered):
    rows = own_ref.shape[1]
    row = lax.broadcasted_iota(jnp.int32, own_ref.shape[1:], 0)
    zonal = jnp.zeros(own_ref.shape[1:], jnp.float32)
    merid = jnp.zeros(own_ref.shape[1:], jnp.float32)
    limit = jnp.zeros(own_ref.shape[1:], jnp.int32)
    for r in range(rows):
        zonal = jnp.where(row == r, zc_ref[r], zonal)
        merid = jnp.where(row == r, mc_ref[r], merid)
        filtered = mask_ref[first_lat + r]
        bound = filtered * cutoff_ref[first_lat + r] + (1 - filtered) * unfiltered
        limit = jnp.where(row == r, bound, limit)
    own_ref[0] = zonal
    own_ref[1] = merid
    own_ref[2] = limit.astype(jnp.float32)


def flipped(index, mask):
    bit = 1
    while bit <= mask:
        if mask & bit:
            index = index + bit * (1 - 2 * (index // bit % 2))
        bit *= 2
    return index


def partner_masks(count):
    return sorted(range(1, count), key=lambda mask: (-bin(mask // 2).count("1"), mask % 2, mask))


def fused_kernel(
    bands, per_band, a_far, zc_far, mc_far, cutoff_far, mask_far, u_far, v_far, w_far, p_far, s_far, table_far, rows_far,
    u_out, v_out, base, winv, p_mid, s_ref, ratio, gain, carry, own_ref, rim_recv,
    x1, x2, d1, ur, vr, ds1, us, vs, w_mid, packed_p, inv, u_ref, v_ref, w_ref, p_ref,
    halo1, low, high, chain_send, chain_recv, table_ref, rows_ref, spec, packed_spec, work, back, filt, sides,
    near, cols_send, cols_recv, rows_send, rows_recv, border_tile, border_send, border_recv, rim_send,
    a_ref, zc_ref, mc_ref, cutoff_ref, mask_ref,
    load_sems, send_sems, recv_sems, edge_send, edge_recv, halo_send, halo_recv, last_send, last_recv, chain_out, chain_in, band_in,
):
    band_me = lax.axis_index("lat")
    lon_me = lax.axis_index("lon")
    lat_rows = u_ref.shape[1]
    units = u_ref.shape[0] // per_band
    channels = rows_ref.shape[0]
    half = channels - 1
    per_unit = channels * lat_rows
    split = u_ref.shape[2] // LANE
    mesh_id = pl.DeviceIdType.MESH
    is_first = band_me == 0
    is_last = band_me == bands - 1
    not_first = jnp.logical_not(is_first)
    not_last = jnp.logical_not(is_last)
    masks = partner_masks(per_band)
    partners = [flipped(lon_me, mask) for mask in masks]

    pairs = (
        (p_far, p_ref), (zc_far, zc_ref), (mc_far, mc_ref), (cutoff_far, cutoff_ref), (mask_far, mask_ref), (a_far, a_ref),
        (rows_far, rows_ref), (u_far, u_ref), (v_far, v_ref), (table_far, table_ref), (s_far, s_ref), (w_far, w_ref),
    )
    loads = [pltpu.make_async_copy(far, here, load_sems.at[n]) for n, (far, here) in enumerate(pairs)]
    loads[0].start()
    barrier = pltpu.get_barrier_semaphore()

    def greet(band, lon):
        pl.semaphore_signal(barrier, inc=1, device_id=(band, lon), device_id_type=mesh_id)

    for partner in partners:
        greet(band_me, partner)
    for there, step in ((not_first, -1), (not_last, 1)):
        @pl.when(there)
        def _():
            greet(band_me + step, lon_me)

    for load in loads[1:]:
        load.start()
    loads[0].wait()
    pl.semaphore_wait(barrier, per_band - 1 + jnp.where(is_first, 0, 1) + jnp.where(is_last, 0, 1))
    for there, step, place in ((not_first, -1, 1), (not_last, 1, 0)):
        @pl.when(there)
        def _():
            pl.semaphore_signal(band_in.at[place], inc=1, device_id=(band_me + step, lon_me), device_id_type=mesh_id)


    def scatter(source, target, sem, unit, count=1):
        for g in partners:
            pltpu.make_async_remote_copy(
                src_ref=source.at[pl.ds(g * units + unit, count)], dst_ref=target.at[pl.ds(lon_me * units + unit, count)],
                send_sem=send_sems.at[sem], recv_sem=recv_sems.at[sem, unit],
                device_id=(band_me, g), device_id_type=mesh_id,
            ).start()
        for n in range(count):
            target[lon_me * units + unit + n] = source[lon_me * units + unit + n]

    def gathered(target, sem, unit, count=1):
        block = target.at[pl.ds(0, (per_band - 1) * count)]
        pltpu.make_async_copy(block, block, recv_sems.at[sem, unit]).wait()

    def sent(source, sem):
        block = source.at[pl.ds(0, (per_band - 1) * units)]
        pltpu.make_async_copy(block, block, send_sems.at[sem]).wait()

    def spread_halo(target):
        def one(source, slot, sem, other):
            for g in partners + [lon_me]:
                pltpu.make_async_remote_copy(
                    src_ref=source.at[g], dst_ref=target.at[slot, lon_me],
                    send_sem=halo_send.at[sem], recv_sem=halo_recv.at[sem],
                    device_id=(other, g), device_id_type=mesh_id,
                ).start()

        @pl.when(not_first)
        def _():
            pl.semaphore_wait(band_in.at[0], 1)
            one(low, 1, 0, band_me - 1)

        @pl.when(not_last)
        def _():
            pl.semaphore_wait(band_in.at[1], 1)
            one(high, 0, 1, band_me + 1)

    def halo_wait(sems, upward):
        @pl.when(not_first)
        def _():
            pltpu.make_async_copy(low, low, sems.at[0 if upward else 1]).wait()

        @pl.when(not_last)
        def _():
            pltpu.make_async_copy(low, low, sems.at[1 if upward else 0]).wait()

    def chain_copy(unit, side):
        return pltpu.make_async_remote_copy(
            src_ref=chain_send.at[side, unit], dst_ref=chain_recv.at[side, unit],
            send_sem=chain_out.at[side], recv_sem=chain_in.at[side, unit],
            device_id=((band_me + bands + 1 - 2 * side) % bands, lon_me), device_id_type=mesh_id,
        )

    def chain_start(unit, tile, place):
        for t in range(channels):
            at = lat_rows * t + place
            chain_send[0, unit, 2 * t:2 * t + 2, :] = packed_spec[tile, at:at + 2, :]
            chain_send[1, unit, 2 * t:2 * t + 2, :] = packed_spec[tile, at + 2:at + 4, :]

        @pl.when(not_last)
        def _():
            chain_copy(unit, 0).start()

        @pl.when(not_first)
        def _():
            chain_copy(unit, 1).start()

    def coef_copy(step, side):
        return pltpu.make_async_remote_copy(
            src_ref=own_ref, dst_ref=near.at[side], send_sem=edge_send.at[4 + side], recv_sem=edge_recv.at[4 + side],
            device_id=((band_me + bands + step) % bands, lon_me), device_id_type=mesh_id,
        )

    for unit in range(0, units, 2):
        scatter(p_ref, x1, 0, unit, 2)
    pack_halo(p_ref, low, high, units)
    spread_halo(halo1)

    for load in loads[1:7]:
        load.wait()
    own_coefs(zc_ref, mc_ref, cutoff_ref, mask_ref, own_ref, band_me * lat_rows, half * TILE)

    @pl.when(not_first)
    def _():
        coef_copy(-1, 1).start()

    @pl.when(not_last)
    def _():
        coef_copy(1, 0).start()

    @pl.when(is_first)
    def _():
        near[0] = jnp.zeros(near.shape[1:], jnp.float32)
        chain_recv[0] = jnp.zeros(chain_recv.shape[1:], jnp.float32)
        for g in range(per_band):
            halo1[0, g] = jnp.zeros(halo1.shape[2:], jnp.float32)

    @pl.when(is_last)
    def _():
        near[1] = jnp.zeros(near.shape[1:], jnp.float32)
        chain_recv[1] = jnp.zeros(chain_recv.shape[1:], jnp.float32)
        for g in range(per_band):
            halo1[1, g] = jnp.zeros(halo1.shape[2:], jnp.float32)

    work[...] = jnp.zeros(work.shape, jnp.float32)
    for load in loads[7:9]:
        load.wait()
    pack_edges(u_ref, v_ref, cols_send.at[0], cols_send.at[1], rows_send.at[0], rows_send.at[1])
    edge_copies = []
    for side, step in ((0, -1), (1, 1)):
        edge_copies.append(pltpu.make_async_remote_copy(
            src_ref=cols_send.at[side], dst_ref=cols_recv.at[side], send_sem=edge_send.at[side], recv_sem=edge_recv.at[side],
            device_id=(band_me, (lon_me + per_band + step) % per_band), device_id_type=mesh_id,
        ))
    for copy in edge_copies:
        copy.start()

    def row_copy(step, side):
        return pltpu.make_async_remote_copy(
            src_ref=rows_send.at[side], dst_ref=rows_recv.at[side], send_sem=edge_send.at[2 + side], recv_sem=edge_recv.at[2 + side],
            device_id=((band_me + bands + step) % bands, lon_me), device_id_type=mesh_id,
        )

    @pl.when(not_first)
    def _():
        row_copy(-1, 0).start()

    @pl.when(not_last)
    def _():
        row_copy(1, 1).start()

    @pl.when(is_first)
    def _():
        rows_recv[1] = jnp.zeros(rows_recv.shape[1:], jnp.float32)

    @pl.when(is_last)
    def _():
        rows_recv[0] = jnp.zeros(rows_recv.shape[1:], jnp.float32)

    for load in loads[9:]:
        load.wait()
    factor_columns(a_ref, s_ref, ratio, inv, gain, carry)
    for level in range(s_ref.shape[0]):
        winv[level] = w_ref[level] * inv[level]

    @pl.when(not_first)
    def _():
        coef_copy(1, 0).wait_recv()

    @pl.when(not_last)
    def _():
        coef_copy(-1, 1).wait_recv()

    filter_terms(rows_ref, own_ref, near, filt, sides)

    def circles(source, first, count, stride):
        return [
            [source[d * stride + first + n, :, h * LANE:(h + 1) * LANE] for d in range(per_band) for h in range(split)]
            for n in range(count)
        ]

    def forward(tiles, places):
        for n, xs in enumerate(tiles):
            forward_fill(xs, rows_ref, work, n * per_unit)
        used = len(tiles) * per_unit
        value = three_products(work[0:whole_tiles(used), :], table_ref)
        for n, place in enumerate(places):
            spec[place] = value[n * per_unit:(n + 1) * per_unit]
        return value

    def inverse(count):
        back[0:whole_tiles(count * per_unit), :] = three_products(work[0:whole_tiles(count * per_unit), :], table_ref)

    merid = own_ref[1, :, 0:1]
    pair_count = units // 2
    halo_wait(halo_recv, False)
    forward([
        [halo1[slot, d, :, h * LANE:(h + 1) * LANE] for d in range(per_band) for h in range(split)] for slot in range(2)
    ], [units, units + 1])
    for pair in range(pair_count):
        gathered(x1, 0, 2 * pair, 2)
        forward(circles(x1, 2 * pair, 2, units), [2 * pair, 2 * pair + 1])
        for t in range(channels):
            both = []
            for l in (2 * pair, 2 * pair + 1):
                at = lat_rows * t + 2 * l
                own, row, mid, v_south, v_north = merid_terms(spec, l, t, filt, sides, spec.at[units], spec.at[units + 1], at)
                upper = jnp.where(row == lat_rows - 1, v_north, pltpu.roll(mid, lat_rows - 1, 0))
                lower = jnp.where(row == 0, v_south, pltpu.roll(mid, 1, 0))
                both.append(filt[t, 2] * own + merid * (upper - lower))
            for half_at in range(2):
                at = half_at * per_unit + lat_rows * t
                work[at:at + lat_rows, :] = packed_half(*both, half_at == 1)
        inverse(2)
        put_blocks(ds1, inverse_blocks(back, rows_ref, 0), pair, units)
        scatter(ds1, d1, 1, pair)
        put_blocks(ds1, inverse_blocks(back, rows_ref, per_unit), pair_count + pair, units)
    for pair in range(pair_count):
        scatter(ds1, d1, 1, pair_count + pair)

    for copy in edge_copies:
        copy.wait_recv()

    @pl.when(not_first)
    def _():
        row_copy(1, 1).wait_recv()

    @pl.when(not_last)
    def _():
        row_copy(-1, 0).wait_recv()

    base_divergence(
        u_ref, v_ref, own_ref, cols_recv.at[1], cols_recv.at[0], rows_recv.at[1], rows_recv.at[0], base,
        is_first, is_last,
    )
    def first_spread(level):
        tile = d1[level // units * units + level % units // 2]
        return base[level] + (pltpu.roll(tile, 2 if level % 2 else lat_rows - 2, 0))

    def second_spread(level):
        place = level // units * units + level % units // 2
        return base[level] + unpacked(d1[place], d1[place + pair_count], level % 2 == 1)

    for half_at, spread in enumerate((first_spread, second_spread)):
        for pair in range(pair_count):
            gathered(d1, 1, half_at * pair_count + pair)
        solve_columns(s_ref, winv, p_ref, spread, ratio, gain, carry, vs, p_mid)
        for pair in range(pair_count):
            for d in range(per_band):
                level = d * units + 2 * pair
                packed_p[d * units + half_at * pair_count + pair] = packed_half(p_mid[level], p_mid[level + 1], half_at == 1)
            scatter(packed_p, x2, 2, half_at * pair_count + pair)
    for level in range(s_ref.shape[0]):
        winv[level] = vs[level] * inv[level]

    for tile in range(units):
        pair, half_at = tile % pair_count, tile // pair_count
        gathered(x2, 2, tile)
        value = forward(circles(x2, tile, 1, units), [])
        for t in range(channels):
            rows = slice(lat_rows * t, lat_rows * (t + 1))
            total = packed_half(spec[2 * pair, rows, :], spec[2 * pair + 1, rows, :], half_at == 1) + value[rows]
            packed_spec[tile, rows, :] = total
            work[rows, :] = filt[t, 3 + half_at] * total
        for l in range(2):
            if not half_at:
                chain_start(2 * pair + l, tile, 4 * l)
                continue
            for t in range(channels):
                rows = slice(lat_rows * t, lat_rows * (t + 1))
                spec[2 * pair + l, rows, :] = unpacked(packed_spec[pair, rows, :], packed_spec[tile, rows, :], l == 1)
        zonal = packed_half(own_ref[0], own_ref[0], half_at == 1)
        inverse(1)
        moved = [-zonal * x for x in circle_diff(inverse_blocks(back, rows_ref, 0))]
        put_blocks(us, moved, tile, units)
        scatter(us, ur, 3, tile)
        border_tiles(border_tile, moved, tile)
    border_rows(border_tile, border_send)

    def last_copy(source, target, n, g):
        return pltpu.make_async_remote_copy(
            src_ref=source.at[pl.ds(g, 1)], dst_ref=target.at[pl.ds(lon_me, 1)], send_sem=last_send.at[n], recv_sem=last_recv.at[n],
            device_id=(band_me, g), device_id_type=mesh_id,
        )

    def last_scatter(source, target, n):
        for g in partners:
            last_copy(source, target, n, g).start()
        target[lon_me] = source[lon_me]

    last_scatter(border_send, border_recv, 0)
    rim_at = per_unit
    for unit in range(units):
        @pl.when(not_first)
        def _():
            chain_copy(unit, 0).wait_recv()

        @pl.when(not_last)
        def _():
            chain_copy(unit, 1).wait_recv()

        for t in range(channels):
            own, row, mid, v_south, v_north = merid_terms(
                spec, unit, t, filt, sides, chain_recv.at[0, unit], chain_recv.at[1, unit], 2 * t,
            )
            work[lat_rows * t:lat_rows * (t + 1), :] = mid
            rim = rim_at + lat_rows * t + 2 * unit
            work[rim:rim + 1, :] = v_south
            work[rim + 1:rim + 2, :] = v_north
        inverse(2 if unit == units - 1 else 1)
        put_blocks(vs, inverse_blocks(back, rows_ref, 0), unit, units)
        scatter(vs, vr, 4, unit)
    rims = inverse_blocks(back, rows_ref, rim_at)
    for b, value in enumerate(rims):
        rim_send[b // split, :, (b % split) * LANE:(b % split + 1) * LANE] = value

    last_scatter(rim_send, rim_recv, 1)

    def last_wait(target, sems, n):
        block = target.at[pl.ds(0, per_band - 1)]
        pltpu.make_async_copy(block, block, sems.at[n]).wait()

    for tile in range(units):
        gathered(ur, 3, tile)
        for d in range(per_band if tile >= pair_count else 0):
            for l in range(2):
                level = d * units + 2 * (tile - pair_count) + l
                moved = unpacked(ur[d * units + tile - pair_count], ur[d * units + tile], l == 1)
                u_out[level] = u_ref[level] + moved
                w_mid[level] = moved
    last_wait(border_recv, last_recv, 0)
    added_borders(own_ref, border_recv, base, units)
    for unit in range(units):
        gathered(vr, 4, unit)
        own_levels = [d * units + unit for d in range(per_band)]
        for level in own_levels:
            v_out[level] = v_ref[level] + vr[level]
        added_divergence(w_mid, vr, own_ref, base, own_levels)
    last_wait(rim_recv, last_recv, 1)
    for source, sem in ((p_ref, 0), (ds1, 1), (packed_p, 2), (us, 3), (vs, 4)):
        sent(source, sem)
    last_wait(border_send, last_send, 0)
    last_wait(rim_send, last_send, 1)
    halo_wait(halo_send, True)
    for copy in edge_copies:
        copy.wait_send()

    @pl.when(not_first)
    def _():
        pltpu.make_async_copy(chain_send.at[1], chain_send.at[1], chain_out.at[1]).wait()
        coef_copy(-1, 1).wait_send()
        row_copy(-1, 0).wait_send()

    @pl.when(not_last)
    def _():
        pltpu.make_async_copy(chain_send.at[0], chain_send.at[0], chain_out.at[0]).wait()
        coef_copy(1, 0).wait_send()
        row_copy(1, 1).wait_send()


def deliver_kernel(
    units, u_ref, v_ref, base, winv, p_mid, s_ref, ratio, gain, carry, own_ref, rim_ref, u_out, v_out, w_out, p_out, w_end, p_end, sems,
):
    copies = [
        pltpu.make_async_copy(source, target, sems.at[n])
        for n, (source, target) in enumerate(((u_ref, u_out), (v_ref, v_out), (w_end, w_out), (p_end, p_out)))
    ]
    copies[0].start()
    copies[1].start()
    row = lax.broadcasted_iota(jnp.int32, u_ref.shape[1:], 0)
    rows = u_ref.shape[1]
    merid = own_ref[1, :, 0:1]
    south = jnp.where(row == 0, -merid, 0.0)
    north = jnp.where(row == rows - 1, merid, 0.0)

    def spread(level):
        d, l = level // units, 2 * (level % units)
        return base[level] + south * rim_ref[d, l:l + 1, :] + north * rim_ref[d, l + 1:l + 2, :]

    solve_columns(s_ref, winv, p_mid, spread, ratio, gain, carry, w_end, p_end)
    copies[2].start()
    copies[3].start()
    for copy in copies:
        copy.wait()


def deliver(units, arrays):
    shape = arrays[0].shape
    return pl.pallas_call(
        functools.partial(deliver_kernel, units),
        out_shape=(jax.ShapeDtypeStruct(shape, jnp.float32),) * 4,
        in_specs=[pl.BlockSpec(memory_space=pltpu.VMEM)] * len(arrays),
        out_specs=(pl.BlockSpec(memory_space=pl.ANY),) * 4,
        scratch_shapes=[pltpu.VMEM(shape, jnp.float32)] * 2 + [pltpu.SemaphoreType.DMA((4,))],
        compiler_params=pltpu.CompilerParams(vmem_limit_bytes=FINISH_VMEM),
    )(*arrays)


def level_body(
    tables,
    zonal_wind,
    merid_wind,
    vertical_wind,
    pressure,
    zonal_coef,
    merid_coef,
    level_coef,
    sound_coef,
    cutoff,
    filter_mask,
):
    table, rows = (jnp.asarray(t) for t in tables)
    channels = rows.shape[0]
    bands = lax.axis_size("lat")
    per_band = lax.axis_size("lon")
    levels, lat_rows, width = pressure.shape
    units = levels // per_band
    per_unit = channels * lat_rows
    vmem = pl.BlockSpec(memory_space=pltpu.VMEM)
    far = pl.BlockSpec(memory_space=pl.ANY)

    def scratch(*shape):
        return pltpu.VMEM(shape, jnp.float32)

    field = scratch(*pressure.shape)
    halo = scratch(2, per_band, lat_rows, width)
    chain = scratch(2, units, -(-2 * channels // 8) * 8, TILE)
    spare = scratch(whole_tiles(2 * per_unit), TILE)
    dma = pltpu.SemaphoreType.DMA
    operands = (
        level_coef, zonal_coef, merid_coef, cutoff, filter_mask,
        zonal_wind, merid_wind, vertical_wind, pressure, sound_coef, table, rows,
    )
    results = pl.pallas_call(
        functools.partial(fused_kernel, bands, per_band),
        out_shape=(pltpu.VMEM(pressure.shape, jnp.float32),) * 9 + (
            pltpu.VMEM((3, lat_rows, LANE), jnp.float32), pltpu.VMEM((per_band, lat_rows, width), jnp.float32),
        ),
        in_specs=[far] * len(operands),
        out_specs=(vmem,) * 11,
        scratch_shapes=[field] * 15 + [halo, scratch(per_band, lat_rows, width), scratch(per_band, lat_rows, width), chain, chain] + [
            pltpu.VMEM(table.shape, table.dtype), scratch(*rows.shape),
            scratch(units + 2, per_unit, TILE), scratch(units, per_unit, TILE), spare, spare,
            scratch(channels, 5, lat_rows, TILE), scratch(channels, 8, TILE),
            scratch(2, 3, lat_rows, LANE),
            scratch(2, lat_rows, LANE), scratch(2, lat_rows, LANE),
            scratch(2, levels, width), scratch(2, levels, width),
            scratch(per_band, lat_rows, LANE), scratch(per_band, 1, LANE), scratch(per_band, 1, LANE),
            scratch(per_band, lat_rows, width),
            pltpu.SMEM(level_coef.shape, jnp.float32), pltpu.SMEM(zonal_coef.shape, jnp.float32),
            pltpu.SMEM(merid_coef.shape, jnp.float32), pltpu.SMEM(cutoff.shape, jnp.int32),
            pltpu.SMEM(filter_mask.shape, jnp.int32),
            dma((len(operands),)), dma((5,)), dma((5, units)), dma((6,)), dma((6,)), dma((2,)), dma((2,)), dma((2,)), dma((2,)), dma((2,)), dma((2, units)),
            pltpu.SemaphoreType.REGULAR((2,)),
        ],
        compiler_params=pltpu.CompilerParams(collective_id=0, has_side_effects=True, vmem_limit_bytes=FUSED_VMEM),
    )(*[pltpu.with_memory_space_constraint(x, pltpu.HBM) for x in operands])
    return deliver(units, results)


def body(tables, *arrays):
    pressure = arrays[3]
    per_band = lax.axis_size("lon")
    levels, lat_rows, width = pressure.shape
    fits = lat_rows == 8 and levels == 4 * per_band and levels <= LANE and width % LANE == 0 and per_band == 8
    if fits:
        return level_body(tables, *arrays)
    return wide_body(*arrays)


def solution(mesh):
    in_specs = (
        P(None, "lat", "lon"),
        P(None, "lat", "lon"),
        P(None, "lat", "lon"),
        P(None, "lat", "lon"),
        P("lat"),
        P("lat"),
        P(),
        P(None, "lat", "lon"),
        P(),
        P(),
    )
    out_specs = (
        P(None, "lat", "lon"),
        P(None, "lat", "lon"),
        P(None, "lat", "lon"),
        P(None, "lat", "lon"),
    )

    def whole(*arrays):
        tables = circle_tables(arrays[0].shape[2])
        step = jax.shard_map(functools.partial(body, tables), mesh=mesh, in_specs=in_specs, out_specs=out_specs, check_vma=False)
        return step(*arrays)

    return whole
```

```python
import functools
import math

import ml_dtypes
import numpy as np
import jax
import jax.numpy as jnp
from jax import lax
from jax.experimental import pallas as pl
from jax.experimental.pallas import tpu as pltpu
from jax.sharding import PartitionSpec as P

SUBSTEPS = 2
FUSED_VMEM = 40 * 2 ** 20
FINISH_VMEM = 4 * 2 ** 20


def extended(block, sides, width):
    for axis, dim in sides:
        count = lax.axis_size(axis)
        forward = [(i, i + 1) for i in range(count - 1)]
        forward.append((count - 1, 0))
        backward = [(target, source) for source, target in forward]
        low = lax.ppermute(
            lax.slice_in_dim(block, block.shape[dim] - width, None, axis=dim), axis, forward
        )
        high = lax.ppermute(lax.slice_in_dim(block, 0, width, axis=dim), axis, backward)
        block = jnp.concatenate([low, block, high], axis=dim)
    return block


def rim_fix(padded, lat_dim):
    band_index = lax.axis_index("lat")
    bands = lax.axis_size("lat")
    extent = padded.shape[lat_dim]
    position = lax.broadcasted_iota(jnp.int32, padded.shape, lat_dim)
    first_edge = jnp.logical_and(position == 0, band_index == 0)
    final_edge = jnp.logical_and(position == extent - 1, band_index == bands - 1)
    return jnp.where(jnp.logical_or(first_edge, final_edge), 0.0, padded)


def dft_tables(length):
    half_len = length // 2
    sample = lax.broadcasted_iota(jnp.int32, (length, length), 0)
    column = lax.broadcasted_iota(jnp.int32, (length, length), 1)
    is_cosine = column <= half_len
    wavenum = jnp.where(is_cosine, column, column - half_len)
    phase = sample * wavenum % length
    angle = 2.0 * math.pi / length * phase.astype(jnp.float32)
    forward = jnp.where(is_cosine, jnp.cos(angle), jnp.sin(angle))
    single = jnp.logical_and(is_cosine, jnp.logical_or(wavenum == 0, wavenum == half_len))
    weight = jnp.where(single, 1.0, 2.0) / length
    inverse = jnp.transpose(forward * weight)
    wave_row = wavenum[0].astype(jnp.float32)
    return (forward, inverse, wave_row)


def damping(wave_row, limits):
    bound_col = limits[:, None]
    ratio = bound_col / jnp.maximum(wave_row[None, :], 1.0)
    return jnp.where(wave_row[None, :] > bound_col, ratio * ratio, 1.0)


def transform_band(block, limits, forward, inverse, wave_row):
    circles = lax.all_to_all(block, "lon", split_axis=1, concat_axis=3, tiled=True)
    spectra = jnp.einsum("vetj,jc->vetc", circles, forward, precision=lax.Precision.HIGHEST)
    scaled = spectra * damping(wave_row, limits)
    damped = jnp.einsum("vetc,cj->vetj", scaled, inverse, precision=lax.Precision.HIGHEST)
    return lax.all_to_all(damped, "lon", split_axis=3, concat_axis=1, tiled=True)


def filtered_increments(increments, own_flags, own_limits, forward, inverse, wave_row):
    flag_cols = own_flags[:, None]
    damped = transform_band(increments, own_limits, forward, inverse, wave_row)
    return jnp.where(flag_cols, damped, increments)


def column_solve(vertical_wind, pstar, level_coef, sound_coef):
    levels = vertical_wind.shape[0]
    zero_slab = jnp.zeros_like(vertical_wind[0])
    ratios = []
    values = []
    prev_ratio = zero_slab
    prev_value = zero_slab
    for level in range(levels):
        alpha = level_coef[level]
        below = alpha * sound_coef[level]
        if level + 1 < levels:
            above = alpha * sound_coef[level + 1]
            rhs = vertical_wind[level] - alpha * (pstar[level + 1] - pstar[level])
        else:
            above = zero_slab
            rhs = vertical_wind[level] + alpha * pstar[level]
        pivot = 1.0 + below + above + below * prev_ratio
        prev_ratio = -above / pivot
        prev_value = (rhs + below * prev_value) / pivot
        ratios.append(prev_ratio)
        values.append(prev_value)
    solved = [zero_slab] * levels
    upper_value = values[levels - 1]
    solved[levels - 1] = upper_value
    for level in range(levels - 2, -1, -1):
        upper_value = values[level] - ratios[level] * upper_value
        solved[level] = upper_value
    new_wind = jnp.stack(solved)
    wind_below = jnp.concatenate([zero_slab[None], new_wind[:-1]], axis=0)
    new_pressure = pstar - sound_coef * (new_wind - wind_below)
    return (new_wind, new_pressure)


def wide_body(
    zonal_wind,
    merid_wind,
    vertical_wind,
    pressure,
    zonal_coef,
    merid_coef,
    level_coef,
    sound_coef,
    cutoff,
    filter_mask,
):
    lat_rows = pressure.shape[1]
    start = lax.axis_index("lat") * lat_rows
    own_flags = lax.dynamic_slice_in_dim(filter_mask, start, lat_rows) > 0
    own_limits = lax.dynamic_slice_in_dim(cutoff, start, lat_rows).astype(jnp.float32)
    forward, inverse, wave_row = dft_tables(pressure.shape[2] * lax.axis_size("lon"))
    zonal_rows = zonal_coef[None, :, None]
    merid_rows = merid_coef[None, :, None]
    for step in range(SUBSTEPS):
        padded = extended(pressure, (("lat", 1), ("lon", 2)), 1)
        padded = rim_fix(padded, 1)
        zonal_step = -zonal_rows * (padded[:, 1:-1, 2:] - padded[:, 1:-1, :-2])
        merid_step = -merid_rows * (padded[:, 2:, 1:-1] - padded[:, :-2, 1:-1])
        increments = jnp.stack([zonal_step, merid_step])
        damped = filtered_increments(increments, own_flags, own_limits, forward, inverse, wave_row)
        winds = jnp.stack([zonal_wind, merid_wind]) + damped
        wind_pad = extended(winds, (("lat", 2), ("lon", 3)), 1)
        wind_pad = rim_fix(wind_pad, 2)
        diverge = zonal_rows * (wind_pad[0, :, 1:-1, 2:] - wind_pad[0, :, 1:-1, :-2])
        diverge = diverge + merid_rows * (wind_pad[1, :, 2:, 1:-1] - wind_pad[1, :, :-2, 1:-1])
        pstar = pressure - sound_coef * diverge
        vertical_wind, pressure = column_solve(vertical_wind, pstar, level_coef, sound_coef)
        zonal_wind = winds[0]
        merid_wind = winds[1]
    return (zonal_wind, merid_wind, vertical_wind, pressure)


LANE = 128
TILE = 2 * LANE


def circle_tables(length):
    blocks = length // LANE
    half = blocks // 2
    m = np.arange(LANE, dtype=np.float64)[:, None]
    c = np.arange(LANE)[None, :]
    angle = 2 * np.pi * ((m * c) % LANE) / LANE
    cos, sin = np.cos(angle) / np.sqrt(LANE), np.sin(angle) / np.sqrt(LANE)
    table = np.block([[cos, -sin], [sin, cos]])
    high = table.astype(ml_dtypes.bfloat16)
    rest = (table - high.astype(np.float64)).astype(ml_dtypes.bfloat16)
    rows = np.zeros((half + 1, 8, TILE), np.float32)
    for k1 in range(half + 1):
        k = k1 + blocks * c[0]
        waves = np.tile(np.minimum(k, length - k), 2)
        scale = (1.0 if k1 in (0, half) else 2.0) / blocks
        turn = 2 * np.pi * m[:, 0] * k1 / length
        rows[k1, 0] = waves
        rows[k1, 1] = 4.0 * np.sin(2 * np.pi * waves / length) ** 2
        rows[k1, 2] = np.where(np.arange(TILE) < LANE, scale, -scale)
        rows[k1, 3] = np.concatenate([np.cos(turn), np.sin(turn)])
    return np.stack([high, rest]), rows


def split_parts(value):
    high = value.astype(jnp.bfloat16)
    rest = (value - high.astype(jnp.float32)).astype(jnp.bfloat16)
    return high, rest


def three_products(value, table_ref):
    high, rest = split_parts(value)
    dims = (((1,), (0,)), ((), ()))
    rows = value.shape[0]
    table = table_ref[0]
    both = lax.dot_general(jnp.concatenate([high, rest], axis=0), table, dims, preferred_element_type=jnp.float32)
    corr = lax.dot_general(high, table_ref[1], dims, preferred_element_type=jnp.float32)
    return both[:rows] + (both[rows:] + corr)


def weighted(terms):
    total = None
    for coef, value in terms:
        if abs(coef) < 1e-12:
            continue
        if abs(abs(coef) - 1.0) < 1e-12:
            term = value
        else:
            term = abs(coef) * value
        if total is None:
            total = term if coef > 0 else -term
        else:
            total = total + term if coef > 0 else total - term
    return total


def coarse_forward(xs):
    count = len(xs)
    half = count // 2
    even = {b: xs[b] + xs[count - b] for b in range(1, half)}
    odd = {b: xs[b] - xs[count - b] for b in range(1, half)}
    real, imag = [], {}
    for k in range(half + 1):
        ends = xs[0] + xs[half] if k % 2 == 0 else xs[0] - xs[half]
        real.append(weighted([(1.0, ends)] + [(math.cos(2 * math.pi * b * k / count), even[b]) for b in range(1, half)]))
    for k in range(1, half):
        imag[k] = weighted([(-math.sin(2 * math.pi * b * k / count), odd[b]) for b in range(1, half)])
    pairs = [(real[0], real[half])] + [(real[k], imag[k]) for k in range(1, half)]
    return pairs


def coarse_inverse(pairs):
    half = len(pairs)
    count = 2 * half
    first, last = pairs[0]
    xs = [None] * count
    for b in range(half + 1):
        ends = first + last if b % 2 == 0 else first - last
        cos_part = weighted([(1.0, ends)] + [(math.cos(2 * math.pi * b * k / count), pairs[k][0]) for k in range(1, half)])
        if b in (0, half):
            xs[b] = cos_part
        else:
            sin_part = weighted([(-math.sin(2 * math.pi * b * k / count), pairs[k][1]) for k in range(1, half)])
            xs[b] = cos_part + sin_part
            xs[count - b] = cos_part - sin_part
    return xs


def whole_tiles(count):
    return -(-count // 16) * 16


def forward_fill(xs, rows_ref, work_ref, start):
    pairs = coarse_forward(xs)
    half = len(pairs)
    first, last = pairs[0]
    for t in range(half + 1):
        cos, sin = rows_ref[t, 3:4, :LANE], rows_ref[t, 3:4, LANE:]
        if t == 0:
            left, right = first, jnp.zeros_like(first)
        elif t == half:
            left, right = last * cos, -(last * sin)
        else:
            real, imag = pairs[t]
            left, right = real * cos + imag * sin, imag * cos - real * sin
        work_ref[start + 8 * t:start + 8 * t + 8, :LANE] = left
        work_ref[start + 8 * t:start + 8 * t + 8, LANE:] = right


def inverse_blocks(back_ref, rows_ref, start):
    half = rows_ref.shape[0] - 1
    pairs = []
    ends = []
    for t in range(half + 1):
        left = back_ref[start + 8 * t:start + 8 * t + 8, :LANE]
        right = back_ref[start + 8 * t:start + 8 * t + 8, LANE:]
        cos, sin = rows_ref[t, 3:4, :LANE], rows_ref[t, 3:4, LANE:]
        if t == 0:
            ends.append(left)
        elif t == half:
            ends.append(left * cos + right * sin)
        else:
            pairs.append((left * cos + right * sin, left * sin - right * cos))
    return coarse_inverse([tuple(ends)] + pairs)


def put_blocks(out_ref, xs, unit, units):
    split = out_ref.shape[2] // LANE
    for b, value in enumerate(xs):
        out_ref[(b // split) * units + unit, :, (b % split) * LANE:(b % split + 1) * LANE] = value


def circle_diff(xs):
    count = len(xs)
    lane = lax.broadcasted_iota(jnp.int32, xs[0].shape, 1)
    ahead = [pltpu.roll(x, LANE - 1, 1) for x in xs]
    behind = [pltpu.roll(x, 1, 1) for x in xs]
    out = []
    for b in range(count):
        nxt = jnp.where(lane == LANE - 1, ahead[(b + 1) % count], ahead[b])
        prv = jnp.where(lane == 0, behind[(b - 1) % count], behind[b])
        out.append(nxt - prv)
    return out


def border_rows(edge_ref, send_ref):
    for d in range(edge_ref.shape[0]):
        send_ref[d] = jnp.sum(pltpu.roll(edge_ref[d], 0, 1, stride=8, stride_axis=0), axis=0, keepdims=True)


def border_columns(row):
    value = jnp.broadcast_to(row, (8, LANE))
    place = lax.broadcasted_iota(jnp.int32, (8, LANE), 0)
    for bit in (1, 2, 4):
        value = jnp.where(place // bit % 2 == 1, pltpu.roll(value, LANE - 8 * bit, 1), value)
    return value


def border_tiles(edge_ref, xs, unit):
    count = len(xs)
    split = count // edge_ref.shape[0]
    lane = lax.broadcasted_iota(jnp.int32, xs[0].shape, 1)
    turned = [pltpu.roll(x, 2 * unit + 1, 1) for x in xs]
    for d in range(edge_ref.shape[0]):
        west, east = turned[(d * split - 1) % count], turned[(d * split + split) % count]
        kept = edge_ref[d] if unit else jnp.zeros_like(west)
        edge_ref[d] = jnp.where(lane == 2 * unit, west, jnp.where(lane == 2 * unit + 1, east, kept))


def filter_values(limit, wave, scale):
    quotient = limit / jnp.maximum(wave, 1.0)
    return jnp.where(wave > limit, quotient * quotient, 1.0) * scale


def filter_terms(rows_ref, own_ref, near_ref, filt_ref, side_ref):
    rows = own_ref.shape[1]
    zonal, merid, limit = own_ref[0, :, 0:1], own_ref[1, :, 0:1], own_ref[2, :, 0:1]
    for t in range(rows_ref.shape[0]):
        wave, sines, scale = rows_ref[t, 0:1, :], rows_ref[t, 1:2, :], rows_ref[t, 2:3, :]
        factor = filter_values(limit, wave, scale)
        filt_ref[t, 0] = factor
        filt_ref[t, 1] = merid * factor
        filt_ref[t, 2] = (zonal * zonal) * sines * factor
        filt_ref[t, 3] = packed_half(factor, factor, False)
        filt_ref[t, 4] = packed_half(factor, factor, True)
        south = near_ref[0, 1, rows - 1:rows, 0:1] * filter_values(near_ref[0, 2, rows - 1:rows, 0:1], wave, scale)
        north = near_ref[1, 1, 0:1, 0:1] * filter_values(near_ref[1, 2, 0:1, 0:1], wave, scale)
        side_ref[t, 0:1, :] = south
        side_ref[t, 1:2, :] = north


def merid_terms(spec_ref, unit, t, filt_ref, side_ref, south_ref, north_ref, at):
    tile = spec_ref.shape[1] // filt_ref.shape[0]
    own = spec_ref[unit, tile * t:tile * t + tile, :]
    row = lax.broadcasted_iota(jnp.int32, own.shape, 0)
    below_far, below = south_ref[at:at + 1, :], south_ref[at + 1:at + 2, :]
    above, above_far = north_ref[at:at + 1, :], north_ref[at + 1:at + 2, :]
    upper = jnp.where(row == tile - 1, above, pltpu.roll(own, tile - 1, 0))
    lower = jnp.where(row == 0, below, pltpu.roll(own, 1, 0))
    mid = -filt_ref[t, 1] * (upper - lower)
    v_south = -side_ref[t, 0:1, :] * (own[0:1] - below_far)
    v_north = -side_ref[t, 1:2, :] * (above_far - own[tile - 1:tile])
    return own, row, mid, v_south, v_north


def factor_columns(a_ref, s_ref, ratio_ref, inv_ref, gain_ref, carry_ref):
    levels = s_ref.shape[0]
    prev = jnp.zeros(s_ref.shape[1:], jnp.float32)
    for level in range(levels):
        alpha = a_ref[level]
        below = alpha * s_ref[level]
        above = alpha * s_ref[level + 1] if level + 1 < levels else jnp.zeros_like(below)
        inv = 1.0 / (1.0 + below + above + below * prev)
        prev = -above * inv
        ratio_ref[level] = prev
        inv_ref[level] = inv
        gain_ref[level] = alpha * inv
        carry_ref[level] = below * inv


def solve_columns(s_ref, winv_ref, p_ref, spread, ratio_ref, gain_ref, carry_ref, w_out, p_out):
    levels = s_ref.shape[0]

    def star(level):
        return p_ref[level] - s_ref[level] * spread(level)

    here = star(0)
    prev = jnp.zeros_like(here)
    for level in range(levels):
        p_out[level] = here
        nxt = star(level + 1) if level + 1 < levels else jnp.zeros_like(here)
        prev = (winv_ref[level] - gain_ref[level] * (nxt - here)) + carry_ref[level] * prev
        w_out[level] = prev
        here = nxt
    upper = w_out[levels - 1]
    for level in range(levels - 1, 0, -1):
        lower = w_out[level - 1] - ratio_ref[level - 1] * upper
        w_out[level - 1] = lower
        p_out[level] = p_out[level] - s_ref[level] * (upper - lower)
        upper = lower
    p_out[0] = p_out[0] - s_ref[0] * upper


def packed_half(first, second, inner):
    rows = first.shape[0]
    row = lax.broadcasted_iota(jnp.int32, first.shape, 0)
    shift = rows - 2 if inner else 2
    return jnp.where(row < rows // 2, pltpu.roll(first, shift, 0), pltpu.roll(second, rows - shift, 0))


def unpacked(outer, inner, second):
    rows = outer.shape[0]
    row = lax.broadcasted_iota(jnp.int32, outer.shape, 0)
    shift = rows - 2 if second else 2
    middle = jnp.logical_and(row >= 2, row < rows - 2)
    return jnp.where(middle, pltpu.roll(inner, shift, 0), pltpu.roll(outer, rows - shift, 0))


def divergence(u, v, zonal, merid, west, east, south, north):
    rows, width = u.shape
    lane = lax.broadcasted_iota(jnp.int32, (rows, width), 1)
    row = lax.broadcasted_iota(jnp.int32, (rows, width), 0)
    ahead = jnp.where(lane == width - 1, east, pltpu.roll(u, width - 1, 1))
    behind = jnp.where(lane == 0, west, pltpu.roll(u, 1, 1))
    upper = jnp.where(row == rows - 1, north, pltpu.roll(v, rows - 1, 0))
    lower = jnp.where(row == 0, south, pltpu.roll(v, 1, 0))
    return zonal * (ahead - behind) + merid * (upper - lower)


def base_divergence(u_ref, v_ref, own_ref, west_ref, east_ref, south_ref, north_ref, base_ref, is_first, is_last):
    zonal, merid = own_ref[0, :, 0:1], own_ref[1, :, 0:1]
    keep_south = jnp.where(is_first, 0.0, 1.0)
    keep_north = jnp.where(is_last, 0.0, 1.0)
    west = west_ref[...]
    east = east_ref[...]
    for level in range(u_ref.shape[0]):
        base_ref[level] = divergence(
            u_ref[level], v_ref[level], zonal, merid, west[:, level:level + 1], east[:, level:level + 1],
            keep_south * south_ref[level:level + 1, :], keep_north * north_ref[level:level + 1, :],
        )


def added_divergence(ur, vr, own_ref, base_ref, levels):
    zonal, merid = own_ref[0, :, 0:1], own_ref[1, :, 0:1]
    for level in levels:
        base_ref[level] = base_ref[level] + divergence(ur[level], vr[level], zonal, merid, 0.0, 0.0, 0.0, 0.0)


def added_borders(own_ref, border_ref, base_ref, units):
    zonal = own_ref[0, :, 0:1]
    width = base_ref.shape[2]
    lane = lax.broadcasted_iota(jnp.int32, (8, LANE), 1)
    for d in range(border_ref.shape[0]):
        border = border_columns(border_ref[d])
        higher = pltpu.roll(border, LANE - units, 1)
        sides = [unpacked(border, higher, l == 1) for l in range(2)]
        for l in range(units):
            level = d * units + l
            at = l // 2 * 2
            west = jnp.where(lane == 0, zonal * sides[l % 2][:, at:at + 1], 0.0)
            east = jnp.where(lane == LANE - 1, zonal * sides[l % 2][:, at + 1:at + 2], 0.0)
            base_ref[level, :, :LANE] = base_ref[level, :, :LANE] - west
            base_ref[level, :, width - LANE:] = base_ref[level, :, width - LANE:] + east


def pack_edges(u_ref, v_ref, first_col, last_col, first_row, last_row):
    rows, width = u_ref.shape[1:]
    lane = lax.broadcasted_iota(jnp.int32, (rows, LANE), 1)
    first = jnp.zeros((rows, LANE), jnp.float32)
    last = jnp.zeros((rows, LANE), jnp.float32)
    for level in range(u_ref.shape[0]):
        first = jnp.where(lane == level, u_ref[level, :, 0:1], first)
        last = jnp.where(lane == level, u_ref[level, :, width - 1:width], last)
        first_row[level:level + 1, :] = v_ref[level, 0:1, :]
        last_row[level:level + 1, :] = v_ref[level, rows - 1:rows, :]
    first_col[...] = first
    last_col[...] = last


def pack_halo(source, low, high, units):
    rows = source.shape[1]
    for g in range(low.shape[0]):
        for l in range(units):
            low[g, 2 * l:2 * l + 2, :] = source[g * units + l, 0:2, :]
            high[g, 2 * l:2 * l + 2, :] = source[g * units + l, rows - 2:rows, :]


def own_coefs(zc_ref, mc_ref, cutoff_ref, mask_ref, own_ref, first_lat, unfiltered):
    rows = own_ref.shape[1]
    row = lax.broadcasted_iota(jnp.int32, own_ref.shape[1:], 0)
    zonal = jnp.zeros(own_ref.shape[1:], jnp.float32)
    merid = jnp.zeros(own_ref.shape[1:], jnp.float32)
    limit = jnp.zeros(own_ref.shape[1:], jnp.int32)
    for r in range(rows):
        zonal = jnp.where(row == r, zc_ref[r], zonal)
        merid = jnp.where(row == r, mc_ref[r], merid)
        filtered = mask_ref[first_lat + r]
        bound = filtered * cutoff_ref[first_lat + r] + (1 - filtered) * unfiltered
        limit = jnp.where(row == r, bound, limit)
    own_ref[0] = zonal
    own_ref[1] = merid
    own_ref[2] = limit.astype(jnp.float32)


def flipped(index, mask):
    bit = 1
    while bit <= mask:
        if mask & bit:
            index = index + bit * (1 - 2 * (index // bit % 2))
        bit *= 2
    return index


def partner_masks(count):
    return sorted(range(1, count), key=lambda mask: (-bin(mask // 2).count("1"), mask % 2, mask))


def fused_kernel(
    bands, per_band, a_far, zc_far, mc_far, cutoff_far, mask_far, u_far, v_far, w_far, p_far, s_far, table_far, rows_far,
    u_out, v_out, base, winv, p_mid, s_ref, ratio, gain, carry, own_ref, rim_recv,
    x1, x2, d1, ur, vr, ds1, us, vs, w_mid, packed_p, inv, u_ref, v_ref, w_ref, p_ref,
    halo1, low, high, chain_send, chain_recv, table_ref, rows_ref, spec, packed_spec, work, back, filt, sides,
    near, cols_send, cols_recv, rows_send, rows_recv, border_tile, border_send, border_recv, rim_send,
    a_ref, zc_ref, mc_ref, cutoff_ref, mask_ref,
    load_sems, send_sems, recv_sems, edge_send, edge_recv, halo_send, halo_recv, last_send, last_recv, chain_out, chain_in, band_in,
):
    band_me = lax.axis_index("lat")
    lon_me = lax.axis_index("lon")
    lat_rows = u_ref.shape[1]
    units = u_ref.shape[0] // per_band
    channels = rows_ref.shape[0]
    half = channels - 1
    per_unit = channels * lat_rows
    split = u_ref.shape[2] // LANE
    mesh_id = pl.DeviceIdType.MESH
    is_first = band_me == 0
    is_last = band_me == bands - 1
    not_first = jnp.logical_not(is_first)
    not_last = jnp.logical_not(is_last)
    masks = partner_masks(per_band)
    partners = [flipped(lon_me, mask) for mask in masks]

    pairs = (
        (p_far, p_ref), (zc_far, zc_ref), (mc_far, mc_ref), (cutoff_far, cutoff_ref), (mask_far, mask_ref), (a_far, a_ref),
        (rows_far, rows_ref), (u_far, u_ref), (v_far, v_ref), (table_far, table_ref), (s_far, s_ref), (w_far, w_ref),
    )
    loads = [pltpu.make_async_copy(far, here, load_sems.at[n]) for n, (far, here) in enumerate(pairs)]
    loads[0].start()
    barrier = pltpu.get_barrier_semaphore()

    def greet(band, lon):
        pl.semaphore_signal(barrier, inc=1, device_id=(band, lon), device_id_type=mesh_id)

    for partner in partners:
        greet(band_me, partner)
    for there, step in ((not_first, -1), (not_last, 1)):
        @pl.when(there)
        def _():
            greet(band_me + step, lon_me)

    for load in loads[1:]:
        load.start()
    loads[0].wait()
    pl.semaphore_wait(barrier, per_band - 1 + jnp.where(is_first, 0, 1) + jnp.where(is_last, 0, 1))
    for there, step, place in ((not_first, -1, 1), (not_last, 1, 0)):
        @pl.when(there)
        def _():
            pl.semaphore_signal(band_in.at[place], inc=1, device_id=(band_me + step, lon_me), device_id_type=mesh_id)


    def scatter(source, target, sem, unit, count=1):
        for g in partners:
            pltpu.make_async_remote_copy(
                src_ref=source.at[pl.ds(g * units + unit, count)], dst_ref=target.at[pl.ds(lon_me * units + unit, count)],
                send_sem=send_sems.at[sem], recv_sem=recv_sems.at[sem, unit],
                device_id=(band_me, g), device_id_type=mesh_id,
            ).start()
        for n in range(count):
            target[lon_me * units + unit + n] = source[lon_me * units + unit + n]

    def gathered(target, sem, unit, count=1):
        block = target.at[pl.ds(0, (per_band - 1) * count)]
        pltpu.make_async_copy(block, block, recv_sems.at[sem, unit]).wait()

    def sent(source, sem):
        block = source.at[pl.ds(0, (per_band - 1) * units)]
        pltpu.make_async_copy(block, block, send_sems.at[sem]).wait()

    def spread_halo(target):
        def one(source, slot, sem, other):
            for g in partners + [lon_me]:
                pltpu.make_async_remote_copy(
                    src_ref=source.at[g], dst_ref=target.at[slot, lon_me],
                    send_sem=halo_send.at[sem], recv_sem=halo_recv.at[sem],
                    device_id=(other, g), device_id_type=mesh_id,
                ).start()

        @pl.when(not_first)
        def _():
            pl.semaphore_wait(band_in.at[0], 1)
            one(low, 1, 0, band_me - 1)

        @pl.when(not_last)
        def _():
            pl.semaphore_wait(band_in.at[1], 1)
            one(high, 0, 1, band_me + 1)

    def halo_wait(sems, upward):
        @pl.when(not_first)
        def _():
            pltpu.make_async_copy(low, low, sems.at[0 if upward else 1]).wait()

        @pl.when(not_last)
        def _():
            pltpu.make_async_copy(low, low, sems.at[1 if upward else 0]).wait()

    def chain_copy(unit, side):
        return pltpu.make_async_remote_copy(
            src_ref=chain_send.at[side, unit], dst_ref=chain_recv.at[side, unit],
            send_sem=chain_out.at[side], recv_sem=chain_in.at[side, unit],
            device_id=((band_me + bands + 1 - 2 * side) % bands, lon_me), device_id_type=mesh_id,
        )

    def chain_start(unit, tile, place):
        for t in range(channels):
            at = lat_rows * t + place
            chain_send[0, unit, 2 * t:2 * t + 2, :] = packed_spec[tile, at:at + 2, :]
            chain_send[1, unit, 2 * t:2 * t + 2, :] = packed_spec[tile, at + 2:at + 4, :]

        @pl.when(not_last)
        def _():
            chain_copy(unit, 0).start()

        @pl.when(not_first)
        def _():
            chain_copy(unit, 1).start()

    def coef_copy(step, side):
        return pltpu.make_async_remote_copy(
            src_ref=own_ref, dst_ref=near.at[side], send_sem=edge_send.at[4 + side], recv_sem=edge_recv.at[4 + side],
            device_id=((band_me + bands + step) % bands, lon_me), device_id_type=mesh_id,
        )

    for unit in range(0, units, 2):
        scatter(p_ref, x1, 0, unit, 2)
    pack_halo(p_ref, low, high, units)
    spread_halo(halo1)

    for load in loads[1:7]:
        load.wait()
    own_coefs(zc_ref, mc_ref, cutoff_ref, mask_ref, own_ref, band_me * lat_rows, half * TILE)

    @pl.when(not_first)
    def _():
        coef_copy(-1, 1).start()

    @pl.when(not_last)
    def _():
        coef_copy(1, 0).start()

    @pl.when(is_first)
    def _():
        near[0] = jnp.zeros(near.shape[1:], jnp.float32)
        chain_recv[0] = jnp.zeros(chain_recv.shape[1:], jnp.float32)
        for g in range(per_band):
            halo1[0, g] = jnp.zeros(halo1.shape[2:], jnp.float32)

    @pl.when(is_last)
    def _():
        near[1] = jnp.zeros(near.shape[1:], jnp.float32)
        chain_recv[1] = jnp.zeros(chain_recv.shape[1:], jnp.float32)
        for g in range(per_band):
            halo1[1, g] = jnp.zeros(halo1.shape[2:], jnp.float32)

    work[...] = jnp.zeros(work.shape, jnp.float32)
    for load in loads[7:9]:
        load.wait()
    pack_edges(u_ref, v_ref, cols_send.at[0], cols_send.at[1], rows_send.at[0], rows_send.at[1])
    edge_copies = []
    for side, step in ((0, -1), (1, 1)):
        edge_copies.append(pltpu.make_async_remote_copy(
            src_ref=cols_send.at[side], dst_ref=cols_recv.at[side], send_sem=edge_send.at[side], recv_sem=edge_recv.at[side],
            device_id=(band_me, (lon_me + per_band + step) % per_band), device_id_type=mesh_id,
        ))
    for copy in edge_copies:
        copy.start()

    def row_copy(step, side):
        return pltpu.make_async_remote_copy(
            src_ref=rows_send.at[side], dst_ref=rows_recv.at[side], send_sem=edge_send.at[2 + side], recv_sem=edge_recv.at[2 + side],
            device_id=((band_me + bands + step) % bands, lon_me), device_id_type=mesh_id,
        )

    @pl.when(not_first)
    def _():
        row_copy(-1, 0).start()

    @pl.when(not_last)
    def _():
        row_copy(1, 1).start()

    @pl.when(is_first)
    def _():
        rows_recv[1] = jnp.zeros(rows_recv.shape[1:], jnp.float32)

    @pl.when(is_last)
    def _():
        rows_recv[0] = jnp.zeros(rows_recv.shape[1:], jnp.float32)

    for load in loads[9:]:
        load.wait()
    factor_columns(a_ref, s_ref, ratio, inv, gain, carry)
    for level in range(s_ref.shape[0]):
        winv[level] = w_ref[level] * inv[level]

    @pl.when(not_first)
    def _():
        coef_copy(1, 0).wait_recv()

    @pl.when(not_last)
    def _():
        coef_copy(-1, 1).wait_recv()

    filter_terms(rows_ref, own_ref, near, filt, sides)

    def circles(source, first, count, stride):
        return [
            [source[d * stride + first + n, :, h * LANE:(h + 1) * LANE] for d in range(per_band) for h in range(split)]
            for n in range(count)
        ]

    def forward(tiles, places):
        for n, xs in enumerate(tiles):
            forward_fill(xs, rows_ref, work, n * per_unit)
        used = len(tiles) * per_unit
        value = three_products(work[0:whole_tiles(used), :], table_ref)
        for n, place in enumerate(places):
            spec[place] = value[n * per_unit:(n + 1) * per_unit]
        return value

    def inverse(count):
        back[0:whole_tiles(count * per_unit), :] = three_products(work[0:whole_tiles(count * per_unit), :], table_ref)

    merid = own_ref[1, :, 0:1]
    pair_count = units // 2
    halo_wait(halo_recv, False)
    forward([
        [halo1[slot, d, :, h * LANE:(h + 1) * LANE] for d in range(per_band) for h in range(split)] for slot in range(2)
    ], [units, units + 1])
    for pair in range(pair_count):
        gathered(x1, 0, 2 * pair, 2)
        forward(circles(x1, 2 * pair, 2, units), [2 * pair, 2 * pair + 1])
        for t in range(channels):
            both = []
            for l in (2 * pair, 2 * pair + 1):
                at = lat_rows * t + 2 * l
                own, row, mid, v_south, v_north = merid_terms(spec, l, t, filt, sides, spec.at[units], spec.at[units + 1], at)
                upper = jnp.where(row == lat_rows - 1, v_north, pltpu.roll(mid, lat_rows - 1, 0))
                lower = jnp.where(row == 0, v_south, pltpu.roll(mid, 1, 0))
                both.append(filt[t, 2] * own + merid * (upper - lower))
            for half_at in range(2):
                at = half_at * per_unit + lat_rows * t
                work[at:at + lat_rows, :] = packed_half(*both, half_at == 1)
        inverse(2)
        put_blocks(ds1, inverse_blocks(back, rows_ref, 0), pair, units)
        scatter(ds1, d1, 1, pair)
        put_blocks(ds1, inverse_blocks(back, rows_ref, per_unit), pair_count + pair, units)
    for pair in range(pair_count):
        scatter(ds1, d1, 1, pair_count + pair)

    for copy in edge_copies:
        copy.wait_recv()

    @pl.when(not_first)
    def _():
        row_copy(1, 1).wait_recv()

    @pl.when(not_last)
    def _():
        row_copy(-1, 0).wait_recv()

    base_divergence(
        u_ref, v_ref, own_ref, cols_recv.at[1], cols_recv.at[0], rows_recv.at[1], rows_recv.at[0], base,
        is_first, is_last,
    )
    def first_spread(level):
        tile = d1[level // units * units + level % units // 2]
        return base[level] + (pltpu.roll(tile, 2 if level % 2 else lat_rows - 2, 0))

    def second_spread(level):
        place = level // units * units + level % units // 2
        return base[level] + unpacked(d1[place], d1[place + pair_count], level % 2 == 1)

    for half_at, spread in enumerate((first_spread, second_spread)):
        for pair in range(pair_count):
            gathered(d1, 1, half_at * pair_count + pair)
        solve_columns(s_ref, winv, p_ref, spread, ratio, gain, carry, vs, p_mid)
        for pair in range(pair_count):
            for d in range(per_band):
                level = d * units + 2 * pair
                packed_p[d * units + half_at * pair_count + pair] = packed_half(p_mid[level], p_mid[level + 1], half_at == 1)
            if not half_at:
                scatter(packed_p, x2, 2, pair)
        if half_at:
            scatter(packed_p, x2, 2, pair_count, pair_count)
    for level in range(s_ref.shape[0]):
        winv[level] = vs[level] * inv[level]

    for tile in range(units):
        pair, half_at = tile % pair_count, tile // pair_count
        if not half_at:
            gathered(x2, 2, tile)
        elif pair == 0:
            gathered(x2, 2, tile, pair_count)
        value = forward(circles(x2, tile, 1, units), [])
        for t in range(channels):
            rows = slice(lat_rows * t, lat_rows * (t + 1))
            total = packed_half(spec[2 * pair, rows, :], spec[2 * pair + 1, rows, :], half_at == 1) + value[rows]
            packed_spec[tile, rows, :] = total
            work[rows, :] = filt[t, 3 + half_at] * total
        for l in range(2):
            if not half_at:
                chain_start(2 * pair + l, tile, 4 * l)
                continue
            for t in range(channels):
                rows = slice(lat_rows * t, lat_rows * (t + 1))
                spec[2 * pair + l, rows, :] = unpacked(packed_spec[pair, rows, :], packed_spec[tile, rows, :], l == 1)
        zonal = packed_half(own_ref[0], own_ref[0], half_at == 1)
        inverse(1)
        moved = [-zonal * x for x in circle_diff(inverse_blocks(back, rows_ref, 0))]
        put_blocks(us, moved, tile, units)
        scatter(us, ur, 3, tile)
        border_tiles(border_tile, moved, tile)
    border_rows(border_tile, border_send)

    def last_copy(source, target, n, g):
        return pltpu.make_async_remote_copy(
            src_ref=source.at[pl.ds(g, 1)], dst_ref=target.at[pl.ds(lon_me, 1)], send_sem=last_send.at[n], recv_sem=last_recv.at[n],
            device_id=(band_me, g), device_id_type=mesh_id,
        )

    def last_scatter(source, target, n):
        for g in partners:
            last_copy(source, target, n, g).start()
        target[lon_me] = source[lon_me]

    last_scatter(border_send, border_recv, 0)
    rim_at = per_unit
    for unit in range(units):
        @pl.when(not_first)
        def _():
            chain_copy(unit, 0).wait_recv()

        @pl.when(not_last)
        def _():
            chain_copy(unit, 1).wait_recv()

        for t in range(channels):
            own, row, mid, v_south, v_north = merid_terms(
                spec, unit, t, filt, sides, chain_recv.at[0, unit], chain_recv.at[1, unit], 2 * t,
            )
            work[lat_rows * t:lat_rows * (t + 1), :] = mid
            rim = rim_at + lat_rows * t + 2 * unit
            work[rim:rim + 1, :] = v_south
            work[rim + 1:rim + 2, :] = v_north
        inverse(2 if unit == units - 1 else 1)
        put_blocks(vs, inverse_blocks(back, rows_ref, 0), unit, units)
        scatter(vs, vr, 4, unit)
    rims = inverse_blocks(back, rows_ref, rim_at)
    for b, value in enumerate(rims):
        rim_send[b // split, :, (b % split) * LANE:(b % split + 1) * LANE] = value

    last_scatter(rim_send, rim_recv, 1)

    def last_wait(target, sems, n):
        block = target.at[pl.ds(0, per_band - 1)]
        pltpu.make_async_copy(block, block, sems.at[n]).wait()

    for tile in range(units):
        gathered(ur, 3, tile)
        for d in range(per_band if tile >= pair_count else 0):
            for l in range(2):
                level = d * units + 2 * (tile - pair_count) + l
                moved = unpacked(ur[d * units + tile - pair_count], ur[d * units + tile], l == 1)
                u_out[level] = u_ref[level] + moved
                w_mid[level] = moved
    last_wait(border_recv, last_recv, 0)
    added_borders(own_ref, border_recv, base, units)
    for unit in range(units):
        gathered(vr, 4, unit)
        own_levels = [d * units + unit for d in range(per_band)]
        for level in own_levels:
            v_out[level] = v_ref[level] + vr[level]
        added_divergence(w_mid, vr, own_ref, base, own_levels)
    last_wait(rim_recv, last_recv, 1)
    for source, sem in ((p_ref, 0), (ds1, 1), (packed_p, 2), (us, 3), (vs, 4)):
        sent(source, sem)
    last_wait(border_send, last_send, 0)
    last_wait(rim_send, last_send, 1)
    halo_wait(halo_send, True)
    for copy in edge_copies:
        copy.wait_send()

    @pl.when(not_first)
    def _():
        pltpu.make_async_copy(chain_send.at[1], chain_send.at[1], chain_out.at[1]).wait()
        coef_copy(-1, 1).wait_send()
        row_copy(-1, 0).wait_send()

    @pl.when(not_last)
    def _():
        pltpu.make_async_copy(chain_send.at[0], chain_send.at[0], chain_out.at[0]).wait()
        coef_copy(1, 0).wait_send()
        row_copy(1, 1).wait_send()


def deliver_kernel(
    units, u_ref, v_ref, base, winv, p_mid, s_ref, ratio, gain, carry, own_ref, rim_ref, u_out, v_out, w_out, p_out, w_end, p_end, sems,
):
    copies = [
        pltpu.make_async_copy(source, target, sems.at[n])
        for n, (source, target) in enumerate(((u_ref, u_out), (v_ref, v_out), (w_end, w_out), (p_end, p_out)))
    ]
    copies[0].start()
    copies[1].start()
    row = lax.broadcasted_iota(jnp.int32, u_ref.shape[1:], 0)
    rows = u_ref.shape[1]
    merid = own_ref[1, :, 0:1]
    south = jnp.where(row == 0, -merid, 0.0)
    north = jnp.where(row == rows - 1, merid, 0.0)

    def spread(level):
        d, l = level // units, 2 * (level % units)
        return base[level] + south * rim_ref[d, l:l + 1, :] + north * rim_ref[d, l + 1:l + 2, :]

    solve_columns(s_ref, winv, p_mid, spread, ratio, gain, carry, w_end, p_end)
    copies[2].start()
    copies[3].start()
    for copy in copies:
        copy.wait()


def deliver(units, arrays):
    shape = arrays[0].shape
    return pl.pallas_call(
        functools.partial(deliver_kernel, units),
        out_shape=(jax.ShapeDtypeStruct(shape, jnp.float32),) * 4,
        in_specs=[pl.BlockSpec(memory_space=pltpu.VMEM)] * len(arrays),
        out_specs=(pl.BlockSpec(memory_space=pl.ANY),) * 4,
        scratch_shapes=[pltpu.VMEM(shape, jnp.float32)] * 2 + [pltpu.SemaphoreType.DMA((4,))],
        compiler_params=pltpu.CompilerParams(vmem_limit_bytes=FINISH_VMEM),
    )(*arrays)


def level_body(
    tables,
    zonal_wind,
    merid_wind,
    vertical_wind,
    pressure,
    zonal_coef,
    merid_coef,
    level_coef,
    sound_coef,
    cutoff,
    filter_mask,
):
    table, rows = (jnp.asarray(t) for t in tables)
    channels = rows.shape[0]
    bands = lax.axis_size("lat")
    per_band = lax.axis_size("lon")
    levels, lat_rows, width = pressure.shape
    units = levels // per_band
    per_unit = channels * lat_rows
    vmem = pl.BlockSpec(memory_space=pltpu.VMEM)
    far = pl.BlockSpec(memory_space=pl.ANY)

    def scratch(*shape):
        return pltpu.VMEM(shape, jnp.float32)

    field = scratch(*pressure.shape)
    halo = scratch(2, per_band, lat_rows, width)
    chain = scratch(2, units, -(-2 * channels // 8) * 8, TILE)
    spare = scratch(whole_tiles(2 * per_unit), TILE)
    dma = pltpu.SemaphoreType.DMA
    operands = (
        level_coef, zonal_coef, merid_coef, cutoff, filter_mask,
        zonal_wind, merid_wind, vertical_wind, pressure, sound_coef, table, rows,
    )
    results = pl.pallas_call(
        functools.partial(fused_kernel, bands, per_band),
        out_shape=(pltpu.VMEM(pressure.shape, jnp.float32),) * 9 + (
            pltpu.VMEM((3, lat_rows, LANE), jnp.float32), pltpu.VMEM((per_band, lat_rows, width), jnp.float32),
        ),
        in_specs=[far] * len(operands),
        out_specs=(vmem,) * 11,
        scratch_shapes=[field] * 15 + [halo, scratch(per_band, lat_rows, width), scratch(per_band, lat_rows, width), chain, chain] + [
            pltpu.VMEM(table.shape, table.dtype), scratch(*rows.shape),
            scratch(units + 2, per_unit, TILE), scratch(units, per_unit, TILE), spare, spare,
            scratch(channels, 5, lat_rows, TILE), scratch(channels, 8, TILE),
            scratch(2, 3, lat_rows, LANE),
            scratch(2, lat_rows, LANE), scratch(2, lat_rows, LANE),
            scratch(2, levels, width), scratch(2, levels, width),
            scratch(per_band, lat_rows, LANE), scratch(per_band, 1, LANE), scratch(per_band, 1, LANE),
            scratch(per_band, lat_rows, width),
            pltpu.SMEM(level_coef.shape, jnp.float32), pltpu.SMEM(zonal_coef.shape, jnp.float32),
            pltpu.SMEM(merid_coef.shape, jnp.float32), pltpu.SMEM(cutoff.shape, jnp.int32),
            pltpu.SMEM(filter_mask.shape, jnp.int32),
            dma((len(operands),)), dma((5,)), dma((5, units)), dma((6,)), dma((6,)), dma((2,)), dma((2,)), dma((2,)), dma((2,)), dma((2,)), dma((2, units)),
            pltpu.SemaphoreType.REGULAR((2,)),
        ],
        compiler_params=pltpu.CompilerParams(collective_id=0, has_side_effects=True, vmem_limit_bytes=FUSED_VMEM),
    )(*[pltpu.with_memory_space_constraint(x, pltpu.HBM) for x in operands])
    return deliver(units, results)


def body(tables, *arrays):
    pressure = arrays[3]
    per_band = lax.axis_size("lon")
    levels, lat_rows, width = pressure.shape
    fits = lat_rows == 8 and levels == 4 * per_band and levels <= LANE and width % LANE == 0 and per_band == 8
    if fits:
        return level_body(tables, *arrays)
    return wide_body(*arrays)


def solution(mesh):
    in_specs = (
        P(None, "lat", "lon"),
        P(None, "lat", "lon"),
        P(None, "lat", "lon"),
        P(None, "lat", "lon"),
        P("lat"),
        P("lat"),
        P(),
        P(None, "lat", "lon"),
        P(),
        P(),
    )
    out_specs = (
        P(None, "lat", "lon"),
        P(None, "lat", "lon"),
        P(None, "lat", "lon"),
        P(None, "lat", "lon"),
    )

    def whole(*arrays):
        tables = circle_tables(arrays[0].shape[2])
        step = jax.shard_map(functools.partial(body, tables), mesh=mesh, in_specs=in_specs, out_specs=out_specs, check_vma=False)
        return step(*arrays)

    return whole
```
